32 devices in a mesh: gx: 4 (over z), gy: 2 (over y), gz: 4 (over x, core).
Axes of the slice: x: 2, y: 2, z: 4, core: 2. Of those that a mesh axis runs over, the one named last changes fastest.
Arguments:
- start_disp: float32 [3, 32, 16, 512], P(None, 'gx', 'gy', 'gz'), may hold values from -2 to 2
- inertial: float32 [3, 32, 16, 512], P(None, 'gx', 'gy', 'gz'), may hold values from -1 to 1
- material: int32 [32, 16, 512], P('gx', 'gy', 'gz'), may hold values from 0 to 7
- pinned: int32 [32, 16, 512], P('gx', 'gy', 'gz'), may hold values 0 or 1
- stiffness: float32 [8], replicated, may hold values from 3 to 100
Outputs:
- displacement: float32 [3, 32, 16, 512], P(None, 'gx', 'gy', 'gz')
The draws below stay inside these ranges and needn't reach their ends.
All inputs are finite; a program needn't handle non-finite values. No bound on the sum of `pinned` on one device may be relied on, other than what follows from the above.
Results may differ from the reference program's by a relative error of at most 0.0003.
Values sent between devices are 32-bit elements; how exact they have to be, the bound alone decides.
No kernel may reach another device: no remote copies, remote signals or barrier semaphores. Data moves between devices by JAX's collectives and lax.ppermute only.
A program may use at most 64 MiB of HBM per device.

```python
import math
import jax
import jax.numpy as jnp
from jax import lax

CX = 8
ITERS = 4
POLAR_STEPS = 6
MATS = 8
NX = 32
NY = 16
NZ = 512


def set_ends(drawn, rng, low, largest):
    spot = [jax.random.randint(jax.random.fold_in(rng, axis), (), 0, length) for axis, length in enumerate(drawn.shape)]
    main_axis = drawn.shape.index(max(drawn.shape))
    next_to = spot[:main_axis] + [(spot[main_axis] + 1) % drawn.shape[main_axis]] + spot[main_axis + 1:]
    return drawn.at[tuple(spot)].set(low).at[tuple(next_to)].set(largest)


def levels(own_key, dims, split, low, largest):
    loudness, own = 1.0, jax.random.fold_in(own_key, 6)
    for position, shards_of in split:
        draws = jnp.exp(jax.random.uniform(jax.random.fold_in(own, position), (shards_of,), jnp.float32, low / len(split), largest / len(split)))
        loudness = loudness * jnp.repeat(draws, dims[position] // shards_of).reshape([-1 if axis == position else 1 for axis in range(len(dims))])
    return loudness


def gaussian(stream_key, extent, spread, most, cuts=(), kind=jnp.bfloat16):
    level = levels(stream_key, extent, cuts, -0.22, 0.18) if cuts else 1.0
    values = jax.random.normal(stream_key, extent, jnp.float32) * spread * level
    return jnp.minimum(jnp.maximum(values, -most), most).astype(kind)


def setup_inputs(seed: int = 0) -> dict:
    key_of = jax.random.split(jax.random.key(seed), 6)
    return {
        "start_disp": gaussian(key_of[0], (3, NX, NY, NZ), 0.5, 2.0, ((1, 4), (2, 2), (3, 4)), jnp.float32),
        "inertial": gaussian(key_of[1], (3, NX, NY, NZ), 0.25, 1.0, ((1, 4), (2, 2), (3, 4)), jnp.float32),
        "material": set_ends(jax.random.randint(key_of[2], (NX, NY, NZ), 0, MATS), jax.random.fold_in(key_of[2], 1), 0, MATS - 1).astype(jnp.int32),
        "pinned": set_ends((jax.random.randint(key_of[3], (NX, NY, NZ), 0, 16) < 1).astype(jnp.int32), jax.random.fold_in(key_of[3], 1), 0, 1),
        "stiffness": jnp.clip(jnp.exp(jax.random.uniform(key_of[4], (MATS,), jnp.float32, math.log(3.0), math.log(100.0))), 3.0, 100.0),
    }


inertia = 1.0
relax = 0.6
radius = 0.9

def forward_diff(field, axis):
    size = field.shape[axis]
    return lax.slice_in_dim(field, 1, size, axis=axis) - lax.slice_in_dim(field, 0, size - 1, axis=axis)

def pair_sum(field, axis):
    size = field.shape[axis]
    return lax.slice_in_dim(field, 1, size, axis=axis) + lax.slice_in_dim(field, 0, size - 1, axis=axis)

def gradient(field, axis):
    result = forward_diff(field, axis)
    for other in range(3):
        if other != axis:
            result = pair_sum(result, other)
    return 0.25 * result

def project(nodes, welem):
    deform = [[gradient(nodes[c], d) + (1.0 if c == d else 0.0) for d in range(3)] for c in range(3)]
    total = sum((deform[c][d] * deform[c][d] for c in range(3) for d in range(3)))
    scale = jnp.maximum(jnp.sqrt(total / 3.0), 1.0)
    rotate = [[deform[c][d] / scale for d in range(3)] for c in range(3)]
    for step in range(POLAR_STEPS):
        middle = [[(1.5 if i == j else 0.0) - 0.5 * sum((rotate[k][i] * rotate[k][j] for k in range(3))) for j in range(3)] for i in range(3)]
        rotate = [[sum((rotate[c][j] * middle[j][d] for j in range(3))) for d in range(3)] for c in range(3)]
    return [welem * (deform[c][d] - rotate[c][d]) for c in range(3) for d in range(3)]

def assemble(stress):
    forces = []
    for c in range(3):
        total = 0.0
        for d in range(3):
            term = stress[3 * c + d]
            for other in range(3):
                if other != d:
                    term = pair_sum(term, other)
            total = total - 0.25 * forward_diff(term, d)
        forces.append(total)
    return jnp.stack(forces)

def diagonal(welem):
    total = welem
    for axis in range(3):
        total = pair_sum(total, axis)
    return inertia + 3.0 / 16.0 * total

def lookup(material, stiffness):
    total = jnp.zeros(material.shape, jnp.float32)
    for index in range(MATS):
        total = total + jnp.where(material == index, stiffness[index], 0.0)
    return total

def reference(start_disp, inertial, material, pinned, stiffness):
    grid_x = lax.broadcasted_iota(jnp.int32, material.shape, 0)
    grid_y = lax.broadcasted_iota(jnp.int32, material.shape, 1)
    grid_z = lax.broadcasted_iota(jnp.int32, material.shape, 2)
    valid = (grid_x < NX - 1) & (grid_y < NY - 1) & (grid_z < NZ - 1)
    weights = jnp.where(valid, lookup(material, stiffness), 0.0)
    welem = jnp.pad(weights, ((1, 0), (1, 0), (1, 0)))
    diag = diagonal(welem)
    pins = pinned[None] > 0
    disp = jnp.where(pins, inertial, start_disp)
    previous = disp
    omega = 1.0
    blocks = NX // CX
    for step in range(ITERS):
        padded = jnp.pad(disp, ((0, 0), (1, 1), (1, 1), (1, 1)))

        def block_forces(index):
            start = (index * CX).astype(jnp.int32)
            nodes = lax.dynamic_slice_in_dim(padded, start, CX + 2, 1)
            wslab = lax.dynamic_slice_in_dim(welem, start, CX + 1, 0)
            return assemble(project([nodes[0], nodes[1], nodes[2]], wslab))
        parts = lax.map(block_forces, jnp.arange(blocks, dtype=jnp.int32))
        forces = jnp.moveaxis(parts, 0, 1).reshape(3, NX, NY, NZ)
        target = disp - relax * (inertia * (disp - inertial) + forces) / diag[None]
        if step == 0:
            fresh = target
        else:
            omega = 2.0 / (2.0 - radius * radius) if step == 1 else 4.0 / (4.0 - radius * radius * omega)
            fresh = omega * (target - previous) + previous
        fresh = jnp.where(pins, inertial, fresh)
        previous = disp
        disp = fresh
    return disp
```

```python
import functools
import math

import jax
import jax.numpy as jnp
from jax import lax
from jax.experimental import pallas as pl
from jax.experimental.pallas import tpu as pltpu
from jax.sharding import PartitionSpec as P

ITERS = 4
POLAR_STEPS = 6
MATS = 8
RELAX = 0.6
RADIUS = 0.9

HALO = ITERS
SCALE = 0.25 / math.sqrt(2.0)
UNIT = 1.0 / math.sqrt(2.0)
CH = 8
W_CH = 6
FREE_CH = 7
GROUPS = 4
SPAN = 32

VM = pl.BlockSpec(memory_space=pltpu.VMEM)
SM = pl.BlockSpec(memory_space=pltpu.SMEM)


def omegas():
    values = [1.0]
    for step in range(1, ITERS):
        if step == 1:
            values.append(2.0 / (2.0 - RADIUS * RADIUS))
        else:
            values.append(4.0 / (4.0 - RADIUS * RADIUS * values[-1]))
    return values


def lane_ids():
    return lax.broadcasted_iota(jnp.int32, (8, 128), 1)


def sub_ids():
    return lax.broadcasted_iota(jnp.int32, (8, 128), 0)


def roll_z(value, amount):
    amount = amount % 128
    return value if amount == 0 else pltpu.roll(value, amount, 1)


def next_x(pair):
    return (pair[1], pltpu.roll(pair[0], 7, 0))


def prev_x(pair):
    return (pltpu.roll(pair[1], 1, 0), pair[0])


def add2(a, b):
    return tuple(x + y for x, y in zip(a, b))


def sub2(a, b):
    return tuple(x - y for x, y in zip(a, b))


def gradient_row(vrow):
    out = []
    for pair in vrow:
        ahead = tuple(roll_z(t, -1) for t in pair)
        sz = add2(pair, ahead)
        dz = sub2(ahead, pair)
        nsz = next_x(sz)
        out.append((add2(sz, nsz), sub2(nsz, sz), add2(dz, next_x(dz))))
    return out


def polar_stress(f, weight):
    def gram(z):
        return {
            (i, j): z[0][i] * z[0][j] + z[1][i] * z[1][j] + z[2][i] * z[2][j]
            for i in range(3)
            for j in range(i, 3)
        }

    def apply(z, diag, off):
        rows = []
        for c in range(3):
            row = []
            for d in range(3):
                value = z[c][d] * diag[d]
                for j in range(3):
                    if j != d:
                        value = value - z[c][j] * off[(min(j, d), max(j, d))]
                row.append(value)
            rows.append(row)
        return rows

    g = gram(f)
    trace = g[(0, 0)] + g[(1, 1)] + g[(2, 2)]
    s = jnp.minimum(lax.rsqrt(trace * (2.0 / 3.0)), 1.0)
    cube = s * s * s
    base = 1.5 * s
    z = apply(
        f,
        [base - cube * g[(i, i)] for i in range(3)],
        {key: cube * g[key] for key in ((0, 1), (0, 2), (1, 2))},
    )
    for _ in range(POLAR_STEPS - 1):
        g = gram(z)
        z = apply(z, [1.5 - g[(i, i)] for i in range(3)], g)
    return [[weight * (z[c][d] - f[c][d]) for d in range(3)] for c in range(3)]


def deform_rows(low, high):
    out = []
    for c in range(3):
        row = [
            add2(low[c][1], high[c][1]),
            sub2(high[c][0], low[c][0]),
            add2(low[c][2], high[c][2]),
        ]
        row[c] = tuple(t + UNIT for t in row[c])
        out.append(row)
    return out


def stress_row(f, weight):
    tiles = [
        polar_stress([[f[c][d][t] for d in range(3)] for c in range(3)], weight[t])
        for t in range(2)
    ]
    return [[(tiles[0][c][d], tiles[1][c][d]) for d in range(3)] for c in range(3)]


def force_parts(now, before):
    out = []
    for c in range(3):
        a = add2(now[c][0], before[c][0])
        b = sub2(now[c][1], before[c][1])
        e = add2(now[c][2], before[c][2])
        left = add2(add2(a, b), prev_x(sub2(b, a)))
        right = add2(e, prev_x(e))
        out.append((add2(left, right), sub2(left, right)))
    return out


def update_row(part, v, vin, prev, g, omega):
    new = []
    for c in range(3):
        row = []
        for t in range(2):
            force = part[c][0][t] + roll_z(part[c][1][t], 1)
            y = v[c][t] - g[t] * ((v[c][t] - vin[c][t]) + force)
            row.append(prev[c][t] + omega * (y - prev[c][t]))
        new.append(tuple(row))
    return new


def omega_at(step):
    values = omegas()
    out = jnp.float32(values[0])
    for index in range(1, ITERS):
        out = jnp.where(step == index, jnp.float32(values[index]), out)
    return out


class Shape:
    def __init__(self, mesh, size):
        self.n = tuple(mesh.shape[a] for a in ("gx", "gy", "gz"))
        self.size = size
        self.mirror = self.n[1] == 2
        self.own = 0 if self.mirror else HALO
        self.rows = size[1] + HALO * (1 if self.mirror else 2)
        self.erows = self.rows // GROUPS


def even(axis):
    return lax.rem(lax.axis_index(axis), 2) == 0


def pack_faces(first, second):
    upper = sub_ids() >= HALO
    low = jnp.where(upper, pltpu.roll(second, HALO, 0), first)
    high = jnp.where(upper, second, pltpu.roll(first, HALO, 0))
    return low, high


def prep_kernel(shape, start, inert, mat, pin, stiff, own, ysend, xsend, xysend):
    sx, sy, sz = shape.size
    gx, gy, gz = (lax.axis_index(a) for a in ("gx", "gy", "gz"))
    flip = (gy == 1) if shape.mirror else False
    sign = jnp.where(flip, -1.0, 1.0).astype(jnp.float32) if shape.mirror else jnp.float32(1.0)
    inside = (sub_ids() + gx * sx < shape.n[0] * sx - 1) & (
        lane_ids() + gz * sz < shape.n[2] * sz - 1
    )
    levels = [stiff[i] * (1.0 / 16.0) for i in range(MATS)]
    own[W_CH, sy] = jnp.zeros((8, 128), jnp.float32)
    for r in range(sy):
        at = pl.ds(r, sx, stride=sy)
        fixed = pin[at, :] > 0
        kind = mat[at, :]
        weight = jnp.zeros((8, 128), jnp.float32)
        for index in range(MATS):
            weight = jnp.where(kind == index, levels[index], weight)
        valid = inside & (r + gy * sy < shape.n[1] * sy - 1)
        weight = jnp.where(valid, weight, 0.0)
        node = jnp.where(flip, sy - 1 - r, r) + 1 if shape.mirror else r + 1
        cell = jnp.where(flip, sy - 2 - r, r) + 1 if shape.mirror else r + 1
        for c in range(3):
            factor = SCALE * sign if c == 1 else SCALE
            goal = inert[c, at, :] * factor
            own[c, node] = jnp.where(fixed, goal, start[c, at, :] * factor)
            own[3 + c, node] = goal
        own[W_CH, cell] = weight
        own[FREE_CH, node] = jnp.where(fixed, 0.0, 1.0)
    ex = even("gx")
    for c in range(CH):
        for k in range(sy // 2):
            low, high = pack_faces(own[c, 2 * k + 1], own[c, 2 * k + 2])
            xsend[0][c, k] = jnp.where(ex, high, low)
            xsend[1][c, k] = jnp.where(ex, low, high)
        for side in range(len(ysend)):
            rows = []
            for d in range(HALO):
                if shape.mirror:
                    node = sy - 1 - d
                    if c == W_CH:
                        node = node - jnp.where(flip, 1, 0)
                else:
                    up = even("gy") if side == 0 else jnp.logical_not(even("gy"))
                    node = jnp.where(up, sy - HALO + d, d)
                rows.append(own[c, node + 1])
                ysend[side][c, d] = rows[-1]
            for k in range(HALO // 2):
                low, high = pack_faces(rows[2 * k], rows[2 * k + 1])
                xysend[2 * side][c, k] = jnp.where(ex, high, low)
                xysend[2 * side + 1][c, k] = jnp.where(ex, low, high)


def join_kernel(shape, own, yrecv, xrecv, xyrecv, full, zsend, nat):
    sx, sy, sz = shape.size
    rows = shape.rows
    ex, ez = even("gx"), even("gz")
    flip = (lax.axis_index("gy") == 1) if shape.mirror else False

    def put(c, row, low, mid, high):
        nat[c, row, 0:HALO] = low
        nat[c, row, HALO : HALO + sx] = mid
        nat[c, row, HALO + sx :] = high

    for c in range(CH):
        turned = shape.mirror and c in (1, 4)
        for k in range(sy // 2):
            a, b = xrecv[0][c, k], xrecv[1][c, k]
            low, high = jnp.where(ex, b, a), jnp.where(ex, a, b)
            for h in range(2):
                part = slice(HALO * h, HALO * h + HALO)
                put(c, shape.own + 2 * k + h, low[part], own[c, 2 * k + h + 1], high[part])
        for side in range(2 if not shape.mirror else 1):
            for k in range(HALO // 2):
                if shape.mirror:
                    a, b = xyrecv[0][c, k], xyrecv[1][c, k]
                    mids = [yrecv[0][c, 2 * k + h] for h in range(2)]
                    if turned:
                        a, b = -a, -b
                        mids = [-t for t in mids]
                else:
                    lower = even("gy") if side else jnp.logical_not(even("gy"))
                    a, b = (jnp.where(lower, xyrecv[i][c, k], xyrecv[2 + i][c, k]) for i in range(2))
                    mids = [
                        jnp.where(lower, yrecv[0][c, 2 * k + h], yrecv[1][c, 2 * k + h])
                        for h in range(2)
                    ]
                low, high = jnp.where(ex, b, a), jnp.where(ex, a, b)
                for h in range(2):
                    part = slice(HALO * h, HALO * h + HALO)
                    d = 2 * k + h
                    if shape.mirror:
                        row = sy + d
                        if c == W_CH:
                            row = row - jnp.where(flip, 1, 0)
                    else:
                        row = d + side * (HALO + sy)
                    put(c, row, low[part], mids[h], high[part])
        if c == W_CH:
            nat[c, rows - 1] = jnp.zeros((sx + 2 * HALO, 128), jnp.float32)
    slot = lane_ids() // HALO
    for m in range(shape.erows):
        for t in range(2):
            up = jnp.zeros((8, 128), jnp.float32)
            down = jnp.zeros((8, 128), jnp.float32)
            for g in range(GROUPS):
                for c in range(CH):
                    tile = nat[c, g * shape.erows + m, pl.ds(t, 8, stride=2), :]
                    full[c, g * shape.erows + m, t] = tile
                    place = slot == (SPAN // HALO) * g + c
                    to = SPAN * g + HALO * c
                    up = jnp.where(place, roll_z(tile, to - (sz - HALO)), up)
                    down = jnp.where(place, roll_z(tile, to), down)
            zsend[0][m, t] = jnp.where(ez, up, down)
            zsend[1][m, t] = jnp.where(ez, down, up)


def load_row(ref, row, channels=range(3)):
    return [(ref[c, row, 0], ref[c, row, 1]) for c in channels]


def step_size(now, before, free):
    total = add2(now, before)
    total = add2(total, prev_x(total))
    return tuple(
        RELAX * f / (1.0 + 3.0 * (t + roll_z(t, 1))) for t, f in zip(total, free)
    )


def main_kernel(shape, full, v, prev, gsize, grad, stress, part):
    rows = shape.rows
    zero = jnp.zeros((8, 128), jnp.float32)
    for row in range(rows):
        for c in range(3):
            for t in range(2):
                tile = full[c, row, t]
                v[c, row + 1, t] = tile
                prev[c, row + 1, t] = tile
        now = load_row(full, row, (W_CH,))[0]
        before = load_row(full, row - 1, (W_CH,))[0] if row else (zero, zero)
        g = step_size(now, before, load_row(full, row, (FREE_CH,))[0])
        for t in range(2):
            gsize[row + 1, t] = g[t]
    for i in range(9):
        for t in range(2):
            stress[i, 0, t] = zero
    for c in range(3):
        for t in range(2):
            v[c, 0, t] = zero
            v[c, rows + 1, t] = zero
            prev[c, 0, t] = zero
    for t in range(2):
        gsize[0, t] = zero

    def put_gradient(row, value):
        for c in range(3):
            for kind in range(3):
                for t in range(2):
                    grad[3 * c + kind, row, t] = value[c][kind][t]

    def get9(ref, row):
        return [[(ref[3 * c + k, row, 0], ref[3 * c + k, row, 1]) for k in range(3)] for c in range(3)]

    def iteration(step, carry):
        omega = omega_at(step)
        first = 0 if shape.mirror else step
        last = rows - 1 - step
        put_gradient(first, gradient_row(load_row(v, first + 1)))
        put_gradient(first + 1, gradient_row(load_row(v, first + 2)))

        def body(j, carry):
            ahead = load_row(v, j + 3)
            low, high = get9(grad, j), get9(grad, j + 1)
            weight = load_row(full, j, (W_CH,))[0]
            before = get9(stress, j)
            held = [
                tuple((part[2 * c + i, j, 0], part[2 * c + i, j, 1]) for i in range(2))
                for c in range(3)
            ]
            old = load_row(v, j)
            oldest = load_row(prev, j)
            goal = load_row(full, max(j - 1, 0), (3, 4, 5))
            g = (gsize[j, 0], gsize[j, 1])

            after = gradient_row(ahead)
            now = stress_row(deform_rows(low, high), weight)
            parts = force_parts(now, before)
            new = update_row(held, old, goal, oldest, g, omega)

            put_gradient(j + 2, after)
            for c in range(3):
                for t in range(2):
                    for d in range(3):
                        stress[3 * c + d, j + 1, t] = now[c][d][t]
                    for i in range(2):
                        part[2 * c + i, j + 1, t] = parts[c][i][t]
                    prev[c, j, t] = old[c][t]
                    v[c, j, t] = new[c][t]
            return carry

        for j in range(first, last):
            body(j, 0)
        held = [
            tuple((part[2 * c + i, last, 0], part[2 * c + i, last, 1]) for i in range(2))
            for c in range(3)
        ]
        old = load_row(v, last)
        new = update_row(
            held,
            old,
            load_row(full, last - 1, (3, 4, 5)),
            load_row(prev, last),
            (gsize[last, 0], gsize[last, 1]),
            omega,
        )
        for c in range(3):
            for t in range(2):
                prev[c, last, t] = old[c][t]
                v[c, last, t] = new[c][t]
        return carry

    for step in range(ITERS):
        iteration(step, 0)


def edge_kernel(shape, full, main, zrecv0, zrecv1, out, v, prev, goal, gsize, stiff, tiles):
    sx, sy, sz = shape.size
    erows = shape.erows
    ez = even("gz")
    lane = lane_ids()
    within = lane % SPAN
    half = SPAN // 2

    def window(c, m, t):
        value = jnp.zeros((8, 128), jnp.float32)
        for g in range(GROUPS):
            tile = full[c, g * erows + m, t]
            base = SPAN * g
            value = jnp.where(
                (lane >= base + HALO) & (lane < base + half), roll_z(tile, base + HALO), value
            )
            value = jnp.where(
                (lane >= base + half) & (lane < base + SPAN - HALO),
                roll_z(tile, base + SPAN - HALO - sz),
                value,
            )
        return value

    for m in range(erows):
        for t in range(2):
            a, b = zrecv0[m, t], zrecv1[m, t]
            low, high = jnp.where(ez, b, a), jnp.where(ez, a, b)

            def extended(c):
                value = window(c, m, t)
                value = jnp.where(within < HALO, roll_z(low, -HALO * c), value)
                return jnp.where(
                    within >= SPAN - HALO, roll_z(high, SPAN - HALO - HALO * c), value
                )

            for c in range(3):
                value = extended(c)
                v[c, m, t] = value
                prev[c, m, t] = value
                goal[c, m, t] = extended(3 + c)
            stiff[m, t] = extended(W_CH)
            gsize[m, t] = extended(FREE_CH)
    weights = [(stiff[m, 0], stiff[m, 1]) for m in range(erows)]
    behind = tuple(roll_z(t, SPAN) for t in weights[-1])
    for m in range(erows):
        g = step_size(weights[m], weights[m - 1] if m else behind, (gsize[m, 0], gsize[m, 1]))
        for t in range(2):
            gsize[m, t] = g[t]

    def iteration(step, carry):
        omega = omega_at(step)
        grads = [gradient_row(load_row(v, m)) for m in range(erows)]
        grads.append([[tuple(roll_z(t, -SPAN) for t in pair) for pair in row] for row in grads[0]])
        stress = [None] * erows
        for m in [erows - 1] + list(range(erows - 1)):
            stress[m] = stress_row(
                deform_rows(grads[m], grads[m + 1]), (stiff[m, 0], stiff[m, 1])
            )
        wrapped = [[tuple(roll_z(t, SPAN) for t in pair) for pair in row] for row in stress[-1]]
        for m in range(erows):
            parts = force_parts(stress[m], stress[m - 1] if m else wrapped)
            old = load_row(v, m)
            new = update_row(
                parts, old, load_row(goal, m), load_row(prev, m), (gsize[m, 0], gsize[m, 1]), omega
            )
            for c in range(3):
                for t in range(2):
                    prev[c, m, t] = old[c][t]
                    v[c, m, t] = new[c][t]
        return carry

    lax.fori_loop(0, ITERS, iteration, 0)
    flip = (lax.axis_index("gy") == 1) if shape.mirror else False
    for r in range(sy):
        row = shape.own + r
        g, m = divmod(row, erows)
        base = SPAN * g
        for c in range(3):
            factor = 1.0 / SCALE
            if shape.mirror and c == 1:
                factor = jnp.where(flip, -factor, factor).astype(jnp.float32)
            for t in range(2):
                edge = v[c, m, t]
                value = main[c, row + 1, t]
                value = jnp.where(lane < HALO, roll_z(edge, -(base + HALO)), value)
                value = jnp.where(
                    lane >= sz - HALO, roll_z(edge, sz - HALO - (base + SPAN - 2 * HALO)), value
                )
                tiles[pl.ds(t, 8, stride=2), :] = value * factor
            place = jnp.where(flip, sy - 1 - r, r) if shape.mirror else r
            out[c, pl.ds(place, sx, stride=sy), :] = tiles[HALO : HALO + sx]


def swap(size, parity):
    pairs = []
    for i in range(size):
        j = i + 1 if i % 2 == parity else i - 1
        if 0 <= j < size:
            pairs.append((i, j))
    return pairs


def swap2(nx, px, ny, py):
    return [
        (i * ny + j, a * ny + b)
        for i, a in swap(nx, px)
        for j, b in swap(ny, py)
    ]


def f32(*dims):
    return jax.ShapeDtypeStruct(dims, jnp.float32)


def scratch(*dims):
    return pltpu.VMEM(dims, jnp.float32)


def call(body, outs, args, scratches=(), specs=None):
    return pl.pallas_call(
        body,
        out_shape=outs,
        in_specs=specs or [VM] * len(args),
        out_specs=jax.tree.map(lambda _: VM, outs),
        scratch_shapes=list(scratches),
        compiler_params=pltpu.CompilerParams(vmem_limit_bytes=40 * 1024 * 1024),
        cost_estimate=pl.CostEstimate(flops=2_000_000, bytes_accessed=100_000, transcendentals=0),
    )(*args)


def per_device(mesh, start_disp, inertial, material, pinned, stiffness):
    shape = Shape(mesh, material.shape)
    sx, sy, sz = shape.size
    nx, ny, nz = shape.n
    sides = 1 if shape.mirror else 2
    rows, erows = shape.rows, shape.erows

    def prep(start, inert, mat, pin, stiff, own, *rest):
        prep_kernel(
            shape, start, inert, mat, pin, stiff, own,
            rest[2 : 2 + sides], rest[:2], rest[2 + sides :],
        )

    outs = prep_outs = [f32(CH, sy + 1, sx, sz)]
    outs += [f32(CH, sy // 2, 8, sz)] * 2 + [f32(CH, HALO, sx, sz)] * sides
    outs += [f32(CH, HALO // 2, 8, sz)] * (2 * sides)
    own, *sent = call(
        prep,
        outs,
        (
            start_disp.reshape(3, sx * sy, sz),
            inertial.reshape(3, sx * sy, sz),
            material.reshape(sx * sy, sz),
            pinned.reshape(sx * sy, sz),
            stiffness,
        ),
        specs=[VM] * 4 + [SM],
    )
    recv = [lax.ppermute(sent[p], "gx", swap(nx, p)) for p in range(2)]
    recv += [lax.ppermute(sent[2 + p], "gy", swap(ny, p)) for p in range(sides)]
    recv += [
        lax.ppermute(sent[2 + sides + 2 * q + p], ("gx", "gy"), swap2(nx, p, ny, q))
        for q in range(sides)
        for p in range(2)
    ]

    def join(own, *rest):
        x, rest = rest[:2], rest[2:]
        y, rest = rest[:sides], rest[sides:]
        xy, rest = rest[: 2 * sides], rest[2 * sides :]
        full, z0, z1, nat = rest
        join_kernel(shape, own, y, x, xy, full, (z0, z1), nat)

    full, z0, z1 = call(
        join,
        [f32(CH, rows, 2, 8, sz), f32(erows, 2, 8, sz), f32(erows, 2, 8, sz)],
        (own, *recv),
        [scratch(CH, rows, sx + 2 * HALO, sz)],
    )
    z0 = lax.ppermute(z0, "gz", swap(nz, 0))
    z1 = lax.ppermute(z1, "gz", swap(nz, 1))
    (main,) = call(
        functools.partial(main_kernel, shape),
        [f32(3, rows + 2, 2, 8, sz)],
        (full,),
        [
            scratch(3, rows + 2, 2, 8, sz),
            scratch(rows + 2, 2, 8, sz),
            scratch(9, rows + 2, 2, 8, sz),
            scratch(9, rows + 2, 2, 8, sz),
            scratch(6, rows + 2, 2, 8, sz),
        ],
    )
    (out,) = call(
        functools.partial(edge_kernel, shape),
        [f32(3, sx * sy, sz)],
        (full, main, z0, z1),
        [
            scratch(3, erows, 2, 8, sz),
            scratch(3, erows, 2, 8, sz),
            scratch(3, erows, 2, 8, sz),
            scratch(erows, 2, 8, sz),
            scratch(erows, 2, 8, sz),
            scratch(2 * 8, sz),
        ],
    )
    return out.reshape(3, sx, sy, sz)


def solution(mesh):
    placed = (
        P(None, "gx", "gy", "gz"),
        P(None, "gx", "gy", "gz"),
        P("gx", "gy", "gz"),
        P("gx", "gy", "gz"),
        P(),
    )
    return jax.shard_map(
        functools.partial(per_device, mesh),
        mesh=mesh,
        in_specs=placed,
        out_specs=P(None, "gx", "gy", "gz"),
        check_vma=False,
    )
```

```python
import functools
import math

import jax
import jax.numpy as jnp
from jax import lax
from jax.experimental import pallas as pl
from jax.experimental.pallas import tpu as pltpu
from jax.sharding import PartitionSpec as P

ITERS = 4
POLAR_STEPS = 6
MATS = 8
RELAX = 0.6
RADIUS = 0.9

HALO = ITERS
SCALE = 0.25 / math.sqrt(2.0)
UNIT = 1.0 / math.sqrt(2.0)
CH = 8
W_CH = 6
FREE_CH = 7
GROUPS = 4
SPAN = 32

VM = pl.BlockSpec(memory_space=pltpu.VMEM)
HBM = pl.BlockSpec(memory_space=pltpu.MemorySpace.HBM)


def omegas():
    values = [1.0]
    for step in range(1, ITERS):
        if step == 1:
            values.append(2.0 / (2.0 - RADIUS * RADIUS))
        else:
            values.append(4.0 / (4.0 - RADIUS * RADIUS * values[-1]))
    return values


def lane_ids():
    return lax.broadcasted_iota(jnp.int32, (8, 128), 1)


def sub_ids():
    return lax.broadcasted_iota(jnp.int32, (8, 128), 0)


def roll_z(value, amount):
    amount = amount % 128
    return value if amount == 0 else pltpu.roll(value, amount, 1)


def next_x(pair):
    return (pair[1], pltpu.roll(pair[0], 7, 0))


def prev_x(pair):
    return (pltpu.roll(pair[1], 1, 0), pair[0])


def add2(a, b):
    return tuple(x + y for x, y in zip(a, b))


def sub2(a, b):
    return tuple(x - y for x, y in zip(a, b))


def gradient_row(vrow):
    out = []
    for pair in vrow:
        ahead = tuple(roll_z(t, -1) for t in pair)
        sz = add2(pair, ahead)
        dz = sub2(ahead, pair)
        nsz = next_x(sz)
        out.append((add2(sz, nsz), sub2(nsz, sz), add2(dz, next_x(dz))))
    return out


def polar_stress(f, weight):
    def gram(z):
        return {
            (i, j): z[0][i] * z[0][j] + z[1][i] * z[1][j] + z[2][i] * z[2][j]
            for i in range(3)
            for j in range(i, 3)
        }

    def apply(z, diag, off):
        rows = []
        for c in range(3):
            row = []
            for d in range(3):
                value = z[c][d] * diag[d]
                for j in range(3):
                    if j != d:
                        value = value - z[c][j] * off[(min(j, d), max(j, d))]
                row.append(value)
            rows.append(row)
        return rows

    g = gram(f)
    trace = g[(0, 0)] + g[(1, 1)] + g[(2, 2)]
    s = jnp.minimum(lax.rsqrt(trace * (2.0 / 3.0)), 1.0)
    cube = s * s * s
    base = 1.5 * s
    z = apply(
        f,
        [base - cube * g[(i, i)] for i in range(3)],
        {key: cube * g[key] for key in ((0, 1), (0, 2), (1, 2))},
    )
    for _ in range(POLAR_STEPS - 1):
        g = gram(z)
        z = apply(z, [1.5 - g[(i, i)] for i in range(3)], g)
    return [[weight * (z[c][d] - f[c][d]) for d in range(3)] for c in range(3)]


def deform_rows(low, high):
    out = []
    for c in range(3):
        row = [
            add2(low[c][1], high[c][1]),
            sub2(high[c][0], low[c][0]),
            add2(low[c][2], high[c][2]),
        ]
        row[c] = tuple(t + UNIT for t in row[c])
        out.append(row)
    return out


def stress_row(f, weight):
    tiles = [
        polar_stress([[f[c][d][t] for d in range(3)] for c in range(3)], weight[t])
        for t in range(2)
    ]
    return [[(tiles[0][c][d], tiles[1][c][d]) for d in range(3)] for c in range(3)]


def force_parts(now, before):
    out = []
    for c in range(3):
        a = add2(now[c][0], before[c][0])
        b = sub2(now[c][1], before[c][1])
        e = add2(now[c][2], before[c][2])
        left = add2(add2(a, b), prev_x(sub2(b, a)))
        right = add2(e, prev_x(e))
        out.append((add2(left, right), sub2(left, right)))
    return out


def update_row(part, v, vin, prev, g, omega):
    new = []
    for c in range(3):
        row = []
        for t in range(2):
            force = part[c][0][t] + roll_z(part[c][1][t], 1)
            y = v[c][t] - g[t] * ((v[c][t] - vin[c][t]) + force)
            row.append(prev[c][t] + omega * (y - prev[c][t]))
        new.append(tuple(row))
    return new


def omega_at(step):
    values = omegas()
    out = jnp.float32(values[0])
    for index in range(1, ITERS):
        out = jnp.where(step == index, jnp.float32(values[index]), out)
    return out


class Shape:
    def __init__(self, mesh, size):
        self.n = tuple(mesh.shape[a] for a in ("gx", "gy", "gz"))
        self.size = size
        self.mirror = self.n[1] == 2
        self.own = 0 if self.mirror else HALO
        self.rows = size[1] + HALO * (1 if self.mirror else 2)
        self.erows = self.rows // GROUPS


def even(axis):
    return lax.rem(lax.axis_index(axis), 2) == 0


def pack_faces(first, second):
    upper = sub_ids() >= HALO
    low = jnp.where(upper, pltpu.roll(second, HALO, 0), first)
    high = jnp.where(upper, second, pltpu.roll(first, HALO, 0))
    return low, high


def prep_kernel(shape, start, inert, mat, pin, stiff, own, ysend, xsend, xysend):
    sx, sy, sz = shape.size
    gx, gy, gz = (lax.axis_index(a) for a in ("gx", "gy", "gz"))
    flip = (gy == 1) if shape.mirror else False
    sign = jnp.where(flip, -1.0, 1.0).astype(jnp.float32) if shape.mirror else jnp.float32(1.0)
    inside = (sub_ids() + gx * sx < shape.n[0] * sx - 1) & (
        lane_ids() + gz * sz < shape.n[2] * sz - 1
    )
    levels = [stiff[i] * (1.0 / 16.0) for i in range(MATS)]
    own[W_CH, sy] = jnp.zeros((8, 128), jnp.float32)
    for r in range(sy):
        at = pl.ds(r, sx, stride=sy)
        fixed = pin[at, :] > 0
        kind = mat[at, :]
        weight = jnp.zeros((8, 128), jnp.float32)
        for index in range(MATS):
            weight = jnp.where(kind == index, levels[index], weight)
        valid = inside & (r + gy * sy < shape.n[1] * sy - 1)
        weight = jnp.where(valid, weight, 0.0)
        node = jnp.where(flip, sy - 1 - r, r) + 1 if shape.mirror else r + 1
        cell = jnp.where(flip, sy - 2 - r, r) + 1 if shape.mirror else r + 1
        for c in range(3):
            factor = SCALE * sign if c == 1 else SCALE
            goal = inert[c, at, :] * factor
            own[c, node] = jnp.where(fixed, goal, start[c, at, :] * factor)
            own[3 + c, node] = goal
        own[W_CH, cell] = weight
        own[FREE_CH, node] = jnp.where(fixed, 0.0, 1.0)
    ex = even("gx")
    for c in range(CH):
        for k in range(sy // 2):
            low, high = pack_faces(own[c, 2 * k + 1], own[c, 2 * k + 2])
            xsend[0][c, k] = jnp.where(ex, high, low)
            xsend[1][c, k] = jnp.where(ex, low, high)
        for side in range(len(ysend)):
            rows = []
            for d in range(HALO):
                if shape.mirror:
                    node = sy - 1 - d
                    if c == W_CH:
                        node = node - jnp.where(flip, 1, 0)
                else:
                    up = even("gy") if side == 0 else jnp.logical_not(even("gy"))
                    node = jnp.where(up, sy - HALO + d, d)
                rows.append(own[c, node + 1])
                ysend[side][c, d] = rows[-1]
            for k in range(HALO // 2):
                low, high = pack_faces(rows[2 * k], rows[2 * k + 1])
                xysend[2 * side][c, k] = jnp.where(ex, high, low)
                xysend[2 * side + 1][c, k] = jnp.where(ex, low, high)


def join_kernel(shape, own, yrecv, xrecv, xyrecv, full, zsend, nat):
    sx, sy, sz = shape.size
    rows = shape.rows
    ex, ez = even("gx"), even("gz")
    flip = (lax.axis_index("gy") == 1) if shape.mirror else False

    gx, gy = lax.axis_index("gx"), lax.axis_index("gy")
    inner = (gx > 0).astype(jnp.float32), (gx < shape.n[0] - 1).astype(jnp.float32)

    def put(c, row, low, mid, high):
        if c == W_CH:
            low, high = low * inner[0], high * inner[1]
        nat[c, row, 0:HALO] = low
        nat[c, row, HALO : HALO + sx] = mid
        nat[c, row, HALO + sx :] = high

    for c in range(CH):
        turned = shape.mirror and c in (1, 4)
        for k in range(sy // 2):
            a, b = xrecv[0][c, k], xrecv[1][c, k]
            low, high = jnp.where(ex, b, a), jnp.where(ex, a, b)
            for h in range(2):
                part = slice(HALO * h, HALO * h + HALO)
                put(c, shape.own + 2 * k + h, low[part], own[c, 2 * k + h + 1], high[part])
        for side in range(2 if not shape.mirror else 1):
            for k in range(HALO // 2):
                if shape.mirror:
                    a, b = xyrecv[0][c, k], xyrecv[1][c, k]
                    mids = [yrecv[0][c, 2 * k + h] for h in range(2)]
                    if turned:
                        a, b = -a, -b
                        mids = [-t for t in mids]
                else:
                    lower = even("gy") if side else jnp.logical_not(even("gy"))
                    a, b = (jnp.where(lower, xyrecv[i][c, k], xyrecv[2 + i][c, k]) for i in range(2))
                    mids = [
                        jnp.where(lower, yrecv[0][c, 2 * k + h], yrecv[1][c, 2 * k + h])
                        for h in range(2)
                    ]
                    if c == W_CH:
                        near = gy < shape.n[1] - 1 if side else gy > 0
                        a, b, *mids = (t * near.astype(jnp.float32) for t in (a, b, *mids))
                low, high = jnp.where(ex, b, a), jnp.where(ex, a, b)
                for h in range(2):
                    part = slice(HALO * h, HALO * h + HALO)
                    d = 2 * k + h
                    if shape.mirror:
                        row = sy + d
                        if c == W_CH:
                            row = row - jnp.where(flip, 1, 0)
                    else:
                        row = d + side * (HALO + sy)
                    put(c, row, low[part], mids[h], high[part])
        if c == W_CH:
            nat[c, rows - 1] = jnp.zeros((sx + 2 * HALO, 128), jnp.float32)
    slot = lane_ids() // HALO
    for m in range(shape.erows):
        for t in range(2):
            up = jnp.zeros((8, 128), jnp.float32)
            down = jnp.zeros((8, 128), jnp.float32)
            for g in range(GROUPS):
                for c in range(CH):
                    tile = nat[c, g * shape.erows + m, pl.ds(t, 8, stride=2), :]
                    full[c, g * shape.erows + m, t] = tile
                    place = slot == (SPAN // HALO) * g + c
                    to = SPAN * g + HALO * c
                    up = jnp.where(place, roll_z(tile, to - (sz - HALO)), up)
                    down = jnp.where(place, roll_z(tile, to), down)
            zsend[0][m, t] = jnp.where(ez, up, down)
            zsend[1][m, t] = jnp.where(ez, down, up)


def load_row(ref, row, channels=range(3)):
    return [(ref[c, row, 0], ref[c, row, 1]) for c in channels]


def step_size(now, before, free):
    total = add2(now, before)
    total = add2(total, prev_x(total))
    return tuple(
        RELAX * f / (1.0 + 3.0 * (t + roll_z(t, 1))) for t, f in zip(total, free)
    )


def main_kernel(shape, full, v, prev, gsize, grad, stress, part):
    rows = shape.rows
    zero = jnp.zeros((8, 128), jnp.float32)
    for row in range(rows):
        for c in range(3):
            for t in range(2):
                tile = full[c, row, t]
                v[c, row + 1, t] = tile
                prev[c, row + 1, t] = tile
        now = load_row(full, row, (W_CH,))[0]
        before = load_row(full, row - 1, (W_CH,))[0] if row else (zero, zero)
        g = step_size(now, before, load_row(full, row, (FREE_CH,))[0])
        for t in range(2):
            gsize[row + 1, t] = g[t]
    for i in range(9):
        for t in range(2):
            stress[i, 0, t] = zero
    for c in range(3):
        for t in range(2):
            v[c, 0, t] = zero
            v[c, rows + 1, t] = zero
            prev[c, 0, t] = zero
    for t in range(2):
        gsize[0, t] = zero

    def put_gradient(row, value):
        for c in range(3):
            for kind in range(3):
                for t in range(2):
                    grad[3 * c + kind, row, t] = value[c][kind][t]

    def get9(ref, row):
        return [[(ref[3 * c + k, row, 0], ref[3 * c + k, row, 1]) for k in range(3)] for c in range(3)]

    def iteration(step, carry):
        omega = omega_at(step)
        first = 0 if shape.mirror else step
        last = rows - 1 - step
        put_gradient(first, gradient_row(load_row(v, first + 1)))
        put_gradient(first + 1, gradient_row(load_row(v, first + 2)))

        def body(j, carry):
            ahead = load_row(v, j + 3)
            low, high = get9(grad, j), get9(grad, j + 1)
            weight = load_row(full, j, (W_CH,))[0]
            before = get9(stress, j)
            held = [
                tuple((part[2 * c + i, j, 0], part[2 * c + i, j, 1]) for i in range(2))
                for c in range(3)
            ]
            old = load_row(v, j)
            oldest = load_row(prev, j)
            goal = load_row(full, max(j - 1, 0), (3, 4, 5))
            g = (gsize[j, 0], gsize[j, 1])

            after = gradient_row(ahead)
            now = stress_row(deform_rows(low, high), weight)
            parts = force_parts(now, before)
            new = update_row(held, old, goal, oldest, g, omega)

            put_gradient(j + 2, after)
            for c in range(3):
                for t in range(2):
                    for d in range(3):
                        stress[3 * c + d, j + 1, t] = now[c][d][t]
                    for i in range(2):
                        part[2 * c + i, j + 1, t] = parts[c][i][t]
                    prev[c, j, t] = old[c][t]
                    v[c, j, t] = new[c][t]
            return carry

        for j in range(first, last):
            body(j, 0)
        held = [
            tuple((part[2 * c + i, last, 0], part[2 * c + i, last, 1]) for i in range(2))
            for c in range(3)
        ]
        old = load_row(v, last)
        new = update_row(
            held,
            old,
            load_row(full, last - 1, (3, 4, 5)),
            load_row(prev, last),
            (gsize[last, 0], gsize[last, 1]),
            omega,
        )
        for c in range(3):
            for t in range(2):
                prev[c, last, t] = old[c][t]
                v[c, last, t] = new[c][t]
        return carry

    for step in range(ITERS):
        iteration(step, 0)


def edge_kernel(shape, full, main, zrecv0, zrecv1, out, v, prev, goal, gsize, stiff, tiles):
    sx, sy, sz = shape.size
    erows = shape.erows
    ez = even("gz")
    lane = lane_ids()
    within = lane % SPAN
    gz = lax.axis_index("gz")
    inner = (gz > 0).astype(jnp.float32), (gz < shape.n[2] - 1).astype(jnp.float32)
    half = SPAN // 2

    def window(c, m, t):
        value = jnp.zeros((8, 128), jnp.float32)
        for g in range(GROUPS):
            tile = full[c, g * erows + m, t]
            base = SPAN * g
            value = jnp.where(
                (lane >= base + HALO) & (lane < base + half), roll_z(tile, base + HALO), value
            )
            value = jnp.where(
                (lane >= base + half) & (lane < base + SPAN - HALO),
                roll_z(tile, base + SPAN - HALO - sz),
                value,
            )
        return value

    for m in range(erows):
        for t in range(2):
            a, b = zrecv0[m, t], zrecv1[m, t]
            low, high = jnp.where(ez, b, a), jnp.where(ez, a, b)

            def extended(c):
                below, above = roll_z(low, -HALO * c), roll_z(high, SPAN - HALO - HALO * c)
                if c == W_CH:
                    below, above = below * inner[0], above * inner[1]
                value = jnp.where(within < HALO, below, window(c, m, t))
                return jnp.where(within >= SPAN - HALO, above, value)

            for c in range(3):
                value = extended(c)
                v[c, m, t] = value
                prev[c, m, t] = value
                goal[c, m, t] = extended(3 + c)
            stiff[m, t] = extended(W_CH)
            gsize[m, t] = extended(FREE_CH)
    weights = [(stiff[m, 0], stiff[m, 1]) for m in range(erows)]
    behind = tuple(roll_z(t, SPAN) for t in weights[-1])
    for m in range(erows):
        g = step_size(weights[m], weights[m - 1] if m else behind, (gsize[m, 0], gsize[m, 1]))
        for t in range(2):
            gsize[m, t] = g[t]

    def iteration(step, carry):
        omega = omega_at(step)
        grads = [gradient_row(load_row(v, m)) for m in range(erows)]
        grads.append([[tuple(roll_z(t, -SPAN) for t in pair) for pair in row] for row in grads[0]])
        stress = [None] * erows
        for m in [erows - 1] + list(range(erows - 1)):
            stress[m] = stress_row(
                deform_rows(grads[m], grads[m + 1]), (stiff[m, 0], stiff[m, 1])
            )
        wrapped = [[tuple(roll_z(t, SPAN) for t in pair) for pair in row] for row in stress[-1]]
        for m in range(erows):
            parts = force_parts(stress[m], stress[m - 1] if m else wrapped)
            old = load_row(v, m)
            new = update_row(
                parts, old, load_row(goal, m), load_row(prev, m), (gsize[m, 0], gsize[m, 1]), omega
            )
            for c in range(3):
                for t in range(2):
                    prev[c, m, t] = old[c][t]
                    v[c, m, t] = new[c][t]
        return carry

    lax.fori_loop(0, ITERS, iteration, 0)
    flip = (lax.axis_index("gy") == 1) if shape.mirror else False
    for r in range(sy):
        row = shape.own + r
        g, m = divmod(row, erows)
        base = SPAN * g
        for c in range(3):
            factor = 1.0 / SCALE
            if shape.mirror and c == 1:
                factor = jnp.where(flip, -factor, factor).astype(jnp.float32)
            for t in range(2):
                edge = v[c, m, t]
                value = main[c, row + 1, t]
                value = jnp.where(lane < HALO, roll_z(edge, -(base + HALO)), value)
                value = jnp.where(
                    lane >= sz - HALO, roll_z(edge, sz - HALO - (base + SPAN - 2 * HALO)), value
                )
                tiles[pl.ds(t, 8, stride=2), :] = value * factor
            place = jnp.where(flip, sy - 1 - r, r) if shape.mirror else r
            out[c, pl.ds(place, sx, stride=sy), :] = tiles[HALO : HALO + sx]


def partner(size, parity, i):
    j = i + 1 if i % 2 == parity else i - 1
    return j if 0 <= j < size else None


def exchange(shape, parities):
    n = shape.n
    pairs = []
    for i in range(n[0]):
        for j in range(n[1]):
            for k in range(n[2]):
                here = (i, j, k)
                there = [
                    at if parity is None else partner(size, parity, at)
                    for at, size, parity in zip(here, n, parities)
                ]
                if None in there:
                    axis = 1 if parities[2] is not None else 2
                    other = partner(n[axis], 0, here[axis])
                    if other is None:
                        continue
                    there = list(here)
                    there[axis] = other
                pairs.append(
                    ((i * n[1] + j) * n[2] + k, (there[0] * n[1] + there[1]) * n[2] + there[2])
                )
    return pairs


def send(shape, value, *parities):
    return lax.ppermute(value, ("gx", "gy", "gz"), exchange(shape, parities))


def f32(*dims):
    return jax.ShapeDtypeStruct(dims, jnp.float32)


def in_hbm(value):
    return pltpu.with_memory_space_constraint(value, pltpu.MemorySpace.HBM)


def scratch(*dims):
    return pltpu.VMEM(dims, jnp.float32)


def call(body, outs, args, scratches=(), specs=None):
    return pl.pallas_call(
        body,
        out_shape=outs,
        in_specs=specs or [VM] * len(args),
        out_specs=jax.tree.map(lambda _: VM, outs),
        scratch_shapes=list(scratches),
        compiler_params=pltpu.CompilerParams(vmem_limit_bytes=40 * 1024 * 1024),
        cost_estimate=pl.CostEstimate(flops=2_000_000, bytes_accessed=100_000, transcendentals=0),
    )(*args)


def per_device(mesh, start_disp, inertial, material, pinned, stiffness):
    shape = Shape(mesh, material.shape)
    sx, sy, sz = shape.size
    sides = 1 if shape.mirror else 2
    rows, erows = shape.rows, shape.erows

    def prep(*refs):
        count = 3 + 3 * sides
        given, (own, *sent), held, sems = refs[:5], refs[5 : 5 + count], refs[5 + count : -1], refs[-1]
        copies = [pltpu.make_async_copy(a, b, sems.at[i]) for i, (a, b) in enumerate(zip(given, held))]
        for copy in copies:
            copy.start()
        for copy in copies:
            copy.wait()
        prep_kernel(shape, *held, own, sent[2 : 2 + sides], sent[:2], sent[2 + sides :])

    outs = [f32(CH, sy + 1, sx, sz)]
    outs += [f32(CH, sy // 2, 8, sz)] * 2 + [f32(CH, HALO, sx, sz)] * sides
    outs += [f32(CH, HALO // 2, 8, sz)] * (2 * sides)
    own, *sent = call(
        prep,
        outs,
        (
            in_hbm(start_disp.reshape(3, sx * sy, sz)),
            in_hbm(inertial.reshape(3, sx * sy, sz)),
            in_hbm(material.reshape(sx * sy, sz)),
            in_hbm(pinned.reshape(sx * sy, sz)),
            in_hbm(stiffness),
        ),
        [
            scratch(3, sx * sy, sz),
            scratch(3, sx * sy, sz),
            pltpu.VMEM((sx * sy, sz), jnp.int32),
            pltpu.VMEM((sx * sy, sz), jnp.int32),
            pltpu.SMEM((MATS,), jnp.float32),
            pltpu.SemaphoreType.DMA((5,)),
        ],
        [HBM] * 5,
    )
    recv = [send(shape, sent[p], p, None, None) for p in range(2)]
    recv += [send(shape, sent[2 + p], None, p, None) for p in range(sides)]
    recv += [
        send(shape, sent[2 + sides + 2 * q + p], p, q, None) for q in range(sides) for p in range(2)
    ]

    def join(own, *rest):
        x, rest = rest[:2], rest[2:]
        y, rest = rest[:sides], rest[sides:]
        xy, rest = rest[: 2 * sides], rest[2 * sides :]
        full, z0, z1, nat = rest
        join_kernel(shape, own, y, x, xy, full, (z0, z1), nat)

    full, z0, z1 = call(
        join,
        [f32(CH, rows, 2, 8, sz), f32(erows, 2, 8, sz), f32(erows, 2, 8, sz)],
        (own, *recv),
        [scratch(CH, rows, sx + 2 * HALO, sz)],
    )
    z0 = send(shape, z0, None, None, 0)
    z1 = send(shape, z1, None, None, 1)
    (main,) = call(
        functools.partial(main_kernel, shape),
        [f32(3, rows + 2, 2, 8, sz)],
        (full,),
        [
            scratch(3, rows + 2, 2, 8, sz),
            scratch(rows + 2, 2, 8, sz),
            scratch(9, rows + 2, 2, 8, sz),
            scratch(9, rows + 2, 2, 8, sz),
            scratch(6, rows + 2, 2, 8, sz),
        ],
    )
    (out,) = call(
        functools.partial(edge_kernel, shape),
        [f32(3, sx * sy, sz)],
        (full, main, z0, z1),
        [
            scratch(3, erows, 2, 8, sz),
            scratch(3, erows, 2, 8, sz),
            scratch(3, erows, 2, 8, sz),
            scratch(erows, 2, 8, sz),
            scratch(erows, 2, 8, sz),
            scratch(2 * 8, sz),
        ],
    )
    return out.reshape(3, sx, sy, sz)


def solution(mesh):
    placed = (
        P(None, "gx", "gy", "gz"),
        P(None, "gx", "gy", "gz"),
        P("gx", "gy", "gz"),
        P("gx", "gy", "gz"),
        P(),
    )
    return jax.shard_map(
        functools.partial(per_device, mesh),
        mesh=mesh,
        in_specs=placed,
        out_specs=P(None, "gx", "gy", "gz"),
        check_vma=False,
    )
```

```python
import functools
import math

import jax
import jax.numpy as jnp
from jax import lax
from jax.experimental import pallas as pl
from jax.experimental.pallas import tpu as pltpu
from jax.sharding import PartitionSpec as P

ITERS = 4
POLAR_STEPS = 6
MATS = 8
RELAX = 0.6
RADIUS = 0.9

HALO = ITERS
SCALE = 0.25 / math.sqrt(2.0)
UNIT = 1.0 / math.sqrt(2.0)
CH = 8
W_CH = 6
FREE_CH = 7
SHALLOW = (3, 4, 5, 7)
CARRY = (0, 1, 2, 3, 4, 5, 7)
LAYERS = tuple((c, d) for c in range(CH) for d in range(HALO - (c in SHALLOW)))
GROUPS = 4
SPAN = 32

VM = pl.BlockSpec(memory_space=pltpu.VMEM)
HBM = pl.BlockSpec(memory_space=pltpu.MemorySpace.HBM)


def omegas():
    values = [1.0]
    for step in range(1, ITERS):
        if step == 1:
            values.append(2.0 / (2.0 - RADIUS * RADIUS))
        else:
            values.append(4.0 / (4.0 - RADIUS * RADIUS * values[-1]))
    return values


def lane_ids():
    return lax.broadcasted_iota(jnp.int32, (8, 128), 1)


def sub_ids():
    return lax.broadcasted_iota(jnp.int32, (8, 128), 0)


def roll_z(value, amount):
    amount = amount % 128
    return value if amount == 0 else pltpu.roll(value, amount, 1)


def turn_x(value, amount):
    amount = amount % 8
    return value if amount == 0 else pltpu.roll(value, amount, 0)


def next_x(pair):
    return (pair[1], pltpu.roll(pair[0], 7, 0))


def prev_x(pair):
    return (pltpu.roll(pair[1], 1, 0), pair[0])


def add2(a, b):
    return tuple(x + y for x, y in zip(a, b))


def sub2(a, b):
    return tuple(x - y for x, y in zip(a, b))


def gradient_row(vrow):
    out = []
    for pair in vrow:
        ahead = tuple(roll_z(t, -1) for t in pair)
        sz = add2(pair, ahead)
        dz = sub2(ahead, pair)
        nsz = next_x(sz)
        out.append((add2(sz, nsz), sub2(nsz, sz), add2(dz, next_x(dz))))
    return out


def polar_stress(f, weight):
    def gram(z):
        return {
            (i, j): z[0][i] * z[0][j] + z[1][i] * z[1][j] + z[2][i] * z[2][j]
            for i in range(3)
            for j in range(i, 3)
        }

    def apply(z, diag, off):
        rows = []
        for c in range(3):
            row = []
            for d in range(3):
                value = z[c][d] * diag[d]
                for j in range(3):
                    if j != d:
                        value = value - z[c][j] * off[(min(j, d), max(j, d))]
                row.append(value)
            rows.append(row)
        return rows

    g = gram(f)
    trace = g[(0, 0)] + g[(1, 1)] + g[(2, 2)]
    s = jnp.minimum(lax.rsqrt(trace * (2.0 / 3.0)), 1.0)
    cube = s * s * s
    base = 1.5 * s
    z = apply(
        f,
        [base - cube * g[(i, i)] for i in range(3)],
        {key: cube * g[key] for key in ((0, 1), (0, 2), (1, 2))},
    )
    for _ in range(POLAR_STEPS - 1):
        g = gram(z)
        z = apply(z, [1.5 - g[(i, i)] for i in range(3)], g)
    return [[weight * (z[c][d] - f[c][d]) for d in range(3)] for c in range(3)]


def deform_rows(low, high):
    out = []
    for c in range(3):
        row = [
            add2(low[c][1], high[c][1]),
            sub2(high[c][0], low[c][0]),
            add2(low[c][2], high[c][2]),
        ]
        row[c] = tuple(t + UNIT for t in row[c])
        out.append(row)
    return out


def stress_row(f, weight):
    tiles = [
        polar_stress([[f[c][d][t] for d in range(3)] for c in range(3)], weight[t])
        for t in range(2)
    ]
    return [[(tiles[0][c][d], tiles[1][c][d]) for d in range(3)] for c in range(3)]


def force_parts(now, before):
    out = []
    for c in range(3):
        a = add2(now[c][0], before[c][0])
        b = sub2(now[c][1], before[c][1])
        e = add2(now[c][2], before[c][2])
        left = add2(add2(a, b), prev_x(sub2(b, a)))
        right = add2(e, prev_x(e))
        out.append((add2(left, right), sub2(left, right)))
    return out


def update_row(part, v, vin, prev, g, omega):
    new = []
    for c in range(3):
        row = []
        for t in range(2):
            force = part[c][0][t] + roll_z(part[c][1][t], 1)
            y = v[c][t] - g[t] * ((v[c][t] - vin[c][t]) + force)
            row.append(prev[c][t] + omega * (y - prev[c][t]))
        new.append(tuple(row))
    return new


class Shape:
    def __init__(self, mesh, size):
        self.n = tuple(mesh.shape[a] for a in ("gx", "gy", "gz"))
        self.size = size
        self.mirror = self.n[1] == 2
        self.own = 0 if self.mirror else HALO
        self.rows = size[1] + HALO * (1 if self.mirror else 2)
        self.erows = self.rows // GROUPS


def even(axis):
    return lax.rem(lax.axis_index(axis), 2) == 0


def pack_faces(first, second):
    upper = sub_ids() >= HALO
    low = jnp.where(upper, pltpu.roll(second, HALO, 0), first)
    high = jnp.where(upper, second, pltpu.roll(first, HALO, 0))
    return low, high


def prep_kernel(shape, start, inert, mat, pin, stiff, own, ysend, xsend, xysend):
    sx, sy, sz = shape.size
    gx, gy, gz = (lax.axis_index(a) for a in ("gx", "gy", "gz"))
    flip = (gy == 1) if shape.mirror else False
    sign = jnp.where(flip, -1.0, 1.0).astype(jnp.float32) if shape.mirror else jnp.float32(1.0)
    inside = (sub_ids() + gx * sx < shape.n[0] * sx - 1) & (
        lane_ids() + gz * sz < shape.n[2] * sz - 1
    )
    levels = [stiff[i] * (1.0 / 16.0) for i in range(MATS)]
    own[W_CH, sy] = jnp.zeros((8, 128), jnp.float32)
    for r in range(sy):
        at = pl.ds(r, sx, stride=sy)
        fixed = pin[at, :] > 0
        kind = mat[at, :]
        weight = jnp.zeros((8, 128), jnp.float32)
        for index in range(MATS):
            weight = jnp.where(kind == index, levels[index], weight)
        valid = inside & (r + gy * sy < shape.n[1] * sy - 1)
        weight = jnp.where(valid, weight, 0.0)
        node = jnp.where(flip, sy - 1 - r, r) + 1 if shape.mirror else r + 1
        cell = jnp.where(flip, sy - 2 - r, r) + 1 if shape.mirror else r + 1
        for c in range(3):
            factor = SCALE * sign if c == 1 else SCALE
            goal = inert[c, at, :] * factor
            own[c, node] = jnp.where(fixed, goal, start[c, at, :] * factor)
            own[3 + c, node] = goal
        own[W_CH, cell] = weight
        own[FREE_CH, node] = jnp.where(fixed, 0.0, 1.0)
    ex = even("gx")
    place = lax.rem(sub_ids(), HALO)
    for k in range(sy // 2):
        wlow, whigh = pack_faces(own[W_CH, 2 * k + 1], own[W_CH, 2 * k + 2])
        for index, c in enumerate(CARRY):
            low, high = pack_faces(own[c, 2 * k + 1], own[c, 2 * k + 2])
            if c in SHALLOW:
                q = SHALLOW.index(c)
                low = jnp.where(place == HALO - 1, turn_x(wlow, HALO - 1 - q), low)
                high = jnp.where(place == 0, turn_x(whigh, -q), high)
            xsend[0][index, k] = jnp.where(ex, high, low)
            xsend[1][index, k] = jnp.where(ex, low, high)
    for side in range(len(ysend)):
        rows = []
        for c, d in LAYERS:
            if shape.mirror:
                node = sy - 1 - d
                if c == W_CH:
                    node = node - jnp.where(flip, 1, 0)
            else:
                up = even("gy") if side == 0 else jnp.logical_not(even("gy"))
                node = jnp.where(up, sy - 1 - d, d)
            rows.append(own[c, node + 1])
            ysend[side][len(rows) - 1] = rows[-1]
        for k in range(len(rows) // 2):
            low, high = pack_faces(rows[2 * k], rows[2 * k + 1])
            xysend[2 * side][k] = jnp.where(ex, high, low)
            xysend[2 * side + 1][k] = jnp.where(ex, low, high)


def join_kernel(shape, own, yrecv, xrecv, xyrecv, full, zsend, nat):
    sx, sy, sz = shape.size
    rows = shape.rows
    ex, ez = even("gx"), even("gz")
    flip = (lax.axis_index("gy") == 1) if shape.mirror else False

    gx, gy = lax.axis_index("gx"), lax.axis_index("gy")
    inner = (gx > 0).astype(jnp.float32), (gx < shape.n[0] - 1).astype(jnp.float32)

    def put(c, row, low, mid, high):
        if c == W_CH:
            low, high = low * inner[0], high * inner[1]
        nat[c, row, 0:HALO] = low
        nat[c, row, HALO : HALO + sx] = mid
        nat[c, row, HALO + sx :] = high

    place = lax.rem(sub_ids(), HALO)
    for k in range(sy // 2):
        wlow = whigh = jnp.zeros((8, 128), jnp.float32)
        faces = {}
        for index, c in enumerate(CARRY):
            a, b = xrecv[0][index, k], xrecv[1][index, k]
            low, high = jnp.where(ex, b, a), jnp.where(ex, a, b)
            faces[c] = low, high
            if c in SHALLOW:
                q = SHALLOW.index(c)
                wlow = jnp.where(place == q, turn_x(low, q), wlow)
                whigh = jnp.where(place == q, turn_x(high, q + 1 - HALO), whigh)
        faces[W_CH] = wlow, whigh
        for c, (low, high) in faces.items():
            for h in range(2):
                part = slice(HALO * h, HALO * h + HALO)
                put(c, shape.own + 2 * k + h, low[part], own[c, 2 * k + h + 1], high[part])
    empty = jnp.zeros((sx + 2 * HALO, 128), jnp.float32)
    for c in SHALLOW:
        nat[c, rows - 1] = empty
        if not shape.mirror:
            nat[c, 0] = empty
    for side in range(1 if shape.mirror else 2):
        for k in range(len(LAYERS) // 2):
            near = LAYERS[2 * k : 2 * k + 2]
            if shape.mirror:
                a, b = xyrecv[0][k], xyrecv[1][k]
                mids = [yrecv[0][2 * k + h] for h in range(2)]
            else:
                lower = even("gy") if side else jnp.logical_not(even("gy"))
                a, b = (jnp.where(lower, xyrecv[i][k], xyrecv[2 + i][k]) for i in range(2))
                mids = [
                    jnp.where(lower, yrecv[0][2 * k + h], yrecv[1][2 * k + h]) for h in range(2)
                ]
            low, high = jnp.where(ex, b, a), jnp.where(ex, a, b)
            for h, (c, d) in enumerate(near):
                part = slice(HALO * h, HALO * h + HALO)
                values = [low[part], mids[h], high[part]]
                if shape.mirror:
                    row = sy + d
                    if c == W_CH:
                        row = row - jnp.where(flip, 1, 0)
                    if c in (1, 4):
                        values = [-t for t in values]
                else:
                    row = HALO + sy + d if side else HALO - 1 - d
                    if c == W_CH:
                        there = (gy < shape.n[1] - 1 if side else gy > 0).astype(jnp.float32)
                        values = [t * there for t in values]
                put(c, row, *values)
    nat[W_CH, rows - 1] = empty
    slot = lane_ids() // HALO
    for m in range(shape.erows):
        for t in range(2):
            up = jnp.zeros((8, 128), jnp.float32)
            down = jnp.zeros((8, 128), jnp.float32)
            for g in range(GROUPS):
                for c in range(CH):
                    tile = nat[c, g * shape.erows + m, pl.ds(t, 8, stride=2), :]
                    full[c, g * shape.erows + m, t] = tile
                    place = slot == (SPAN // HALO) * g + c
                    to = SPAN * g + HALO * c
                    up = jnp.where(place, roll_z(tile, to - (sz - HALO)), up)
                    down = jnp.where(place, roll_z(tile, to), down)
            zsend[0][m, t] = jnp.where(ez, up, down)
            zsend[1][m, t] = jnp.where(ez, down, up)


def load_row(ref, row, channels=range(3)):
    return [(ref[c, row, 0], ref[c, row, 1]) for c in channels]


def step_size(now, before, free):
    total = add2(now, before)
    total = add2(total, prev_x(total))
    return tuple(
        RELAX * f / (1.0 + 3.0 * (t + roll_z(t, 1))) for t, f in zip(total, free)
    )


def step_sizes(shape, full, gsize):
    zero = jnp.zeros((8, 128), jnp.float32)
    for row in range(shape.rows):
        now = load_row(full, row, (W_CH,))[0]
        before = load_row(full, row - 1, (W_CH,))[0] if row else (zero, zero)
        g = step_size(now, before, load_row(full, row, (FREE_CH,))[0])
        for t in range(2):
            gsize[row, t] = g[t]


def put9(ref, row, value):
    for c in range(3):
        for k in range(3):
            for t in range(2):
                ref[3 * c + k, row, t] = value[c][k][t]


def get9(ref, row):
    return [[(ref[3 * c + k, row, 0], ref[3 * c + k, row, 1]) for k in range(3)] for c in range(3)]


def main_steps(shape, full, gsize, old, oldest, write, grad, stress, part, step):
    omega = omegas()[step]
    first = 0 if shape.mirror else step
    last = shape.rows - 1 - step
    zero = jnp.zeros((8, 128), jnp.float32)

    def update(row):
        held = [
            tuple((part[2 * c + i, row, 0], part[2 * c + i, row, 1]) for i in range(2))
            for c in range(3)
        ]
        write(
            row,
            update_row(
                held,
                load_row(old, row),
                load_row(full, row, (3, 4, 5)),
                load_row(oldest, row),
                (gsize[row, 0], gsize[row, 1]),
                omega,
            ),
        )

    def head():
        for row in (first, first + 1):
            put9(grad, row, gradient_row(load_row(old, row)))

    def body(j):
        after = gradient_row(load_row(old, j + 2)) if j + 2 <= last else None
        now = stress_row(
            deform_rows(get9(grad, j), get9(grad, j + 1)), load_row(full, j, (W_CH,))[0]
        )
        before = get9(stress, j - 1) if j > first else [[(zero, zero)] * 3] * 3
        parts = force_parts(now, before)
        if j > first:
            update(j - 1)
        if after is not None:
            put9(grad, j + 2, after)
        put9(stress, j, now)
        for c in range(3):
            for t in range(2):
                for i in range(2):
                    part[2 * c + i, j, t] = parts[c][i][t]
        if j == last - 1:
            update(j)

    return head, [functools.partial(body, j) for j in range(first, last)]


def writer(ref):
    def write(row, new):
        for c in range(3):
            for t in range(2):
                ref[c, row, t] = new[c][t]

    return write


def main_kernel(shape, full, one, two, gsize, grad, stress, part):
    step_sizes(shape, full, gsize)
    for step, (old, oldest, new) in enumerate(((full, full, one), (one, full, two))):
        head, steps = main_steps(
            shape, full, gsize, old, oldest, writer(new), grad, stress, part, step
        )
        head()
        for run in steps:
            run()


def edge_parts(shape, full, zrecv, bufs, goal, gsize, stiff, grad, stress):
    sz = shape.size[2]
    erows = shape.erows
    ez = even("gz")
    lane = lane_ids()
    within = lane % SPAN
    half = SPAN // 2
    gz = lax.axis_index("gz")
    inner = (gz > 0).astype(jnp.float32), (gz < shape.n[2] - 1).astype(jnp.float32)

    def window(c, m, t):
        value = jnp.zeros((8, 128), jnp.float32)
        for g in range(GROUPS):
            tile = full[c, g * erows + m, t]
            base = SPAN * g
            value = jnp.where(
                (lane >= base + HALO) & (lane < base + half), roll_z(tile, base + HALO), value
            )
            value = jnp.where(
                (lane >= base + half) & (lane < base + SPAN - HALO),
                roll_z(tile, base + SPAN - HALO - sz),
                value,
            )
        return value

    def setup():
        for m in range(erows):
            for t in range(2):
                a, b = zrecv[0][m, t], zrecv[1][m, t]
                low, high = jnp.where(ez, b, a), jnp.where(ez, a, b)

                def extended(c):
                    below, above = roll_z(low, -HALO * c), roll_z(high, SPAN - HALO - HALO * c)
                    if c == W_CH:
                        below, above = below * inner[0], above * inner[1]
                    value = jnp.where(within < HALO, below, window(c, m, t))
                    return jnp.where(within >= SPAN - HALO, above, value)

                for c in range(3):
                    bufs[0][c, m, t] = extended(c)
                    goal[c, m, t] = extended(3 + c)
                stiff[m, t] = extended(W_CH)
                gsize[m, t] = extended(FREE_CH)
        weights = [(stiff[m, 0], stiff[m, 1]) for m in range(erows)]
        behind = tuple(roll_z(t, SPAN) for t in weights[-1])
        for m in range(erows):
            g = step_size(weights[m], weights[m - 1] if m else behind, (gsize[m, 0], gsize[m, 1]))
            for t in range(2):
                gsize[m, t] = g[t]

    def gradients(step):
        for m in range(erows):
            put9(grad, m, gradient_row(load_row(bufs[step], m)))
        turned = [tuple(roll_z(t, -SPAN) for t in pair) for pair in load_row(bufs[step], 0)]
        put9(grad, erows, gradient_row(turned))

    def stresses(m):
        now = stress_row(deform_rows(get9(grad, m), get9(grad, m + 1)), (stiff[m, 0], stiff[m, 1]))
        put9(stress, m + 1, now)
        if m == erows - 1:
            put9(stress, 0, [[tuple(roll_z(t, SPAN) for t in pair) for pair in row] for row in now])

    def updates(step, m):
        new = update_row(
            force_parts(get9(stress, m + 1), get9(stress, m)),
            load_row(bufs[step], m),
            load_row(goal, m),
            load_row(bufs[max(step - 1, 0)], m),
            (gsize[m, 0], gsize[m, 1]),
            omegas()[step],
        )
        writer(bufs[step + 1])(m, new)

    return setup, gradients, stresses, updates


def last_kernel(
    shape, full, one, two, gsize, zrecv0, zrecv1, out,
    three, grad, stress, part, bufs, egoal, egsize, estiff, egrad, estress, tiles,
):
    sx, sy, sz = shape.size
    erows = shape.erows
    lane = lane_ids()
    setup, gradients, stresses, updates = edge_parts(
        shape, full, (zrecv0, zrecv1), bufs, egoal, egsize, estiff, egrad, estress
    )
    flip = (lax.axis_index("gy") == 1) if shape.mirror else False
    turned = jnp.where(flip, -1.0 / SCALE, 1.0 / SCALE).astype(jnp.float32) if shape.mirror else 1.0 / SCALE

    def finish(row, new):
        r = row - shape.own
        if not 0 <= r < sy:
            return
        g, m = divmod(row, erows)
        base = SPAN * g
        place = jnp.where(flip, sy - 1 - r, r) if shape.mirror else r
        for c in range(3):
            for t in range(2):
                edge = bufs[ITERS][c, m, t]
                value = jnp.where(lane < HALO, roll_z(edge, -(base + HALO)), new[c][t])
                value = jnp.where(
                    lane >= sz - HALO, roll_z(edge, sz - HALO - (base + SPAN - 2 * HALO)), value
                )
                tiles[r, c, pl.ds(t, 8, stride=2), :] = value * (turned if c == 1 else 1.0 / SCALE)
            out[c, pl.ds(place, sx, stride=sy), :] = tiles[r, c, HALO : HALO + sx]

    edge = [setup]
    for step in range(ITERS):
        edge.append(functools.partial(gradients, step))
        order = [erows - 1] + list(range(erows - 1))
        edge.append(lambda order=order: [stresses(m) for m in order])
        edge.append(lambda step=step: [updates(step, m) for m in range(erows)])
    head, steps = main_steps(
        shape, full, gsize, two, one, writer(three), grad, stress, part, 2
    )
    head()
    total = len(steps)
    given = 0
    for index, run in enumerate(steps):
        upto = -(-len(edge) * (index + 1) // total)
        for work in edge[given:upto]:
            work()
        given = max(given, upto)
        run()
    head, steps = main_steps(shape, full, gsize, three, two, finish, grad, stress, part, 3)
    head()
    for run in steps:
        run()


def partner(size, parity, i):
    j = i + 1 if i % 2 == parity else i - 1
    return j if 0 <= j < size else None


def exchange(shape, parities):
    n = shape.n
    pairs = []
    for i in range(n[0]):
        for j in range(n[1]):
            for k in range(n[2]):
                here = (i, j, k)
                there = [
                    at if parity is None else partner(size, parity, at)
                    for at, size, parity in zip(here, n, parities)
                ]
                if None in there:
                    axis = 1 if parities[2] is not None else 2
                    other = partner(n[axis], 0, here[axis])
                    if other is None:
                        continue
                    there = list(here)
                    there[axis] = other
                pairs.append(
                    ((i * n[1] + j) * n[2] + k, (there[0] * n[1] + there[1]) * n[2] + there[2])
                )
    return pairs


def send(shape, value, *parities):
    return lax.ppermute(value, ("gx", "gy", "gz"), exchange(shape, parities))


def f32(*dims):
    return jax.ShapeDtypeStruct(dims, jnp.float32)


def in_hbm(value):
    return pltpu.with_memory_space_constraint(value, pltpu.MemorySpace.HBM)


def scratch(*dims):
    return pltpu.VMEM(dims, jnp.float32)


def call(body, outs, args, scratches=(), specs=None):
    return pl.pallas_call(
        body,
        out_shape=outs,
        in_specs=specs or [VM] * len(args),
        out_specs=jax.tree.map(lambda _: VM, outs),
        scratch_shapes=list(scratches),
        compiler_params=pltpu.CompilerParams(vmem_limit_bytes=40 * 1024 * 1024),
        cost_estimate=pl.CostEstimate(flops=2_000_000, bytes_accessed=100_000, transcendentals=0),
    )(*args)


def per_device(mesh, start_disp, inertial, material, pinned, stiffness):
    shape = Shape(mesh, material.shape)
    sx, sy, sz = shape.size
    sides = 1 if shape.mirror else 2
    rows, erows = shape.rows, shape.erows

    def prep(*refs):
        count = 3 + 3 * sides
        given, (own, *sent), held, sems = refs[:5], refs[5 : 5 + count], refs[5 + count : -1], refs[-1]
        copies = [pltpu.make_async_copy(a, b, sems.at[i]) for i, (a, b) in enumerate(zip(given, held))]
        for copy in copies:
            copy.start()
        for copy in copies:
            copy.wait()
        prep_kernel(shape, *held, own, sent[2 : 2 + sides], sent[:2], sent[2 + sides :])

    outs = [f32(CH, sy + 1, sx, sz)]
    outs += [f32(len(CARRY), sy // 2, 8, sz)] * 2 + [f32(len(LAYERS), sx, sz)] * sides
    outs += [f32(len(LAYERS) // 2, 8, sz)] * (2 * sides)
    own, *sent = call(
        prep,
        outs,
        (
            in_hbm(start_disp.reshape(3, sx * sy, sz)),
            in_hbm(inertial.reshape(3, sx * sy, sz)),
            in_hbm(material.reshape(sx * sy, sz)),
            in_hbm(pinned.reshape(sx * sy, sz)),
            in_hbm(stiffness),
        ),
        [
            scratch(3, sx * sy, sz),
            scratch(3, sx * sy, sz),
            pltpu.VMEM((sx * sy, sz), jnp.int32),
            pltpu.VMEM((sx * sy, sz), jnp.int32),
            pltpu.SMEM((MATS,), jnp.float32),
            pltpu.SemaphoreType.DMA((5,)),
        ],
        [HBM] * 5,
    )
    recv = [send(shape, sent[p], p, None, None) for p in range(2)]
    recv += [send(shape, sent[2 + p], None, p, None) for p in range(sides)]
    recv += [
        send(shape, sent[2 + sides + 2 * q + p], p, q, None) for q in range(sides) for p in range(2)
    ]

    def join(own, *rest):
        x, rest = rest[:2], rest[2:]
        y, rest = rest[:sides], rest[sides:]
        xy, rest = rest[: 2 * sides], rest[2 * sides :]
        full, z0, z1, nat = rest
        join_kernel(shape, own, y, x, xy, full, (z0, z1), nat)

    full, z0, z1 = call(
        join,
        [f32(CH, rows, 2, 8, sz), f32(erows, 2, 8, sz), f32(erows, 2, 8, sz)],
        (own, *recv),
        [scratch(CH, rows, sx + 2 * HALO, sz)],
    )
    z0 = send(shape, z0, None, None, 0)
    z1 = send(shape, z1, None, None, 1)
    one, two, gsize = call(
        functools.partial(main_kernel, shape),
        [f32(3, rows, 2, 8, sz), f32(3, rows, 2, 8, sz), f32(rows, 2, 8, sz)],
        (full,),
        [scratch(count, rows, 2, 8, sz) for count in (9, 9, 6)],
    )

    def last(*refs):
        ends = 11 + ITERS + 1
        last_kernel(shape, *refs[:11], refs[11:ends], *refs[ends:])

    (out,) = call(
        last,
        [f32(3, sx * sy, sz)],
        (full, one, two, gsize, z0, z1),
        [scratch(3, rows, 2, 8, sz)]
        + [scratch(count, rows, 2, 8, sz) for count in (9, 9, 6)]
        + [scratch(3, erows, 2, 8, sz) for _ in range(ITERS + 2)]
        + [scratch(erows, 2, 8, sz)] * 2
        + [scratch(9, erows + 1, 2, 8, sz)] * 2
        + [scratch(sy, 3, 2 * 8, sz)],
    )
    return out.reshape(3, sx, sy, sz)


def solution(mesh):
    placed = (
        P(None, "gx", "gy", "gz"),
        P(None, "gx", "gy", "gz"),
        P("gx", "gy", "gz"),
        P("gx", "gy", "gz"),
        P(),
    )
    return jax.shard_map(
        functools.partial(per_device, mesh),
        mesh=mesh,
        in_specs=placed,
        out_specs=P(None, "gx", "gy", "gz"),
        check_vma=False,
    )
```

```python
import functools
import math

import jax
import jax.numpy as jnp
from jax import lax
from jax.experimental import pallas as pl
from jax.experimental.pallas import tpu as pltpu
from jax.sharding import PartitionSpec as P

ITERS = 4
POLAR_STEPS = 6
MATS = 8
RELAX = 0.6
RADIUS = 0.9

HALO = ITERS
SCALE = 0.25 / math.sqrt(2.0)
UNIT = 1.0 / math.sqrt(2.0)
CH = 8
W_CH = 6
FREE_CH = 7
SHALLOW = (3, 4, 5, 7)
CARRY = (0, 1, 2, 3, 4, 5, 7)
LAYERS = tuple((c, d) for c in range(CH) for d in range(HALO - (c in SHALLOW)))
GROUPS = 4
SPAN = 32

VM = pl.BlockSpec(memory_space=pltpu.VMEM)
HBM = pl.BlockSpec(memory_space=pltpu.MemorySpace.HBM)


def omegas():
    values = [1.0]
    for step in range(1, ITERS):
        if step == 1:
            values.append(2.0 / (2.0 - RADIUS * RADIUS))
        else:
            values.append(4.0 / (4.0 - RADIUS * RADIUS * values[-1]))
    return values


def lane_ids():
    return lax.broadcasted_iota(jnp.int32, (8, 128), 1)


def sub_ids():
    return lax.broadcasted_iota(jnp.int32, (8, 128), 0)


def roll_z(value, amount):
    amount = amount % 128
    return value if amount == 0 else pltpu.roll(value, amount, 1)


def turn_x(value, amount):
    amount = amount % 8
    return value if amount == 0 else pltpu.roll(value, amount, 0)


def next_x(pair):
    return (pair[1], pltpu.roll(pair[0], 7, 0))


def prev_x(pair):
    return (pltpu.roll(pair[1], 1, 0), pair[0])


def add2(a, b):
    return tuple(x + y for x, y in zip(a, b))


def sub2(a, b):
    return tuple(x - y for x, y in zip(a, b))


def gradient_row(vrow):
    out = []
    for pair in vrow:
        ahead = tuple(roll_z(t, -1) for t in pair)
        sz = add2(pair, ahead)
        dz = sub2(ahead, pair)
        nsz = next_x(sz)
        out.append((add2(sz, nsz), sub2(nsz, sz), add2(dz, next_x(dz))))
    return out


THIRD_ANGLE = (
    0.866025405599564,
    0.16666637114459312,
    -0.04810444145461756,
    0.02460429680494765,
    -0.01510727520943827,
    0.009383330672620772,
    -0.004929691292929874,
    0.0017648569477158788,
    -0.0003028542202729437,
)


def polar_stress(f, weight):
    xx, yy, zz = (f[0][i] * f[0][i] + f[1][i] * f[1][i] + f[2][i] * f[2][i] for i in range(3))
    xy, xz, yz = (
        f[0][i] * f[0][j] + f[1][i] * f[1][j] + f[2][i] * f[2][j]
        for i, j in ((0, 1), (0, 2), (1, 2))
    )
    trace = xx + yy + zz
    s = jnp.minimum(lax.rsqrt(trace * (2.0 / 3.0)), 1.0)
    s2 = s * s
    mean = trace * (1.0 / 3.0)
    xx, yy, zz = xx - mean, yy - mean, zz - mean
    xy2, xz2, yz2 = xy * xy, xz * xz, yz * yz
    xyz = xy * xz
    sx2, sy2, sz2 = xx * xx + xy2, yy * yy + yz2, zz * zz + xz2
    spread = (sx2 + sy2 + sz2 + (xy2 + yz2 + xz2)) * (1.0 / 6.0)
    inverse = lax.rsqrt(jnp.maximum(spread, 1e-24))
    cross = xyz * yz
    det = xx * (yy * zz - yz2) + (cross + cross) - yy * xz2 - zz * xy2
    ratio = (det * 0.5) * inverse * inverse * inverse
    radius = spread * inverse * s2
    turn = jnp.minimum(jnp.abs(ratio), 1.0)
    c = jnp.full_like(turn, THIRD_ANGLE[-1])
    for value in THIRD_ANGLE[-2::-1]:
        c = c * turn + value
    square = jnp.maximum(1.0 - c * c, 1e-20)
    apart = radius * math.sqrt(3.0) * (square * lax.rsqrt(square))
    half = jnp.where(ratio < 0.0, -radius, radius) * c
    near = (apart - half, -apart - half, half + half)
    center = mean * s2
    level = [v + center for v in near]
    slope = None
    for step in range(POLAR_STEPS):
        m = [1.5 - v for v in level]
        if step == 0:
            q, dq = list(m), -1.0
        else:
            dq = dq * m[0] - q[1] * slope
            q = [a * b for a, b in zip(q, m)]
        if step < POLAR_STEPS - 1:
            m2 = [v * v for v in m]
            growth = m2[0] - level[1] * (m[0] + m[1])
            slope = growth if slope is None else slope * growth
            level = [a * b for a, b in zip(level, m2)]
    gap1, gap2 = near[0] - near[2], near[1] - near[2]
    inv = pl.reciprocal(jnp.maximum(gap1 * gap2, 1e-30))
    bend = (dq - (q[1] - q[2]) * (gap1 * inv)) * (gap2 * inv)
    k0 = (q[0] - dq * near[0] + bend * (near[0] * near[1])) * s
    k1 = (dq - bend * (near[0] + near[1])) * (s * s2)
    k2 = bend * (s * (s2 * s2))
    diag = (
        k0 + k1 * xx + k2 * (sx2 + xz2),
        k0 + k1 * yy + k2 * (sy2 + xy2),
        k0 + k1 * zz + k2 * (sz2 + yz2),
    )
    off = {
        (0, 1): k1 * xy + k2 * (xy * (xx + yy) + xz * yz),
        (0, 2): k1 * xz + k2 * (xz * (xx + zz) + xy * yz),
        (1, 2): k1 * yz + k2 * (yz * (yy + zz) + xyz),
    }
    diag = tuple(v - 1.0 for v in diag)
    out = []
    for c in range(3):
        row = []
        for d in range(3):
            value = f[c][d] * diag[d]
            for j in range(3):
                if j != d:
                    value = value + f[c][j] * off[(min(j, d), max(j, d))]
            row.append(weight * value)
        out.append(row)
    return out


def deform_rows(low, high):
    out = []
    for c in range(3):
        row = [
            add2(low[c][1], high[c][1]),
            sub2(high[c][0], low[c][0]),
            add2(low[c][2], high[c][2]),
        ]
        row[c] = tuple(t + UNIT for t in row[c])
        out.append(row)
    return out


def stress_row(f, weight):
    tiles = [
        polar_stress([[f[c][d][t] for d in range(3)] for c in range(3)], weight[t])
        for t in range(2)
    ]
    return [[(tiles[0][c][d], tiles[1][c][d]) for d in range(3)] for c in range(3)]


def force_parts(now, before):
    out = []
    for c in range(3):
        a = add2(now[c][0], before[c][0])
        b = sub2(now[c][1], before[c][1])
        e = add2(now[c][2], before[c][2])
        left = add2(add2(a, b), prev_x(sub2(b, a)))
        right = add2(e, prev_x(e))
        out.append((add2(left, right), sub2(left, right)))
    return out


def update_row(part, v, vin, prev, g, omega):
    new = []
    for c in range(3):
        row = []
        for t in range(2):
            force = part[c][0][t] + roll_z(part[c][1][t], 1)
            y = v[c][t] - g[t] * ((v[c][t] - vin[c][t]) + force)
            row.append(prev[c][t] + omega * (y - prev[c][t]))
        new.append(tuple(row))
    return new


class Shape:
    def __init__(self, mesh, size):
        self.n = tuple(mesh.shape[a] for a in ("gx", "gy", "gz"))
        self.size = size
        self.mirror = self.n[1] == 2
        self.own = 0 if self.mirror else HALO
        self.rows = size[1] + HALO * (1 if self.mirror else 2)
        self.erows = self.rows // GROUPS


def even(axis):
    return lax.rem(lax.axis_index(axis), 2) == 0


def pack_faces(first, second):
    upper = sub_ids() >= HALO
    low = jnp.where(upper, pltpu.roll(second, HALO, 0), first)
    high = jnp.where(upper, second, pltpu.roll(first, HALO, 0))
    return low, high


def prep_kernel(shape, start, inert, mat, pin, stiff, own, ysend, xsend, xysend):
    sx, sy, sz = shape.size
    gx, gy, gz = (lax.axis_index(a) for a in ("gx", "gy", "gz"))
    flip = (gy == 1) if shape.mirror else False
    sign = jnp.where(flip, -1.0, 1.0).astype(jnp.float32) if shape.mirror else jnp.float32(1.0)
    inside = (sub_ids() + gx * sx < shape.n[0] * sx - 1) & (
        lane_ids() + gz * sz < shape.n[2] * sz - 1
    )
    levels = [stiff[i] * (1.0 / 16.0) for i in range(MATS)]
    own[W_CH, sy] = jnp.zeros((8, 128), jnp.float32)
    for r in range(sy):
        at = pl.ds(r, sx, stride=sy)
        fixed = pin[at, :] > 0
        kind = mat[at, :]
        weight = jnp.zeros((8, 128), jnp.float32)
        for index in range(MATS):
            weight = jnp.where(kind == index, levels[index], weight)
        valid = inside & (r + gy * sy < shape.n[1] * sy - 1)
        weight = jnp.where(valid, weight, 0.0)
        node = jnp.where(flip, sy - 1 - r, r) + 1 if shape.mirror else r + 1
        cell = jnp.where(flip, sy - 2 - r, r) + 1 if shape.mirror else r + 1
        for c in range(3):
            factor = SCALE * sign if c == 1 else SCALE
            goal = inert[c, at, :] * factor
            own[c, node] = jnp.where(fixed, goal, start[c, at, :] * factor)
            own[3 + c, node] = goal
        own[W_CH, cell] = weight
        own[FREE_CH, node] = jnp.where(fixed, 0.0, 1.0)
    ex = even("gx")
    place = lax.rem(sub_ids(), HALO)
    for k in range(sy // 2):
        wlow, whigh = pack_faces(own[W_CH, 2 * k + 1], own[W_CH, 2 * k + 2])
        for index, c in enumerate(CARRY):
            low, high = pack_faces(own[c, 2 * k + 1], own[c, 2 * k + 2])
            if c in SHALLOW:
                q = SHALLOW.index(c)
                low = jnp.where(place == HALO - 1, turn_x(wlow, HALO - 1 - q), low)
                high = jnp.where(place == 0, turn_x(whigh, -q), high)
            xsend[0][index, k] = jnp.where(ex, high, low)
            xsend[1][index, k] = jnp.where(ex, low, high)
    for side in range(len(ysend)):
        rows = []
        for c, d in LAYERS:
            if shape.mirror:
                node = sy - 1 - d
                if c == W_CH:
                    node = node - jnp.where(flip, 1, 0)
            else:
                up = even("gy") if side == 0 else jnp.logical_not(even("gy"))
                node = jnp.where(up, sy - 1 - d, d)
            rows.append(own[c, node + 1])
            ysend[side][len(rows) - 1] = rows[-1]
        for k in range(len(rows) // 2):
            low, high = pack_faces(rows[2 * k], rows[2 * k + 1])
            xysend[2 * side][k] = jnp.where(ex, high, low)
            xysend[2 * side + 1][k] = jnp.where(ex, low, high)


def join_kernel(shape, own, yrecv, xrecv, xyrecv, full, zsend, nat):
    sx, sy, sz = shape.size
    rows = shape.rows
    ex, ez = even("gx"), even("gz")
    flip = (lax.axis_index("gy") == 1) if shape.mirror else False

    gx, gy = lax.axis_index("gx"), lax.axis_index("gy")
    inner = (gx > 0).astype(jnp.float32), (gx < shape.n[0] - 1).astype(jnp.float32)

    def put(c, row, low, mid, high):
        if c == W_CH:
            low, high = low * inner[0], high * inner[1]
        nat[c, row, 0:HALO] = low
        nat[c, row, HALO : HALO + sx] = mid
        nat[c, row, HALO + sx :] = high

    place = lax.rem(sub_ids(), HALO)
    for k in range(sy // 2):
        wlow = whigh = jnp.zeros((8, 128), jnp.float32)
        faces = {}
        for index, c in enumerate(CARRY):
            a, b = xrecv[0][index, k], xrecv[1][index, k]
            low, high = jnp.where(ex, b, a), jnp.where(ex, a, b)
            faces[c] = low, high
            if c in SHALLOW:
                q = SHALLOW.index(c)
                wlow = jnp.where(place == q, turn_x(low, q), wlow)
                whigh = jnp.where(place == q, turn_x(high, q + 1 - HALO), whigh)
        faces[W_CH] = wlow, whigh
        for c, (low, high) in faces.items():
            for h in range(2):
                part = slice(HALO * h, HALO * h + HALO)
                put(c, shape.own + 2 * k + h, low[part], own[c, 2 * k + h + 1], high[part])
    empty = jnp.zeros((sx + 2 * HALO, 128), jnp.float32)
    for c in SHALLOW:
        nat[c, rows - 1] = empty
        if not shape.mirror:
            nat[c, 0] = empty
    for side in range(1 if shape.mirror else 2):
        for k in range(len(LAYERS) // 2):
            near = LAYERS[2 * k : 2 * k + 2]
            if shape.mirror:
                a, b = xyrecv[0][k], xyrecv[1][k]
                mids = [yrecv[0][2 * k + h] for h in range(2)]
            else:
                lower = even("gy") if side else jnp.logical_not(even("gy"))
                a, b = (jnp.where(lower, xyrecv[i][k], xyrecv[2 + i][k]) for i in range(2))
                mids = [
                    jnp.where(lower, yrecv[0][2 * k + h], yrecv[1][2 * k + h]) for h in range(2)
                ]
            low, high = jnp.where(ex, b, a), jnp.where(ex, a, b)
            for h, (c, d) in enumerate(near):
                part = slice(HALO * h, HALO * h + HALO)
                values = [low[part], mids[h], high[part]]
                if shape.mirror:
                    row = sy + d
                    if c == W_CH:
                        row = row - jnp.where(flip, 1, 0)
                    if c in (1, 4):
                        values = [-t for t in values]
                else:
                    row = HALO + sy + d if side else HALO - 1 - d
                    if c == W_CH:
                        there = (gy < shape.n[1] - 1 if side else gy > 0).astype(jnp.float32)
                        values = [t * there for t in values]
                put(c, row, *values)
    nat[W_CH, rows - 1] = empty
    slot = lane_ids() // HALO
    for m in range(shape.erows):
        for t in range(2):
            up = jnp.zeros((8, 128), jnp.float32)
            down = jnp.zeros((8, 128), jnp.float32)
            for g in range(GROUPS):
                for c in range(CH):
                    tile = nat[c, g * shape.erows + m, pl.ds(t, 8, stride=2), :]
                    full[c, g * shape.erows + m, t] = tile
                    place = slot == (SPAN // HALO) * g + c
                    to = SPAN * g + HALO * c
                    up = jnp.where(place, roll_z(tile, to - (sz - HALO)), up)
                    down = jnp.where(place, roll_z(tile, to), down)
            zsend[0][m, t] = jnp.where(ez, up, down)
            zsend[1][m, t] = jnp.where(ez, down, up)


def load_row(ref, row, channels=range(3)):
    return [(ref[c, row, 0], ref[c, row, 1]) for c in channels]


def step_size(now, before, free):
    total = add2(now, before)
    total = add2(total, prev_x(total))
    return tuple(
        RELAX * f / (1.0 + 3.0 * (t + roll_z(t, 1))) for t, f in zip(total, free)
    )


def step_sizes(shape, full, gsize):
    zero = jnp.zeros((8, 128), jnp.float32)
    for row in range(shape.rows):
        now = load_row(full, row, (W_CH,))[0]
        before = load_row(full, row - 1, (W_CH,))[0] if row else (zero, zero)
        g = step_size(now, before, load_row(full, row, (FREE_CH,))[0])
        for t in range(2):
            gsize[row, t] = g[t]


def put9(ref, row, value):
    for c in range(3):
        for k in range(3):
            for t in range(2):
                ref[3 * c + k, row, t] = value[c][k][t]


def get9(ref, row):
    return [[(ref[3 * c + k, row, 0], ref[3 * c + k, row, 1]) for k in range(3)] for c in range(3)]


def main_steps(shape, full, gsize, old, oldest, write, grad, stress, part, step):
    omega = omegas()[step]
    first = 0 if shape.mirror else step
    last = shape.rows - 1 - step
    zero = jnp.zeros((8, 128), jnp.float32)

    def update(row):
        held = [
            tuple((part[2 * c + i, row, 0], part[2 * c + i, row, 1]) for i in range(2))
            for c in range(3)
        ]
        write(
            row,
            update_row(
                held,
                load_row(old, row),
                load_row(full, row, (3, 4, 5)),
                load_row(oldest, row),
                (gsize[row, 0], gsize[row, 1]),
                omega,
            ),
        )

    def head():
        for row in (first, first + 1):
            put9(grad, row, gradient_row(load_row(old, row)))

    def body(j):
        after = gradient_row(load_row(old, j + 2)) if j + 2 <= last else None
        now = stress_row(
            deform_rows(get9(grad, j), get9(grad, j + 1)), load_row(full, j, (W_CH,))[0]
        )
        before = get9(stress, j - 1) if j > first else [[(zero, zero)] * 3] * 3
        parts = force_parts(now, before)
        if j > first:
            update(j - 1)
        if after is not None:
            put9(grad, j + 2, after)
        put9(stress, j, now)
        for c in range(3):
            for t in range(2):
                for i in range(2):
                    part[2 * c + i, j, t] = parts[c][i][t]
        if j == last - 1:
            update(j)

    return head, [functools.partial(body, j) for j in range(first, last)]


def writer(ref):
    def write(row, new):
        for c in range(3):
            for t in range(2):
                ref[c, row, t] = new[c][t]

    return write


def main_kernel(shape, full, one, two, gsize, grad, stress, part):
    step_sizes(shape, full, gsize)
    for step, (old, oldest, new) in enumerate(((full, full, one), (one, full, two))):
        head, steps = main_steps(
            shape, full, gsize, old, oldest, writer(new), grad, stress, part, step
        )
        head()
        for run in steps:
            run()


def edge_parts(shape, full, zrecv, bufs, goal, gsize, stiff, grad, stress):
    sz = shape.size[2]
    erows = shape.erows
    ez = even("gz")
    lane = lane_ids()
    within = lane % SPAN
    half = SPAN // 2
    gz = lax.axis_index("gz")
    inner = (gz > 0).astype(jnp.float32), (gz < shape.n[2] - 1).astype(jnp.float32)

    def window(c, m, t):
        value = jnp.zeros((8, 128), jnp.float32)
        for g in range(GROUPS):
            tile = full[c, g * erows + m, t]
            base = SPAN * g
            value = jnp.where(
                (lane >= base + HALO) & (lane < base + half), roll_z(tile, base + HALO), value
            )
            value = jnp.where(
                (lane >= base + half) & (lane < base + SPAN - HALO),
                roll_z(tile, base + SPAN - HALO - sz),
                value,
            )
        return value

    def setup():
        for m in range(erows):
            for t in range(2):
                a, b = zrecv[0][m, t], zrecv[1][m, t]
                low, high = jnp.where(ez, b, a), jnp.where(ez, a, b)

                def extended(c):
                    below, above = roll_z(low, -HALO * c), roll_z(high, SPAN - HALO - HALO * c)
                    if c == W_CH:
                        below, above = below * inner[0], above * inner[1]
                    value = jnp.where(within < HALO, below, window(c, m, t))
                    return jnp.where(within >= SPAN - HALO, above, value)

                for c in range(3):
                    bufs[0][c, m, t] = extended(c)
                    goal[c, m, t] = extended(3 + c)
                stiff[m, t] = extended(W_CH)
                gsize[m, t] = extended(FREE_CH)
        weights = [(stiff[m, 0], stiff[m, 1]) for m in range(erows)]
        behind = tuple(roll_z(t, SPAN) for t in weights[-1])
        for m in range(erows):
            g = step_size(weights[m], weights[m - 1] if m else behind, (gsize[m, 0], gsize[m, 1]))
            for t in range(2):
                gsize[m, t] = g[t]

    def gradients(step):
        for m in range(erows):
            put9(grad, m, gradient_row(load_row(bufs[step], m)))
        turned = [tuple(roll_z(t, -SPAN) for t in pair) for pair in load_row(bufs[step], 0)]
        put9(grad, erows, gradient_row(turned))

    def stresses(m):
        now = stress_row(deform_rows(get9(grad, m), get9(grad, m + 1)), (stiff[m, 0], stiff[m, 1]))
        put9(stress, m + 1, now)
        if m == erows - 1:
            put9(stress, 0, [[tuple(roll_z(t, SPAN) for t in pair) for pair in row] for row in now])

    def updates(step, m):
        new = update_row(
            force_parts(get9(stress, m + 1), get9(stress, m)),
            load_row(bufs[step], m),
            load_row(goal, m),
            load_row(bufs[max(step - 1, 0)], m),
            (gsize[m, 0], gsize[m, 1]),
            omegas()[step],
        )
        writer(bufs[step + 1])(m, new)

    return setup, gradients, stresses, updates


def last_kernel(
    shape, full, one, two, gsize, zrecv0, zrecv1, out,
    three, grad, stress, part, bufs, egoal, egsize, estiff, egrad, estress, tiles,
):
    sx, sy, sz = shape.size
    erows = shape.erows
    lane = lane_ids()
    setup, gradients, stresses, updates = edge_parts(
        shape, full, (zrecv0, zrecv1), bufs, egoal, egsize, estiff, egrad, estress
    )
    flip = (lax.axis_index("gy") == 1) if shape.mirror else False
    turned = jnp.where(flip, -1.0 / SCALE, 1.0 / SCALE).astype(jnp.float32) if shape.mirror else 1.0 / SCALE

    def finish(row, new):
        r = row - shape.own
        if not 0 <= r < sy:
            return
        g, m = divmod(row, erows)
        base = SPAN * g
        place = jnp.where(flip, sy - 1 - r, r) if shape.mirror else r
        for c in range(3):
            for t in range(2):
                edge = bufs[ITERS][c, m, t]
                value = jnp.where(lane < HALO, roll_z(edge, -(base + HALO)), new[c][t])
                value = jnp.where(
                    lane >= sz - HALO, roll_z(edge, sz - HALO - (base + SPAN - 2 * HALO)), value
                )
                tiles[r, c, pl.ds(t, 8, stride=2), :] = value * (turned if c == 1 else 1.0 / SCALE)
            out[c, pl.ds(place, sx, stride=sy), :] = tiles[r, c, HALO : HALO + sx]

    edge = [setup]
    for step in range(ITERS):
        edge.append(functools.partial(gradients, step))
        order = [erows - 1] + list(range(erows - 1))
        edge.append(lambda order=order: [stresses(m) for m in order])
        edge.append(lambda step=step: [updates(step, m) for m in range(erows)])
    head, steps = main_steps(
        shape, full, gsize, two, one, writer(three), grad, stress, part, 2
    )
    head()
    total = len(steps)
    given = 0
    for index, run in enumerate(steps):
        upto = -(-len(edge) * (index + 1) // total)
        for work in edge[given:upto]:
            work()
        given = max(given, upto)
        run()
    head, steps = main_steps(shape, full, gsize, three, two, finish, grad, stress, part, 3)
    head()
    for run in steps:
        run()


def partner(size, parity, i):
    j = i + 1 if i % 2 == parity else i - 1
    return j if 0 <= j < size else None


def exchange(shape, parities):
    n = shape.n
    pairs = []
    for i in range(n[0]):
        for j in range(n[1]):
            for k in range(n[2]):
                here = (i, j, k)
                there = [
                    at if parity is None else partner(size, parity, at)
                    for at, size, parity in zip(here, n, parities)
                ]
                if None in there:
                    axis = 1 if parities[2] is not None else 2
                    other = partner(n[axis], 0, here[axis])
                    if other is None:
                        continue
                    there = list(here)
                    there[axis] = other
                pairs.append(
                    ((i * n[1] + j) * n[2] + k, (there[0] * n[1] + there[1]) * n[2] + there[2])
                )
    return pairs


def send(shape, value, *parities):
    return lax.ppermute(value, ("gx", "gy", "gz"), exchange(shape, parities))


def f32(*dims):
    return jax.ShapeDtypeStruct(dims, jnp.float32)


def in_hbm(value):
    return pltpu.with_memory_space_constraint(value, pltpu.MemorySpace.HBM)


def scratch(*dims):
    return pltpu.VMEM(dims, jnp.float32)


def call(body, outs, args, scratches=(), specs=None):
    return pl.pallas_call(
        body,
        out_shape=outs,
        in_specs=specs or [VM] * len(args),
        out_specs=jax.tree.map(lambda _: VM, outs),
        scratch_shapes=list(scratches),
        compiler_params=pltpu.CompilerParams(vmem_limit_bytes=40 * 1024 * 1024),
        cost_estimate=pl.CostEstimate(flops=2_000_000, bytes_accessed=100_000, transcendentals=0),
    )(*args)


def per_device(mesh, start_disp, inertial, material, pinned, stiffness):
    shape = Shape(mesh, material.shape)
    sx, sy, sz = shape.size
    sides = 1 if shape.mirror else 2
    rows, erows = shape.rows, shape.erows

    def prep(*refs):
        count = 3 + 3 * sides
        given, (own, *sent), held, sems = refs[:5], refs[5 : 5 + count], refs[5 + count : -1], refs[-1]
        copies = [pltpu.make_async_copy(a, b, sems.at[i]) for i, (a, b) in enumerate(zip(given, held))]
        for copy in copies:
            copy.start()
        for copy in copies:
            copy.wait()
        prep_kernel(shape, *held, own, sent[2 : 2 + sides], sent[:2], sent[2 + sides :])

    outs = [f32(CH, sy + 1, sx, sz)]
    outs += [f32(len(CARRY), sy // 2, 8, sz)] * 2 + [f32(len(LAYERS), sx, sz)] * sides
    outs += [f32(len(LAYERS) // 2, 8, sz)] * (2 * sides)
    own, *sent = call(
        prep,
        outs,
        (
            in_hbm(start_disp.reshape(3, sx * sy, sz)),
            in_hbm(inertial.reshape(3, sx * sy, sz)),
            in_hbm(material.reshape(sx * sy, sz)),
            in_hbm(pinned.reshape(sx * sy, sz)),
            in_hbm(stiffness),
        ),
        [
            scratch(3, sx * sy, sz),
            scratch(3, sx * sy, sz),
            pltpu.VMEM((sx * sy, sz), jnp.int32),
            pltpu.VMEM((sx * sy, sz), jnp.int32),
            pltpu.SMEM((MATS,), jnp.float32),
            pltpu.SemaphoreType.DMA((5,)),
        ],
        [HBM] * 5,
    )
    recv = [send(shape, sent[p], p, None, None) for p in range(2)]
    recv += [send(shape, sent[2 + p], None, p, None) for p in range(sides)]
    recv += [
        send(shape, sent[2 + sides + 2 * q + p], p, q, None) for q in range(sides) for p in range(2)
    ]

    def join(own, *rest):
        x, rest = rest[:2], rest[2:]
        y, rest = rest[:sides], rest[sides:]
        xy, rest = rest[: 2 * sides], rest[2 * sides :]
        full, z0, z1, nat = rest
        join_kernel(shape, own, y, x, xy, full, (z0, z1), nat)

    full, z0, z1 = call(
        join,
        [f32(CH, rows, 2, 8, sz), f32(erows, 2, 8, sz), f32(erows, 2, 8, sz)],
        (own, *recv),
        [scratch(CH, rows, sx + 2 * HALO, sz)],
    )
    z0 = send(shape, z0, None, None, 0)
    z1 = send(shape, z1, None, None, 1)
    one, two, gsize = call(
        functools.partial(main_kernel, shape),
        [f32(3, rows, 2, 8, sz), f32(3, rows, 2, 8, sz), f32(rows, 2, 8, sz)],
        (full,),
        [scratch(count, rows, 2, 8, sz) for count in (9, 9, 6)],
    )

    def last(*refs):
        ends = 11 + ITERS + 1
        last_kernel(shape, *refs[:11], refs[11:ends], *refs[ends:])

    (out,) = call(
        last,
        [f32(3, sx * sy, sz)],
        (full, one, two, gsize, z0, z1),
        [scratch(3, rows, 2, 8, sz)]
        + [scratch(count, rows, 2, 8, sz) for count in (9, 9, 6)]
        + [scratch(3, erows, 2, 8, sz) for _ in range(ITERS + 2)]
        + [scratch(erows, 2, 8, sz)] * 2
        + [scratch(9, erows + 1, 2, 8, sz)] * 2
        + [scratch(sy, 3, 2 * 8, sz)],
    )
    return out.reshape(3, sx, sy, sz)


def solution(mesh):
    placed = (
        P(None, "gx", "gy", "gz"),
        P(None, "gx", "gy", "gz"),
        P("gx", "gy", "gz"),
        P("gx", "gy", "gz"),
        P(),
    )
    return jax.shard_map(
        functools.partial(per_device, mesh),
        mesh=mesh,
        in_specs=placed,
        out_specs=P(None, "gx", "gy", "gz"),
        check_vma=False,
    )
```

```python
import functools
import math

import jax
import jax.numpy as jnp
from jax import lax
from jax.experimental import pallas as pl
from jax.experimental.pallas import tpu as pltpu
from jax.sharding import PartitionSpec as P

ITERS = 4
POLAR_STEPS = 6
MATS = 8
RELAX = 0.6
RADIUS = 0.9

HALO = ITERS
SCALE = 0.25 / math.sqrt(2.0)
UNIT = 1.0 / math.sqrt(2.0)
CH = 8
W_CH = 6
FREE_CH = 7
SHALLOW = (3, 4, 5, 7)
CARRY = (0, 1, 2, 3, 4, 5, 7)
LAYERS = tuple((c, d) for c in range(CH) for d in range(HALO - (c in SHALLOW)))
GROUPS = 4
SPAN = 32

VM = pl.BlockSpec(memory_space=pltpu.VMEM)
HBM = pl.BlockSpec(memory_space=pltpu.MemorySpace.HBM)


def omegas():
    values = [1.0]
    for step in range(1, ITERS):
        if step == 1:
            values.append(2.0 / (2.0 - RADIUS * RADIUS))
        else:
            values.append(4.0 / (4.0 - RADIUS * RADIUS * values[-1]))
    return values


def lane_ids():
    return lax.broadcasted_iota(jnp.int32, (8, 128), 1)


def sub_ids():
    return lax.broadcasted_iota(jnp.int32, (8, 128), 0)


def roll_z(value, amount):
    amount = amount % 128
    return value if amount == 0 else pltpu.roll(value, amount, 1)


def turn_x(value, amount):
    amount = amount % 8
    return value if amount == 0 else pltpu.roll(value, amount, 0)


def next_x(pair):
    return (pair[1], pltpu.roll(pair[0], 7, 0))


def prev_x(pair):
    return (pltpu.roll(pair[1], 1, 0), pair[0])


def add2(a, b):
    return tuple(x + y for x, y in zip(a, b))


def sub2(a, b):
    return tuple(x - y for x, y in zip(a, b))


def gradient_row(vrow):
    out = []
    for pair in vrow:
        ahead = tuple(roll_z(t, -1) for t in pair)
        sz = add2(pair, ahead)
        dz = sub2(ahead, pair)
        nsz = next_x(sz)
        out.append((add2(sz, nsz), sub2(nsz, sz), add2(dz, next_x(dz))))
    return out


THIRD_ANGLE = (
    0.866025405599564,
    0.16666637114459312,
    -0.04810444145461756,
    0.02460429680494765,
    -0.01510727520943827,
    0.009383330672620772,
    -0.004929691292929874,
    0.0017648569477158788,
    -0.0003028542202729437,
)


def polar_stress(f, weight):
    xx, yy, zz = (f[0][i] * f[0][i] + f[1][i] * f[1][i] + f[2][i] * f[2][i] for i in range(3))
    xy, xz, yz = (
        f[0][i] * f[0][j] + f[1][i] * f[1][j] + f[2][i] * f[2][j]
        for i, j in ((0, 1), (0, 2), (1, 2))
    )
    trace = xx + yy + zz
    s = jnp.minimum(lax.rsqrt(trace * (2.0 / 3.0)), 1.0)
    s2 = s * s
    mean = trace * (1.0 / 3.0)
    xx, yy, zz = xx - mean, yy - mean, zz - mean
    xy2, xz2, yz2 = xy * xy, xz * xz, yz * yz
    xyz = xy * xz
    sx2, sy2, sz2 = xx * xx + xy2, yy * yy + yz2, zz * zz + xz2
    spread = (sx2 + sy2 + sz2 + (xy2 + yz2 + xz2)) * (1.0 / 6.0)
    inverse = lax.rsqrt(jnp.maximum(spread, 1e-24))
    cross = xyz * yz
    det = xx * (yy * zz - yz2) + (cross + cross) - yy * xz2 - zz * xy2
    ratio = (det * 0.5) * inverse * inverse * inverse
    radius = spread * inverse * s2
    turn = jnp.minimum(jnp.abs(ratio), 1.0)
    c = jnp.full_like(turn, THIRD_ANGLE[-1])
    for value in THIRD_ANGLE[-2::-1]:
        c = c * turn + value
    square = jnp.maximum(1.0 - c * c, 1e-20)
    apart = radius * math.sqrt(3.0) * (square * lax.rsqrt(square))
    half = jnp.where(ratio < 0.0, -radius, radius) * c
    near = (apart - half, -apart - half, half + half)
    center = mean * s2
    level = [v + center for v in near]
    slope = None
    for step in range(POLAR_STEPS):
        m = [1.5 - v for v in level]
        if step == 0:
            q, dq = list(m), -1.0
        else:
            dq = dq * m[0] - q[1] * slope
            q = [a * b for a, b in zip(q, m)]
        if step < POLAR_STEPS - 1:
            m2 = [v * v for v in m]
            growth = m2[0] - level[1] * (m[0] + m[1])
            slope = growth if slope is None else slope * growth
            level = [a * b for a, b in zip(level, m2)]
    gap1, gap2 = near[0] - near[2], near[1] - near[2]
    inv = pl.reciprocal(jnp.maximum(gap1 * gap2, 1e-30))
    bend = (dq - (q[1] - q[2]) * (gap1 * inv)) * (gap2 * inv)
    k0 = (q[0] - dq * near[0] + bend * (near[0] * near[1])) * s
    k1 = (dq - bend * (near[0] + near[1])) * (s * s2)
    k2 = bend * (s * (s2 * s2))
    diag = (
        k0 + k1 * xx + k2 * (sx2 + xz2),
        k0 + k1 * yy + k2 * (sy2 + xy2),
        k0 + k1 * zz + k2 * (sz2 + yz2),
    )
    off = {
        (0, 1): k1 * xy + k2 * (xy * (xx + yy) + xz * yz),
        (0, 2): k1 * xz + k2 * (xz * (xx + zz) + xy * yz),
        (1, 2): k1 * yz + k2 * (yz * (yy + zz) + xyz),
    }
    diag = tuple(v - 1.0 for v in diag)
    out = []
    for c in range(3):
        row = []
        for d in range(3):
            value = f[c][d] * diag[d]
            for j in range(3):
                if j != d:
                    value = value + f[c][j] * off[(min(j, d), max(j, d))]
            row.append(weight * value)
        out.append(row)
    return out


def deform_rows(low, high):
    out = []
    for c in range(3):
        row = [
            add2(low[c][1], high[c][1]),
            sub2(high[c][0], low[c][0]),
            add2(low[c][2], high[c][2]),
        ]
        row[c] = tuple(t + UNIT for t in row[c])
        out.append(row)
    return out


def stress_row(f, weight):
    tiles = [
        polar_stress([[f[c][d][t] for d in range(3)] for c in range(3)], weight[t])
        for t in range(2)
    ]
    return [[(tiles[0][c][d], tiles[1][c][d]) for d in range(3)] for c in range(3)]


def force_parts(now, before):
    out = []
    for c in range(3):
        a = add2(now[c][0], before[c][0])
        b = sub2(now[c][1], before[c][1])
        e = add2(now[c][2], before[c][2])
        left = add2(add2(a, b), prev_x(sub2(b, a)))
        right = add2(e, prev_x(e))
        out.append((add2(left, right), sub2(left, right)))
    return out


def update_row(part, v, vin, prev, g, omega):
    new = []
    for c in range(3):
        row = []
        for t in range(2):
            force = part[c][0][t] + roll_z(part[c][1][t], 1)
            y = v[c][t] - g[t] * ((v[c][t] - vin[c][t]) + force)
            row.append(prev[c][t] + omega * (y - prev[c][t]))
        new.append(tuple(row))
    return new


class Shape:
    def __init__(self, mesh, size):
        self.n = tuple(mesh.shape[a] for a in ("gx", "gy", "gz"))
        self.size = size
        self.mirror = self.n[1] == 2
        self.own = 0 if self.mirror else HALO
        self.rows = size[1] + HALO * (1 if self.mirror else 2)
        self.erows = self.rows // GROUPS


def even(axis):
    return lax.rem(lax.axis_index(axis), 2) == 0


def pack_faces(first, second):
    upper = sub_ids() >= HALO
    low = jnp.where(upper, pltpu.roll(second, HALO, 0), first)
    high = jnp.where(upper, second, pltpu.roll(first, HALO, 0))
    return low, high


def prep_kernel(shape, start, inert, mat, pin, stiff, own, ysend, xsend, xysend):
    sx, sy, sz = shape.size
    gx, gy, gz = (lax.axis_index(a) for a in ("gx", "gy", "gz"))
    flip = (gy == 1) if shape.mirror else False
    sign = jnp.where(flip, -1.0, 1.0).astype(jnp.float32) if shape.mirror else jnp.float32(1.0)
    inside = (sub_ids() + gx * sx < shape.n[0] * sx - 1) & (
        lane_ids() + gz * sz < shape.n[2] * sz - 1
    )
    levels = [stiff[i] * (1.0 / 16.0) for i in range(MATS)]
    own[W_CH, sy] = jnp.zeros((8, 128), jnp.float32)
    for r in range(sy):
        at = pl.ds(r, sx, stride=sy)
        fixed = pin[at, :] > 0
        kind = mat[at, :]
        weight = jnp.zeros((8, 128), jnp.float32)
        for index in range(MATS):
            weight = jnp.where(kind == index, levels[index], weight)
        valid = inside & (r + gy * sy < shape.n[1] * sy - 1)
        weight = jnp.where(valid, weight, 0.0)
        node = jnp.where(flip, sy - 1 - r, r) + 1 if shape.mirror else r + 1
        cell = jnp.where(flip, sy - 2 - r, r) + 1 if shape.mirror else r + 1
        for c in range(3):
            factor = SCALE * sign if c == 1 else SCALE
            goal = inert[c, at, :] * factor
            own[c, node] = jnp.where(fixed, goal, start[c, at, :] * factor)
            own[3 + c, node] = goal
        own[W_CH, cell] = weight
        own[FREE_CH, node] = jnp.where(fixed, 0.0, 1.0)
    ex = even("gx")
    place = lax.rem(sub_ids(), HALO)
    for k in range(sy // 2):
        wlow, whigh = pack_faces(own[W_CH, 2 * k + 1], own[W_CH, 2 * k + 2])
        for index, c in enumerate(CARRY):
            low, high = pack_faces(own[c, 2 * k + 1], own[c, 2 * k + 2])
            if c in SHALLOW:
                q = SHALLOW.index(c)
                low = jnp.where(place == HALO - 1, turn_x(wlow, HALO - 1 - q), low)
                high = jnp.where(place == 0, turn_x(whigh, -q), high)
            xsend[0][index, k] = jnp.where(ex, high, low)
            xsend[1][index, k] = jnp.where(ex, low, high)
    for side in range(len(ysend)):
        rows = []
        for c, d in LAYERS:
            if shape.mirror:
                node = sy - 1 - d
                if c == W_CH:
                    node = node - jnp.where(flip, 1, 0)
            else:
                up = even("gy") if side == 0 else jnp.logical_not(even("gy"))
                node = jnp.where(up, sy - 1 - d, d)
            rows.append(own[c, node + 1])
            ysend[side][len(rows) - 1] = rows[-1]
        for k in range(len(rows) // 2):
            low, high = pack_faces(rows[2 * k], rows[2 * k + 1])
            xysend[2 * side][k] = jnp.where(ex, high, low)
            xysend[2 * side + 1][k] = jnp.where(ex, low, high)


def join_kernel(shape, own, yrecv, xrecv, xyrecv, full, zsend, nat):
    sx, sy, sz = shape.size
    rows = shape.rows
    ex, ez = even("gx"), even("gz")
    flip = (lax.axis_index("gy") == 1) if shape.mirror else False

    gx, gy = lax.axis_index("gx"), lax.axis_index("gy")
    inner = (gx > 0).astype(jnp.float32), (gx < shape.n[0] - 1).astype(jnp.float32)

    def put(c, row, low, mid, high):
        if c == W_CH:
            low, high = low * inner[0], high * inner[1]
        nat[c, row, 0:HALO] = low
        nat[c, row, HALO : HALO + sx] = mid
        nat[c, row, HALO + sx :] = high

    place = lax.rem(sub_ids(), HALO)
    for k in range(sy // 2):
        wlow = whigh = jnp.zeros((8, 128), jnp.float32)
        faces = {}
        for index, c in enumerate(CARRY):
            a, b = xrecv[0][index, k], xrecv[1][index, k]
            low, high = jnp.where(ex, b, a), jnp.where(ex, a, b)
            faces[c] = low, high
            if c in SHALLOW:
                q = SHALLOW.index(c)
                wlow = jnp.where(place == q, turn_x(low, q), wlow)
                whigh = jnp.where(place == q, turn_x(high, q + 1 - HALO), whigh)
        faces[W_CH] = wlow, whigh
        for c, (low, high) in faces.items():
            for h in range(2):
                part = slice(HALO * h, HALO * h + HALO)
                put(c, shape.own + 2 * k + h, low[part], own[c, 2 * k + h + 1], high[part])
    empty = jnp.zeros((sx + 2 * HALO, 128), jnp.float32)
    for c in SHALLOW:
        nat[c, rows - 1] = empty
        if not shape.mirror:
            nat[c, 0] = empty
    for side in range(1 if shape.mirror else 2):
        for k in range(len(LAYERS) // 2):
            near = LAYERS[2 * k : 2 * k + 2]
            if shape.mirror:
                a, b = xyrecv[0][k], xyrecv[1][k]
                mids = [yrecv[0][2 * k + h] for h in range(2)]
            else:
                lower = even("gy") if side else jnp.logical_not(even("gy"))
                a, b = (jnp.where(lower, xyrecv[i][k], xyrecv[2 + i][k]) for i in range(2))
                mids = [
                    jnp.where(lower, yrecv[0][2 * k + h], yrecv[1][2 * k + h]) for h in range(2)
                ]
            low, high = jnp.where(ex, b, a), jnp.where(ex, a, b)
            for h, (c, d) in enumerate(near):
                part = slice(HALO * h, HALO * h + HALO)
                values = [low[part], mids[h], high[part]]
                if shape.mirror:
                    row = sy + d
                    if c == W_CH:
                        row = row - jnp.where(flip, 1, 0)
                    if c in (1, 4):
                        values = [-t for t in values]
                else:
                    row = HALO + sy + d if side else HALO - 1 - d
                    if c == W_CH:
                        there = (gy < shape.n[1] - 1 if side else gy > 0).astype(jnp.float32)
                        values = [t * there for t in values]
                put(c, row, *values)
    nat[W_CH, rows - 1] = empty
    slot = lane_ids() // HALO
    for m in range(shape.erows):
        for t in range(2):
            up = jnp.zeros((8, 128), jnp.float32)
            down = jnp.zeros((8, 128), jnp.float32)
            for g in range(GROUPS):
                for c in range(CH):
                    tile = nat[c, g * shape.erows + m, pl.ds(t, 8, stride=2), :]
                    full[c, g * shape.erows + m, t] = tile
                    place = slot == (SPAN // HALO) * g + c
                    to = SPAN * g + HALO * c
                    up = jnp.where(place, roll_z(tile, to - (sz - HALO)), up)
                    down = jnp.where(place, roll_z(tile, to), down)
            zsend[0][m, t] = jnp.where(ez, up, down)
            zsend[1][m, t] = jnp.where(ez, down, up)


def load_row(ref, row, channels=range(3)):
    return [(ref[c, row, 0], ref[c, row, 1]) for c in channels]


def step_size(now, before, free):
    total = add2(now, before)
    total = add2(total, prev_x(total))
    return tuple(
        RELAX * f / (1.0 + 3.0 * (t + roll_z(t, 1))) for t, f in zip(total, free)
    )


def step_sizes(shape, full, gsize):
    zero = jnp.zeros((8, 128), jnp.float32)
    for row in range(shape.rows):
        now = load_row(full, row, (W_CH,))[0]
        before = load_row(full, row - 1, (W_CH,))[0] if row else (zero, zero)
        g = step_size(now, before, load_row(full, row, (FREE_CH,))[0])
        for t in range(2):
            gsize[row, t] = g[t]


def put9(ref, row, value):
    for c in range(3):
        for k in range(3):
            for t in range(2):
                ref[3 * c + k, row, t] = value[c][k][t]


def get9(ref, row):
    return [[(ref[3 * c + k, row, 0], ref[3 * c + k, row, 1]) for k in range(3)] for c in range(3)]


def packed_stresses(shape, full, step, rows, flat):
    fflat, wflat, pflat = flat
    width = shape.size[0] + 2 * HALO - 1 - 2 * step
    spans = []
    for t in range(2):
        first = -(-(step - t) // 2)
        spans.append((first, (shape.size[0] + 2 * HALO - 2 - t - step) // 2 - first + 1))
    begin = rows[0]
    state = {"tiles": 0, "rows": 0}

    def at(j, t, first, count):
        return pl.ds(8 + (j - begin) * width + 2 * first + t - step, count, stride=2)

    def run(j, f):
        for t, (first, count) in enumerate(spans):
            here = at(j, t, first, count)
            part = slice(first, first + count)
            for c in range(3):
                for d in range(3):
                    fflat[3 * c + d, here, :] = f[c][d][t][part]
            wflat[here, :] = full[W_CH, j, t][part]
        filled = (j - begin + 1) * width
        upto = filled // 8 if j < rows[-1] else -(-filled // 8)
        for i in range(state["tiles"], upto):
            tile = pl.ds(8 + 8 * i, 8)
            p = polar_stress(
                [[fflat[3 * c + d, tile, :] for d in range(3)] for c in range(3)], wflat[tile, :]
            )
            for c in range(3):
                for d in range(3):
                    pflat[3 * c + d, tile, :] = p[c][d]
        state["tiles"] = upto
        known = []
        while state["rows"] < len(rows) and (state["rows"] + 1) * width <= 8 * upto:
            r = begin + state["rows"]
            known.append(
                (
                    r,
                    [
                        [tuple(pflat[3 * c + d, at(r, t, 0, 8), :] for t in range(2)) for d in range(3)]
                        for c in range(3)
                    ],
                )
            )
            state["rows"] += 1
        return known

    return run


def main_steps(shape, full, gsize, old, oldest, write, grad, stress, part, step, flat=None):
    omega = omegas()[step]
    first = 0 if shape.mirror else step
    last = shape.rows - 1 - step
    zero = jnp.zeros((8, 128), jnp.float32)

    def update(row):
        held = [
            tuple((part[2 * c + i, row, 0], part[2 * c + i, row, 1]) for i in range(2))
            for c in range(3)
        ]
        write(
            row,
            update_row(
                held,
                load_row(old, row),
                load_row(full, row, (3, 4, 5)),
                load_row(oldest, row),
                (gsize[row, 0], gsize[row, 1]),
                omega,
            ),
        )

    def head():
        for row in (first, first + 1):
            put9(grad, row, gradient_row(load_row(old, row)))

    if flat:
        packed = packed_stresses(shape, full, step, range(first, last), flat)

    def body(j):
        after = gradient_row(load_row(old, j + 2)) if j + 2 <= last else None
        f = deform_rows(get9(grad, j), get9(grad, j + 1))
        if flat:
            known = packed(j, f)
        else:
            known = [(j, stress_row(f, load_row(full, j, (W_CH,))[0]))]
        if after is not None:
            put9(grad, j + 2, after)
        for r, now in known:
            before = get9(stress, r - 1) if r > first else [[(zero, zero)] * 3] * 3
            parts = force_parts(now, before)
            if r > first:
                update(r - 1)
            put9(stress, r, now)
            for c in range(3):
                for t in range(2):
                    for i in range(2):
                        part[2 * c + i, r, t] = parts[c][i][t]
            if r == last - 1:
                update(r)

    return head, [functools.partial(body, j) for j in range(first, last)]


def writer(ref):
    def write(row, new):
        for c in range(3):
            for t in range(2):
                ref[c, row, t] = new[c][t]

    return write


def main_kernel(shape, full, one, two, gsize, grad, stress, part):
    step_sizes(shape, full, gsize)
    for step, (old, oldest, new) in enumerate(((full, full, one), (one, full, two))):
        head, steps = main_steps(
            shape, full, gsize, old, oldest, writer(new), grad, stress, part, step
        )
        head()
        for run in steps:
            run()


def edge_parts(shape, full, zrecv, bufs, goal, gsize, stiff, grad, stress):
    sz = shape.size[2]
    erows = shape.erows
    ez = even("gz")
    lane = lane_ids()
    within = lane % SPAN
    half = SPAN // 2
    gz = lax.axis_index("gz")
    inner = (gz > 0).astype(jnp.float32), (gz < shape.n[2] - 1).astype(jnp.float32)

    def window(c, m, t):
        value = jnp.zeros((8, 128), jnp.float32)
        for g in range(GROUPS):
            tile = full[c, g * erows + m, t]
            base = SPAN * g
            value = jnp.where(
                (lane >= base + HALO) & (lane < base + half), roll_z(tile, base + HALO), value
            )
            value = jnp.where(
                (lane >= base + half) & (lane < base + SPAN - HALO),
                roll_z(tile, base + SPAN - HALO - sz),
                value,
            )
        return value

    def setup():
        for m in range(erows):
            for t in range(2):
                a, b = zrecv[0][m, t], zrecv[1][m, t]
                low, high = jnp.where(ez, b, a), jnp.where(ez, a, b)

                def extended(c):
                    below, above = roll_z(low, -HALO * c), roll_z(high, SPAN - HALO - HALO * c)
                    if c == W_CH:
                        below, above = below * inner[0], above * inner[1]
                    value = jnp.where(within < HALO, below, window(c, m, t))
                    return jnp.where(within >= SPAN - HALO, above, value)

                for c in range(3):
                    bufs[0][c, m, t] = extended(c)
                    goal[c, m, t] = extended(3 + c)
                stiff[m, t] = extended(W_CH)
                gsize[m, t] = extended(FREE_CH)
        weights = [(stiff[m, 0], stiff[m, 1]) for m in range(erows)]
        behind = tuple(roll_z(t, SPAN) for t in weights[-1])
        for m in range(erows):
            g = step_size(weights[m], weights[m - 1] if m else behind, (gsize[m, 0], gsize[m, 1]))
            for t in range(2):
                gsize[m, t] = g[t]

    def gradients(step):
        for m in range(erows):
            put9(grad, m, gradient_row(load_row(bufs[step], m)))
        turned = [tuple(roll_z(t, -SPAN) for t in pair) for pair in load_row(bufs[step], 0)]
        put9(grad, erows, gradient_row(turned))

    def stresses(m):
        now = stress_row(deform_rows(get9(grad, m), get9(grad, m + 1)), (stiff[m, 0], stiff[m, 1]))
        put9(stress, m + 1, now)
        if m == erows - 1:
            put9(stress, 0, [[tuple(roll_z(t, SPAN) for t in pair) for pair in row] for row in now])

    def updates(step, m):
        new = update_row(
            force_parts(get9(stress, m + 1), get9(stress, m)),
            load_row(bufs[step], m),
            load_row(goal, m),
            load_row(bufs[max(step - 1, 0)], m),
            (gsize[m, 0], gsize[m, 1]),
            omegas()[step],
        )
        writer(bufs[step + 1])(m, new)

    return setup, gradients, stresses, updates


def last_kernel(
    shape, full, one, two, gsize, zrecv0, zrecv1, out,
    three, grad, stress, part, bufs, egoal, egsize, estiff, egrad, estress, tiles, *flat,
):
    sx, sy, sz = shape.size
    erows = shape.erows
    lane = lane_ids()
    setup, gradients, stresses, updates = edge_parts(
        shape, full, (zrecv0, zrecv1), bufs, egoal, egsize, estiff, egrad, estress
    )
    flip = (lax.axis_index("gy") == 1) if shape.mirror else False
    turned = jnp.where(flip, -1.0 / SCALE, 1.0 / SCALE).astype(jnp.float32) if shape.mirror else 1.0 / SCALE

    def finish(row, new):
        r = row - shape.own
        if not 0 <= r < sy:
            return
        g, m = divmod(row, erows)
        base = SPAN * g
        place = jnp.where(flip, sy - 1 - r, r) if shape.mirror else r
        for c in range(3):
            for t in range(2):
                edge = bufs[ITERS][c, m, t]
                value = jnp.where(lane < HALO, roll_z(edge, -(base + HALO)), new[c][t])
                value = jnp.where(
                    lane >= sz - HALO, roll_z(edge, sz - HALO - (base + SPAN - 2 * HALO)), value
                )
                tiles[r, c, pl.ds(t, 8, stride=2), :] = value * (turned if c == 1 else 1.0 / SCALE)
            out[c, pl.ds(place, sx, stride=sy), :] = tiles[r, c, HALO : HALO + sx]

    edge = [setup]
    for step in range(ITERS):
        edge.append(functools.partial(gradients, step))
        order = [erows - 1] + list(range(erows - 1))
        edge.append(lambda order=order: [stresses(m) for m in order])
        edge.append(lambda step=step: [updates(step, m) for m in range(erows)])
    head, steps = main_steps(
        shape, full, gsize, two, one, writer(three), grad, stress, part, 2, flat
    )
    head()
    total = len(steps)
    given = 0
    for index, run in enumerate(steps):
        upto = -(-len(edge) * (index + 1) // total)
        for work in edge[given:upto]:
            work()
        given = max(given, upto)
        run()
    head, steps = main_steps(shape, full, gsize, three, two, finish, grad, stress, part, 3, flat)
    head()
    for run in steps:
        run()


def partner(size, parity, i):
    j = i + 1 if i % 2 == parity else i - 1
    return j if 0 <= j < size else None


def exchange(shape, parities):
    n = shape.n
    pairs = []
    for i in range(n[0]):
        for j in range(n[1]):
            for k in range(n[2]):
                here = (i, j, k)
                there = [
                    at if parity is None else partner(size, parity, at)
                    for at, size, parity in zip(here, n, parities)
                ]
                if None in there:
                    axis = 1 if parities[2] is not None else 2
                    other = partner(n[axis], 0, here[axis])
                    if other is None:
                        continue
                    there = list(here)
                    there[axis] = other
                pairs.append(
                    ((i * n[1] + j) * n[2] + k, (there[0] * n[1] + there[1]) * n[2] + there[2])
                )
    return pairs


def send(shape, value, *parities):
    return lax.ppermute(value, ("gx", "gy", "gz"), exchange(shape, parities))


def f32(*dims):
    return jax.ShapeDtypeStruct(dims, jnp.float32)


def in_hbm(value):
    return pltpu.with_memory_space_constraint(value, pltpu.MemorySpace.HBM)


def scratch(*dims):
    return pltpu.VMEM(dims, jnp.float32)


def call(body, outs, args, scratches=(), specs=None):
    return pl.pallas_call(
        body,
        out_shape=outs,
        in_specs=specs or [VM] * len(args),
        out_specs=jax.tree.map(lambda _: VM, outs),
        scratch_shapes=list(scratches),
        compiler_params=pltpu.CompilerParams(vmem_limit_bytes=40 * 1024 * 1024),
        cost_estimate=pl.CostEstimate(flops=2_000_000, bytes_accessed=100_000, transcendentals=0),
    )(*args)


def per_device(mesh, start_disp, inertial, material, pinned, stiffness):
    shape = Shape(mesh, material.shape)
    sx, sy, sz = shape.size
    sides = 1 if shape.mirror else 2
    rows, erows = shape.rows, shape.erows

    def prep(*refs):
        count = 3 + 3 * sides
        given, (own, *sent), held, sems = refs[:5], refs[5 : 5 + count], refs[5 + count : -1], refs[-1]
        copies = [pltpu.make_async_copy(a, b, sems.at[i]) for i, (a, b) in enumerate(zip(given, held))]
        for copy in copies:
            copy.start()
        for copy in copies:
            copy.wait()
        prep_kernel(shape, *held, own, sent[2 : 2 + sides], sent[:2], sent[2 + sides :])

    outs = [f32(CH, sy + 1, sx, sz)]
    outs += [f32(len(CARRY), sy // 2, 8, sz)] * 2 + [f32(len(LAYERS), sx, sz)] * sides
    outs += [f32(len(LAYERS) // 2, 8, sz)] * (2 * sides)
    own, *sent = call(
        prep,
        outs,
        (
            in_hbm(start_disp.reshape(3, sx * sy, sz)),
            in_hbm(inertial.reshape(3, sx * sy, sz)),
            in_hbm(material.reshape(sx * sy, sz)),
            in_hbm(pinned.reshape(sx * sy, sz)),
            in_hbm(stiffness),
        ),
        [
            scratch(3, sx * sy, sz),
            scratch(3, sx * sy, sz),
            pltpu.VMEM((sx * sy, sz), jnp.int32),
            pltpu.VMEM((sx * sy, sz), jnp.int32),
            pltpu.SMEM((MATS,), jnp.float32),
            pltpu.SemaphoreType.DMA((5,)),
        ],
        [HBM] * 5,
    )
    recv = [send(shape, sent[p], p, None, None) for p in range(2)]
    recv += [send(shape, sent[2 + p], None, p, None) for p in range(sides)]
    recv += [
        send(shape, sent[2 + sides + 2 * q + p], p, q, None) for q in range(sides) for p in range(2)
    ]

    def join(own, *rest):
        x, rest = rest[:2], rest[2:]
        y, rest = rest[:sides], rest[sides:]
        xy, rest = rest[: 2 * sides], rest[2 * sides :]
        full, z0, z1, nat = rest
        join_kernel(shape, own, y, x, xy, full, (z0, z1), nat)

    full, z0, z1 = call(
        join,
        [f32(CH, rows, 2, 8, sz), f32(erows, 2, 8, sz), f32(erows, 2, 8, sz)],
        (own, *recv),
        [scratch(CH, rows, sx + 2 * HALO, sz)],
    )
    z0 = send(shape, z0, None, None, 0)
    z1 = send(shape, z1, None, None, 1)
    one, two, gsize = call(
        functools.partial(main_kernel, shape),
        [f32(3, rows, 2, 8, sz), f32(3, rows, 2, 8, sz), f32(rows, 2, 8, sz)],
        (full,),
        [scratch(count, rows, 2, 8, sz) for count in (9, 9, 6)],
    )

    def last(*refs):
        ends = 11 + ITERS + 1
        last_kernel(shape, *refs[:11], refs[11:ends], *refs[ends:])

    (out,) = call(
        last,
        [f32(3, sx * sy, sz)],
        (full, one, two, gsize, z0, z1),
        [scratch(3, rows, 2, 8, sz)]
        + [scratch(count, rows, 2, 8, sz) for count in (9, 9, 6)]
        + [scratch(3, erows, 2, 8, sz) for _ in range(ITERS + 2)]
        + [scratch(erows, 2, 8, sz)] * 2
        + [scratch(9, erows + 1, 2, 8, sz)] * 2
        + [scratch(sy, 3, 2 * 8, sz)]
        + [scratch(9, 16 * (rows + 2), sz), scratch(16 * (rows + 2), sz), scratch(9, 16 * (rows + 2), sz)],
    )
    return out.reshape(3, sx, sy, sz)


def solution(mesh):
    placed = (
        P(None, "gx", "gy", "gz"),
        P(None, "gx", "gy", "gz"),
        P("gx", "gy", "gz"),
        P("gx", "gy", "gz"),
        P(),
    )
    return jax.shard_map(
        functools.partial(per_device, mesh),
        mesh=mesh,
        in_specs=placed,
        out_specs=P(None, "gx", "gy", "gz"),
        check_vma=False,
    )
```

```python
import functools
import math

import jax
import jax.numpy as jnp
from jax import lax
from jax.experimental import pallas as pl
from jax.experimental.pallas import tpu as pltpu
from jax.sharding import PartitionSpec as P

ITERS = 4
POLAR_STEPS = 6
MATS = 8
RELAX = 0.6
RADIUS = 0.9

HALO = ITERS
SCALE = 0.25 / math.sqrt(2.0)
UNIT = 1.0 / math.sqrt(2.0)
CH = 8
W_CH = 6
FREE_CH = 7
SHALLOW = (3, 4, 5, 7)
CARRY = (0, 1, 2, 3, 4, 5, 7)
LAYERS = tuple((c, d) for c in range(CH) for d in range(HALO - (c in SHALLOW)))
GROUPS = 4
SPAN = 32

VM = pl.BlockSpec(memory_space=pltpu.VMEM)
HBM = pl.BlockSpec(memory_space=pltpu.MemorySpace.HBM)


def omegas():
    values = [1.0]
    for step in range(1, ITERS):
        if step == 1:
            values.append(2.0 / (2.0 - RADIUS * RADIUS))
        else:
            values.append(4.0 / (4.0 - RADIUS * RADIUS * values[-1]))
    return values


def lane_ids():
    return lax.broadcasted_iota(jnp.int32, (8, 128), 1)


def sub_ids():
    return lax.broadcasted_iota(jnp.int32, (8, 128), 0)


def roll_z(value, amount):
    amount = amount % 128
    return value if amount == 0 else pltpu.roll(value, amount, 1)


def turn_x(value, amount):
    amount = amount % 8
    return value if amount == 0 else pltpu.roll(value, amount, 0)


def next_x(pair):
    return (pair[1], pltpu.roll(pair[0], 7, 0))


def prev_x(pair):
    return (pltpu.roll(pair[1], 1, 0), pair[0])


def add2(a, b):
    return tuple(x + y for x, y in zip(a, b))


def sub2(a, b):
    return tuple(x - y for x, y in zip(a, b))


def gradient_row(vrow):
    out = []
    for pair in vrow:
        ahead = tuple(roll_z(t, -1) for t in pair)
        sz = add2(pair, ahead)
        dz = sub2(ahead, pair)
        nsz = next_x(sz)
        out.append((add2(sz, nsz), sub2(nsz, sz), add2(dz, next_x(dz))))
    return out


THIRD_ANGLE = (
    0.866025405599564,
    0.16666637114459312,
    -0.04810444145461756,
    0.02460429680494765,
    -0.01510727520943827,
    0.009383330672620772,
    -0.004929691292929874,
    0.0017648569477158788,
    -0.0003028542202729437,
)


def polar_stress(f, weight):
    xx, yy, zz = (f[0][i] * f[0][i] + f[1][i] * f[1][i] + f[2][i] * f[2][i] for i in range(3))
    xy, xz, yz = (
        f[0][i] * f[0][j] + f[1][i] * f[1][j] + f[2][i] * f[2][j]
        for i, j in ((0, 1), (0, 2), (1, 2))
    )
    trace = xx + yy + zz
    s = jnp.minimum(lax.rsqrt(trace * (2.0 / 3.0)), 1.0)
    s2 = s * s
    mean = trace * (1.0 / 3.0)
    xx, yy, zz = xx - mean, yy - mean, zz - mean
    xy2, xz2, yz2 = xy * xy, xz * xz, yz * yz
    xyz = xy * xz
    sx2, sy2, sz2 = xx * xx + xy2, yy * yy + yz2, zz * zz + xz2
    spread = (sx2 + sy2 + sz2 + (xy2 + yz2 + xz2)) * (1.0 / 6.0)
    inverse = lax.rsqrt(jnp.maximum(spread, 1e-24))
    cross = xyz * yz
    det = xx * (yy * zz - yz2) + (cross + cross) - yy * xz2 - zz * xy2
    ratio = (det * 0.5) * inverse * inverse * inverse
    radius = spread * inverse * s2
    turn = jnp.minimum(jnp.abs(ratio), 1.0)
    c = jnp.full_like(turn, THIRD_ANGLE[-1])
    for value in THIRD_ANGLE[-2::-1]:
        c = c * turn + value
    square = jnp.maximum(1.0 - c * c, 1e-20)
    apart = radius * math.sqrt(3.0) * (square * lax.rsqrt(square))
    half = jnp.where(ratio < 0.0, -radius, radius) * c
    near = (apart - half, -apart - half, half + half)
    center = mean * s2
    level = [v + center for v in near]
    slope = None
    for step in range(POLAR_STEPS):
        m = [1.5 - v for v in level]
        if step == 0:
            q, dq = list(m), -1.0
        else:
            dq = dq * m[0] - q[1] * slope
            q = [a * b for a, b in zip(q, m)]
        if step < POLAR_STEPS - 1:
            m2 = [v * v for v in m]
            growth = m2[0] - level[1] * (m[0] + m[1])
            slope = growth if slope is None else slope * growth
            level = [a * b for a, b in zip(level, m2)]
    gap1, gap2 = near[0] - near[2], near[1] - near[2]
    inv = pl.reciprocal(jnp.maximum(gap1 * gap2, 1e-30))
    bend = (dq - (q[1] - q[2]) * (gap1 * inv)) * (gap2 * inv)
    k0 = (q[0] - dq * near[0] + bend * (near[0] * near[1])) * s
    k1 = (dq - bend * (near[0] + near[1])) * (s * s2)
    k2 = bend * (s * (s2 * s2))
    diag = (
        k0 + k1 * xx + k2 * (sx2 + xz2),
        k0 + k1 * yy + k2 * (sy2 + xy2),
        k0 + k1 * zz + k2 * (sz2 + yz2),
    )
    off = {
        (0, 1): k1 * xy + k2 * (xy * (xx + yy) + xz * yz),
        (0, 2): k1 * xz + k2 * (xz * (xx + zz) + xy * yz),
        (1, 2): k1 * yz + k2 * (yz * (yy + zz) + xyz),
    }
    diag = tuple(v - 1.0 for v in diag)
    out = []
    for c in range(3):
        row = []
        for d in range(3):
            value = f[c][d] * diag[d]
            for j in range(3):
                if j != d:
                    value = value + f[c][j] * off[(min(j, d), max(j, d))]
            row.append(weight * value)
        out.append(row)
    return out


def deform_rows(low, high):
    out = []
    for c in range(3):
        row = [
            add2(low[c][1], high[c][1]),
            sub2(high[c][0], low[c][0]),
            add2(low[c][2], high[c][2]),
        ]
        row[c] = tuple(t + UNIT for t in row[c])
        out.append(row)
    return out


def stress_row(f, weight):
    tiles = [
        polar_stress([[f[c][d][t] for d in range(3)] for c in range(3)], weight[t])
        for t in range(2)
    ]
    return [[(tiles[0][c][d], tiles[1][c][d]) for d in range(3)] for c in range(3)]


def force_parts(now, before):
    out = []
    for c in range(3):
        a = add2(now[c][0], before[c][0])
        b = sub2(now[c][1], before[c][1])
        e = add2(now[c][2], before[c][2])
        left = add2(add2(a, b), prev_x(sub2(b, a)))
        right = add2(e, prev_x(e))
        out.append((add2(left, right), sub2(left, right)))
    return out


def update_row(part, v, vin, prev, g, omega):
    new = []
    for c in range(3):
        row = []
        for t in range(2):
            force = part[c][0][t] + roll_z(part[c][1][t], 1)
            y = v[c][t] - g[t] * ((v[c][t] - vin[c][t]) + force)
            row.append(prev[c][t] + omega * (y - prev[c][t]))
        new.append(tuple(row))
    return new


class Shape:
    def __init__(self, mesh, size):
        self.n = tuple(mesh.shape[a] for a in ("gx", "gy", "gz"))
        self.size = size
        self.mirror = self.n[1] == 2
        self.own = 0 if self.mirror else HALO
        self.rows = size[1] + HALO * (1 if self.mirror else 2)
        self.erows = self.rows // GROUPS


def even(axis):
    return lax.rem(lax.axis_index(axis), 2) == 0


def pack_faces(first, second):
    upper = sub_ids() >= HALO
    low = jnp.where(upper, pltpu.roll(second, HALO, 0), first)
    high = jnp.where(upper, second, pltpu.roll(first, HALO, 0))
    return low, high


def prep_kernel(shape, start, inert, mat, pin, stiff, own, ysend, xsend, xysend):
    sx, sy, sz = shape.size
    gx, gy, gz = (lax.axis_index(a) for a in ("gx", "gy", "gz"))
    flip = (gy == 1) if shape.mirror else False
    sign = jnp.where(flip, -1.0, 1.0).astype(jnp.float32) if shape.mirror else jnp.float32(1.0)
    inside = (sub_ids() + gx * sx < shape.n[0] * sx - 1) & (
        lane_ids() + gz * sz < shape.n[2] * sz - 1
    )
    levels = [stiff[i] * (1.0 / 16.0) for i in range(MATS)]
    own[W_CH, sy] = jnp.zeros((8, 128), jnp.float32)
    for r in range(sy):
        at = pl.ds(r, sx, stride=sy)
        fixed = pin[at, :] > 0
        kind = mat[at, :]
        weight = jnp.zeros((8, 128), jnp.float32)
        for index in range(MATS):
            weight = jnp.where(kind == index, levels[index], weight)
        valid = inside & (r + gy * sy < shape.n[1] * sy - 1)
        weight = jnp.where(valid, weight, 0.0)
        node = jnp.where(flip, sy - 1 - r, r) + 1 if shape.mirror else r + 1
        cell = jnp.where(flip, sy - 2 - r, r) + 1 if shape.mirror else r + 1
        for c in range(3):
            factor = SCALE * sign if c == 1 else SCALE
            goal = inert[c, at, :] * factor
            own[c, node] = jnp.where(fixed, goal, start[c, at, :] * factor)
            own[3 + c, node] = goal
        own[W_CH, cell] = weight
        own[FREE_CH, node] = jnp.where(fixed, 0.0, 1.0)
    ex = even("gx")
    place = lax.rem(sub_ids(), HALO)
    for k in range(sy // 2):
        wlow, whigh = pack_faces(own[W_CH, 2 * k + 1], own[W_CH, 2 * k + 2])
        for index, c in enumerate(CARRY):
            low, high = pack_faces(own[c, 2 * k + 1], own[c, 2 * k + 2])
            if c in SHALLOW:
                q = SHALLOW.index(c)
                low = jnp.where(place == HALO - 1, turn_x(wlow, HALO - 1 - q), low)
                high = jnp.where(place == 0, turn_x(whigh, -q), high)
            xsend[0][index, k] = jnp.where(ex, high, low)
            xsend[1][index, k] = jnp.where(ex, low, high)
    for side in range(len(ysend)):
        rows = []
        for c, d in LAYERS:
            if shape.mirror:
                node = sy - 1 - d
                if c == W_CH:
                    node = node - jnp.where(flip, 1, 0)
            else:
                up = even("gy") if side == 0 else jnp.logical_not(even("gy"))
                node = jnp.where(up, sy - 1 - d, d)
            rows.append(own[c, node + 1])
            ysend[side][len(rows) - 1] = rows[-1]
        for k in range(len(rows) // 2):
            low, high = pack_faces(rows[2 * k], rows[2 * k + 1])
            xysend[2 * side][k] = jnp.where(ex, high, low)
            xysend[2 * side + 1][k] = jnp.where(ex, low, high)


def join_kernel(shape, own, yrecv, xrecv, xyrecv, full, zsend, nat):
    sx, sy, sz = shape.size
    rows = shape.rows
    ex, ez = even("gx"), even("gz")
    flip = (lax.axis_index("gy") == 1) if shape.mirror else False

    gx, gy = lax.axis_index("gx"), lax.axis_index("gy")
    inner = (gx > 0).astype(jnp.float32), (gx < shape.n[0] - 1).astype(jnp.float32)

    def put(c, row, low, mid, high):
        if c == W_CH:
            low, high = low * inner[0], high * inner[1]
        nat[c, row, 0:HALO] = low
        nat[c, row, HALO : HALO + sx] = mid
        nat[c, row, HALO + sx :] = high

    place = lax.rem(sub_ids(), HALO)
    for k in range(sy // 2):
        wlow = whigh = jnp.zeros((8, 128), jnp.float32)
        faces = {}
        for index, c in enumerate(CARRY):
            a, b = xrecv[0][index, k], xrecv[1][index, k]
            low, high = jnp.where(ex, b, a), jnp.where(ex, a, b)
            faces[c] = low, high
            if c in SHALLOW:
                q = SHALLOW.index(c)
                wlow = jnp.where(place == q, turn_x(low, q), wlow)
                whigh = jnp.where(place == q, turn_x(high, q + 1 - HALO), whigh)
        faces[W_CH] = wlow, whigh
        for c, (low, high) in faces.items():
            for h in range(2):
                part = slice(HALO * h, HALO * h + HALO)
                put(c, shape.own + 2 * k + h, low[part], own[c, 2 * k + h + 1], high[part])
    empty = jnp.zeros((sx + 2 * HALO, 128), jnp.float32)
    for c in SHALLOW:
        nat[c, rows - 1] = empty
        if not shape.mirror:
            nat[c, 0] = empty
    for side in range(1 if shape.mirror else 2):
        for k in range(len(LAYERS) // 2):
            near = LAYERS[2 * k : 2 * k + 2]
            if shape.mirror:
                a, b = xyrecv[0][k], xyrecv[1][k]
                mids = [yrecv[0][2 * k + h] for h in range(2)]
            else:
                lower = even("gy") if side else jnp.logical_not(even("gy"))
                a, b = (jnp.where(lower, xyrecv[i][k], xyrecv[2 + i][k]) for i in range(2))
                mids = [
                    jnp.where(lower, yrecv[0][2 * k + h], yrecv[1][2 * k + h]) for h in range(2)
                ]
            low, high = jnp.where(ex, b, a), jnp.where(ex, a, b)
            for h, (c, d) in enumerate(near):
                part = slice(HALO * h, HALO * h + HALO)
                values = [low[part], mids[h], high[part]]
                if shape.mirror:
                    row = sy + d
                    if c == W_CH:
                        row = row - jnp.where(flip, 1, 0)
                    if c in (1, 4):
                        values = [-t for t in values]
                else:
                    row = HALO + sy + d if side else HALO - 1 - d
                    if c == W_CH:
                        there = (gy < shape.n[1] - 1 if side else gy > 0).astype(jnp.float32)
                        values = [t * there for t in values]
                put(c, row, *values)
    nat[W_CH, rows - 1] = empty
    slot = lane_ids() // HALO
    for m in range(shape.erows):
        for t in range(2):
            up = jnp.zeros((8, 128), jnp.float32)
            down = jnp.zeros((8, 128), jnp.float32)
            for g in range(GROUPS):
                for c in range(CH):
                    tile = nat[c, g * shape.erows + m, pl.ds(t, 8, stride=2), :]
                    full[c, g * shape.erows + m, t] = tile
                    place = slot == (SPAN // HALO) * g + c
                    to = SPAN * g + HALO * c
                    up = jnp.where(place, roll_z(tile, to - (sz - HALO)), up)
                    down = jnp.where(place, roll_z(tile, to), down)
            zsend[0][m, t] = jnp.where(ez, up, down)
            zsend[1][m, t] = jnp.where(ez, down, up)


def load_row(ref, row, channels=range(3)):
    return [(ref[c, row, 0], ref[c, row, 1]) for c in channels]


def step_size(now, before, free):
    total = add2(now, before)
    total = add2(total, prev_x(total))
    return tuple(
        RELAX * f / (1.0 + 3.0 * (t + roll_z(t, 1))) for t, f in zip(total, free)
    )


def step_sizes(shape, full, gsize):
    zero = jnp.zeros((8, 128), jnp.float32)
    for row in range(shape.rows):
        now = load_row(full, row, (W_CH,))[0]
        before = load_row(full, row - 1, (W_CH,))[0] if row else (zero, zero)
        g = step_size(now, before, load_row(full, row, (FREE_CH,))[0])
        for t in range(2):
            gsize[row, t] = g[t]


def put9(ref, row, value):
    for c in range(3):
        for k in range(3):
            for t in range(2):
                ref[3 * c + k, row, t] = value[c][k][t]


def get9(ref, row):
    return [[(ref[3 * c + k, row, 0], ref[3 * c + k, row, 1]) for k in range(3)] for c in range(3)]


def packed_stresses(shape, weight, step, rows, flat):
    fflat, wflat, pflat = flat
    width = shape.size[0] + 2 * HALO - 1 - 2 * step
    spans = []
    for t in range(2):
        first = -(-(step - t) // 2)
        spans.append((first, (shape.size[0] + 2 * HALO - 2 - t - step) // 2 - first + 1))
    begin = rows[0]
    state = {"tiles": 0, "rows": 0}

    def at(j, t, first, count):
        return pl.ds(8 + (j - begin) * width + 2 * first + t - step, count, stride=2)

    def run(j, f):
        for t, (first, count) in enumerate(spans):
            here = at(j, t, first, count)
            part = slice(first, first + count)
            for c in range(3):
                for d in range(3):
                    fflat[3 * c + d, here, :] = f[c][d][t][part]
            wflat[here, :] = weight(j)[t][part]
        filled = (j - begin + 1) * width
        upto = filled // 8 if j < rows[-1] else -(-filled // 8)
        for i in range(state["tiles"], upto):
            tile = pl.ds(8 + 8 * i, 8)
            p = polar_stress(
                [[fflat[3 * c + d, tile, :] for d in range(3)] for c in range(3)], wflat[tile, :]
            )
            for c in range(3):
                for d in range(3):
                    pflat[3 * c + d, tile, :] = p[c][d]
        state["tiles"] = upto
        known = []
        while state["rows"] < len(rows) and (state["rows"] + 1) * width <= 8 * upto:
            r = begin + state["rows"]
            known.append(
                (
                    r,
                    [
                        [tuple(pflat[3 * c + d, at(r, t, 0, 8), :] for t in range(2)) for d in range(3)]
                        for c in range(3)
                    ],
                )
            )
            state["rows"] += 1
        return known

    return run


def main_steps(shape, full, gsize, old, oldest, write, grad, stress, part, step, flat=None):
    omega = omegas()[step]
    first = 0 if shape.mirror else step
    last = shape.rows - 1 - step
    zero = jnp.zeros((8, 128), jnp.float32)

    def update(row):
        held = [
            tuple((part[2 * c + i, row, 0], part[2 * c + i, row, 1]) for i in range(2))
            for c in range(3)
        ]
        write(
            row,
            update_row(
                held,
                load_row(old, row),
                load_row(full, row, (3, 4, 5)),
                load_row(oldest, row),
                (gsize[row, 0], gsize[row, 1]),
                omega,
            ),
        )

    def head():
        for row in (first, first + 1):
            put9(grad, row, gradient_row(load_row(old, row)))

    if flat:
        packed = packed_stresses(
            shape,
            lambda j: load_row(full, j, (W_CH,))[0],
            step,
            range(first, last),
            flat,
        )

    def body(j):
        after = gradient_row(load_row(old, j + 2)) if j + 2 <= last else None
        f = deform_rows(get9(grad, j), get9(grad, j + 1))
        if flat:
            known = packed(j, f)
        else:
            known = [(j, stress_row(f, load_row(full, j, (W_CH,))[0]))]
        if after is not None:
            put9(grad, j + 2, after)
        for r, now in known:
            before = get9(stress, r - 1) if r > first else [[(zero, zero)] * 3] * 3
            parts = force_parts(now, before)
            if r > first:
                update(r - 1)
            put9(stress, r, now)
            for c in range(3):
                for t in range(2):
                    for i in range(2):
                        part[2 * c + i, r, t] = parts[c][i][t]
            if r == last - 1:
                update(r)

    return head, [functools.partial(body, j) for j in range(first, last)]


def writer(ref):
    def write(row, new):
        for c in range(3):
            for t in range(2):
                ref[c, row, t] = new[c][t]

    return write


def main_kernel(shape, full, one, two, gsize, grad, stress, part, *flat):
    step_sizes(shape, full, gsize)
    for step, (old, oldest, new) in enumerate(((full, full, one), (one, full, two))):
        head, steps = main_steps(
            shape, full, gsize, old, oldest, writer(new), grad, stress, part, step, flat if step else None
        )
        head()
        for run in steps:
            run()


def edge_parts(shape, full, zrecv, bufs, goal, gsize, stiff, grad, stress, flat):
    sz = shape.size[2]
    erows = shape.erows
    ez = even("gz")
    lane = lane_ids()
    within = lane % SPAN
    half = SPAN // 2
    gz = lax.axis_index("gz")
    inner = (gz > 0).astype(jnp.float32), (gz < shape.n[2] - 1).astype(jnp.float32)

    def window(c, m, t):
        value = jnp.zeros((8, 128), jnp.float32)
        for g in range(GROUPS):
            tile = full[c, g * erows + m, t]
            base = SPAN * g
            value = jnp.where(
                (lane >= base + HALO) & (lane < base + half), roll_z(tile, base + HALO), value
            )
            value = jnp.where(
                (lane >= base + half) & (lane < base + SPAN - HALO),
                roll_z(tile, base + SPAN - HALO - sz),
                value,
            )
        return value

    def setup():
        for m in range(erows):
            for t in range(2):
                a, b = zrecv[0][m, t], zrecv[1][m, t]
                low, high = jnp.where(ez, b, a), jnp.where(ez, a, b)

                def extended(c):
                    below, above = roll_z(low, -HALO * c), roll_z(high, SPAN - HALO - HALO * c)
                    if c == W_CH:
                        below, above = below * inner[0], above * inner[1]
                    value = jnp.where(within < HALO, below, window(c, m, t))
                    return jnp.where(within >= SPAN - HALO, above, value)

                for c in range(3):
                    bufs[0][c, m, t] = extended(c)
                    goal[c, m, t] = extended(3 + c)
                stiff[m, t] = extended(W_CH)
                gsize[m, t] = extended(FREE_CH)
        weights = [(stiff[m, 0], stiff[m, 1]) for m in range(erows)]
        behind = tuple(roll_z(t, SPAN) for t in weights[-1])
        for m in range(erows):
            g = step_size(weights[m], weights[m - 1] if m else behind, (gsize[m, 0], gsize[m, 1]))
            for t in range(2):
                gsize[m, t] = g[t]

    def gradients(step):
        for m in range(erows):
            put9(grad, m, gradient_row(load_row(bufs[step], m)))
        turned = [tuple(roll_z(t, -SPAN) for t in pair) for pair in load_row(bufs[step], 0)]
        put9(grad, erows, gradient_row(turned))

    def keep(m, now):
        put9(stress, m + 1, now)
        if m == erows - 1:
            put9(stress, 0, [[tuple(roll_z(t, SPAN) for t in pair) for pair in row] for row in now])

    def stresses(step):
        def weight(m):
            return (stiff[m, 0], stiff[m, 1])

        rows = range(erows)
        if step:
            packed = packed_stresses(shape, weight, step, rows, flat)
        for m in rows if step else [erows - 1, *rows[:-1]]:
            f = deform_rows(get9(grad, m), get9(grad, m + 1))
            for known in packed(m, f) if step else [(m, stress_row(f, weight(m)))]:
                keep(*known)

    def updates(step, m):
        new = update_row(
            force_parts(get9(stress, m + 1), get9(stress, m)),
            load_row(bufs[step], m),
            load_row(goal, m),
            load_row(bufs[max(step - 1, 0)], m),
            (gsize[m, 0], gsize[m, 1]),
            omegas()[step],
        )
        writer(bufs[step + 1])(m, new)

    return setup, gradients, stresses, updates


def last_kernel(
    shape, full, one, two, gsize, zrecv0, zrecv1, out,
    three, grad, stress, part, bufs, egoal, egsize, estiff, egrad, estress, tiles, *flat,
):
    sx, sy, sz = shape.size
    erows = shape.erows
    lane = lane_ids()
    setup, gradients, stresses, updates = edge_parts(
        shape, full, (zrecv0, zrecv1), bufs, egoal, egsize, estiff, egrad, estress, flat[3:]
    )
    flat = flat[:3]
    flip = (lax.axis_index("gy") == 1) if shape.mirror else False
    turned = jnp.where(flip, -1.0 / SCALE, 1.0 / SCALE).astype(jnp.float32) if shape.mirror else 1.0 / SCALE

    def finish(row, new):
        r = row - shape.own
        if not 0 <= r < sy:
            return
        g, m = divmod(row, erows)
        base = SPAN * g
        place = jnp.where(flip, sy - 1 - r, r) if shape.mirror else r
        for c in range(3):
            for t in range(2):
                edge = bufs[ITERS][c, m, t]
                value = jnp.where(lane < HALO, roll_z(edge, -(base + HALO)), new[c][t])
                value = jnp.where(
                    lane >= sz - HALO, roll_z(edge, sz - HALO - (base + SPAN - 2 * HALO)), value
                )
                tiles[r, c, pl.ds(t, 8, stride=2), :] = value * (turned if c == 1 else 1.0 / SCALE)
            out[c, pl.ds(place, sx, stride=sy), :] = tiles[r, c, HALO : HALO + sx]

    edge = [setup]
    for step in range(ITERS):
        edge.append(functools.partial(gradients, step))
        edge.append(functools.partial(stresses, step))
        edge.append(lambda step=step: [updates(step, m) for m in range(erows)])
    head, steps = main_steps(
        shape, full, gsize, two, one, writer(three), grad, stress, part, 2, flat
    )
    head()
    total = len(steps)
    given = 0
    for index, run in enumerate(steps):
        upto = -(-len(edge) * (index + 1) // total)
        for work in edge[given:upto]:
            work()
        given = max(given, upto)
        run()
    head, steps = main_steps(shape, full, gsize, three, two, finish, grad, stress, part, 3, flat)
    head()
    for run in steps:
        run()


def partner(size, parity, i):
    j = i + 1 if i % 2 == parity else i - 1
    return j if 0 <= j < size else None


def exchange(shape, parities):
    n = shape.n
    pairs = []
    for i in range(n[0]):
        for j in range(n[1]):
            for k in range(n[2]):
                here = (i, j, k)
                there = [
                    at if parity is None else partner(size, parity, at)
                    for at, size, parity in zip(here, n, parities)
                ]
                if None in there:
                    axis = 1 if parities[2] is not None else 2
                    other = partner(n[axis], 0, here[axis])
                    if other is None:
                        continue
                    there = list(here)
                    there[axis] = other
                pairs.append(
                    ((i * n[1] + j) * n[2] + k, (there[0] * n[1] + there[1]) * n[2] + there[2])
                )
    return pairs


def send(shape, value, *parities):
    return lax.ppermute(value, ("gx", "gy", "gz"), exchange(shape, parities))


def f32(*dims):
    return jax.ShapeDtypeStruct(dims, jnp.float32)


def in_hbm(value):
    return pltpu.with_memory_space_constraint(value, pltpu.MemorySpace.HBM)


def scratch(*dims):
    return pltpu.VMEM(dims, jnp.float32)


def call(body, outs, args, scratches=(), specs=None):
    return pl.pallas_call(
        body,
        out_shape=outs,
        in_specs=specs or [VM] * len(args),
        out_specs=jax.tree.map(lambda _: VM, outs),
        scratch_shapes=list(scratches),
        compiler_params=pltpu.CompilerParams(vmem_limit_bytes=40 * 1024 * 1024),
        cost_estimate=pl.CostEstimate(flops=2_000_000, bytes_accessed=100_000, transcendentals=0),
    )(*args)


def per_device(mesh, start_disp, inertial, material, pinned, stiffness):
    shape = Shape(mesh, material.shape)
    sx, sy, sz = shape.size
    sides = 1 if shape.mirror else 2
    rows, erows = shape.rows, shape.erows

    def prep(*refs):
        count = 3 + 3 * sides
        given, (own, *sent), held, sems = refs[:5], refs[5 : 5 + count], refs[5 + count : -1], refs[-1]
        copies = [pltpu.make_async_copy(a, b, sems.at[i]) for i, (a, b) in enumerate(zip(given, held))]
        for copy in copies:
            copy.start()
        for copy in copies:
            copy.wait()
        prep_kernel(shape, *held, own, sent[2 : 2 + sides], sent[:2], sent[2 + sides :])

    outs = [f32(CH, sy + 1, sx, sz)]
    outs += [f32(len(CARRY), sy // 2, 8, sz)] * 2 + [f32(len(LAYERS), sx, sz)] * sides
    outs += [f32(len(LAYERS) // 2, 8, sz)] * (2 * sides)
    own, *sent = call(
        prep,
        outs,
        (
            in_hbm(start_disp.reshape(3, sx * sy, sz)),
            in_hbm(inertial.reshape(3, sx * sy, sz)),
            in_hbm(material.reshape(sx * sy, sz)),
            in_hbm(pinned.reshape(sx * sy, sz)),
            in_hbm(stiffness),
        ),
        [
            scratch(3, sx * sy, sz),
            scratch(3, sx * sy, sz),
            pltpu.VMEM((sx * sy, sz), jnp.int32),
            pltpu.VMEM((sx * sy, sz), jnp.int32),
            pltpu.SMEM((MATS,), jnp.float32),
            pltpu.SemaphoreType.DMA((5,)),
        ],
        [HBM] * 5,
    )
    recv = [send(shape, sent[p], p, None, None) for p in range(2)]
    recv += [send(shape, sent[2 + p], None, p, None) for p in range(sides)]
    recv += [
        send(shape, sent[2 + sides + 2 * q + p], p, q, None) for q in range(sides) for p in range(2)
    ]

    def join(own, *rest):
        x, rest = rest[:2], rest[2:]
        y, rest = rest[:sides], rest[sides:]
        xy, rest = rest[: 2 * sides], rest[2 * sides :]
        full, z0, z1, nat = rest
        join_kernel(shape, own, y, x, xy, full, (z0, z1), nat)

    full, z0, z1 = call(
        join,
        [f32(CH, rows, 2, 8, sz), f32(erows, 2, 8, sz), f32(erows, 2, 8, sz)],
        (own, *recv),
        [scratch(CH, rows, sx + 2 * HALO, sz)],
    )
    z0 = send(shape, z0, None, None, 0)
    z1 = send(shape, z1, None, None, 1)
    def flat(count):
        length = 16 * (count + 2)
        return [scratch(9, length, sz), scratch(length, sz), scratch(9, length, sz)]

    one, two, gsize = call(
        functools.partial(main_kernel, shape),
        [f32(3, rows, 2, 8, sz), f32(3, rows, 2, 8, sz), f32(rows, 2, 8, sz)],
        (full,),
        [scratch(count, rows, 2, 8, sz) for count in (9, 9, 6)] + flat(rows),
    )

    def last(*refs):
        ends = 11 + ITERS + 1
        last_kernel(shape, *refs[:11], refs[11:ends], *refs[ends:])

    (out,) = call(
        last,
        [f32(3, sx * sy, sz)],
        (full, one, two, gsize, z0, z1),
        [scratch(3, rows, 2, 8, sz)]
        + [scratch(count, rows, 2, 8, sz) for count in (9, 9, 6)]
        + [scratch(3, erows, 2, 8, sz) for _ in range(ITERS + 2)]
        + [scratch(erows, 2, 8, sz)] * 2
        + [scratch(9, erows + 1, 2, 8, sz)] * 2
        + [scratch(sy, 3, 2 * 8, sz)]
        + flat(rows)
        + flat(erows),
    )
    return out.reshape(3, sx, sy, sz)


def solution(mesh):
    placed = (
        P(None, "gx", "gy", "gz"),
        P(None, "gx", "gy", "gz"),
        P("gx", "gy", "gz"),
        P("gx", "gy", "gz"),
        P(),
    )
    return jax.shard_map(
        functools.partial(per_device, mesh),
        mesh=mesh,
        in_specs=placed,
        out_specs=P(None, "gx", "gy", "gz"),
        check_vma=False,
    )
```

```python
import functools
import math

import jax
import jax.numpy as jnp
from jax import lax
from jax.experimental import pallas as pl
from jax.experimental.pallas import tpu as pltpu
from jax.sharding import PartitionSpec as P

ITERS = 4
POLAR_STEPS = 6
MATS = 8
RELAX = 0.6
RADIUS = 0.9

HALO = ITERS
SCALE = 0.25 / math.sqrt(2.0)
UNIT = 1.0 / math.sqrt(2.0)
CH = 8
W_CH = 6
FREE_CH = 7
SHALLOW = (3, 4, 5, 7)
CARRY = (0, 1, 2, 3, 4, 5, 7)
LAYERS = tuple((c, d) for c in range(CH) for d in range(HALO - (c in SHALLOW)))
GROUPS = 4
SPAN = 32

VM = pl.BlockSpec(memory_space=pltpu.VMEM)
HBM = pl.BlockSpec(memory_space=pltpu.MemorySpace.HBM)


def omegas():
    values = [1.0]
    for step in range(1, ITERS):
        if step == 1:
            values.append(2.0 / (2.0 - RADIUS * RADIUS))
        else:
            values.append(4.0 / (4.0 - RADIUS * RADIUS * values[-1]))
    return values


def lane_ids():
    return lax.broadcasted_iota(jnp.int32, (8, 128), 1)


def sub_ids():
    return lax.broadcasted_iota(jnp.int32, (8, 128), 0)


def roll_z(value, amount):
    amount = amount % 128
    return value if amount == 0 else pltpu.roll(value, amount, 1)


def turn_x(value, amount):
    amount = amount % 8
    return value if amount == 0 else pltpu.roll(value, amount, 0)


def next_x(pair):
    return (pair[1], pltpu.roll(pair[0], 7, 0))


def prev_x(pair):
    return (pltpu.roll(pair[1], 1, 0), pair[0])


def add2(a, b):
    return tuple(x + y for x, y in zip(a, b))


def sub2(a, b):
    return tuple(x - y for x, y in zip(a, b))


def gradient_row(vrow):
    out = []
    for pair in vrow:
        ahead = tuple(roll_z(t, -1) for t in pair)
        sz = add2(pair, ahead)
        dz = sub2(ahead, pair)
        nsz = next_x(sz)
        out.append((add2(sz, nsz), sub2(nsz, sz), add2(dz, next_x(dz))))
    return out


THIRD_ANGLE = (
    0.866025405599564,
    0.16666637114459312,
    -0.04810444145461756,
    0.02460429680494765,
    -0.01510727520943827,
    0.009383330672620772,
    -0.004929691292929874,
    0.0017648569477158788,
    -0.0003028542202729437,
)


def polar_stress(f, weight):
    xx, yy, zz = (f[0][i] * f[0][i] + f[1][i] * f[1][i] + f[2][i] * f[2][i] for i in range(3))
    xy, xz, yz = (
        f[0][i] * f[0][j] + f[1][i] * f[1][j] + f[2][i] * f[2][j]
        for i, j in ((0, 1), (0, 2), (1, 2))
    )
    trace = xx + yy + zz
    s = jnp.minimum(lax.rsqrt(trace * (2.0 / 3.0)), 1.0)
    s2 = s * s
    mean = trace * (1.0 / 3.0)
    xx, yy, zz = xx - mean, yy - mean, zz - mean
    xy2, xz2, yz2 = xy * xy, xz * xz, yz * yz
    xyz = xy * xz
    sx2, sy2, sz2 = xx * xx + xy2, yy * yy + yz2, zz * zz + xz2
    spread = (sx2 + sy2 + sz2 + (xy2 + yz2 + xz2)) * (1.0 / 6.0)
    inverse = lax.rsqrt(jnp.maximum(spread, 1e-24))
    cross = xyz * yz
    det = xx * (yy * zz - yz2) + (cross + cross) - yy * xz2 - zz * xy2
    ratio = (det * 0.5) * inverse * inverse * inverse
    radius = spread * inverse * s2
    turn = jnp.minimum(jnp.abs(ratio), 1.0)
    c = jnp.full_like(turn, THIRD_ANGLE[-1])
    for value in THIRD_ANGLE[-2::-1]:
        c = c * turn + value
    square = jnp.maximum(1.0 - c * c, 1e-20)
    apart = radius * math.sqrt(3.0) * (square * lax.rsqrt(square))
    half = jnp.where(ratio < 0.0, -radius, radius) * c
    near = (apart - half, -apart - half, half + half)
    center = mean * s2
    level = [v + center for v in near]
    slope = None
    for step in range(POLAR_STEPS):
        m = [1.5 - v for v in level]
        if step == 0:
            q, dq = list(m), -1.0
        else:
            dq = dq * m[0] - q[1] * slope
            q = [a * b for a, b in zip(q, m)]
        if step < POLAR_STEPS - 1:
            m2 = [v * v for v in m]
            growth = m2[0] - level[1] * (m[0] + m[1])
            slope = growth if slope is None else slope * growth
            level = [a * b for a, b in zip(level, m2)]
    gap1, gap2 = near[0] - near[2], near[1] - near[2]
    inv = pl.reciprocal(jnp.maximum(gap1 * gap2, 1e-30))
    bend = (dq - (q[1] - q[2]) * (gap1 * inv)) * (gap2 * inv)
    k0 = (q[0] - dq * near[0] + bend * (near[0] * near[1])) * s
    k1 = (dq - bend * (near[0] + near[1])) * (s * s2)
    k2 = bend * (s * (s2 * s2))
    diag = (
        k0 + k1 * xx + k2 * (sx2 + xz2),
        k0 + k1 * yy + k2 * (sy2 + xy2),
        k0 + k1 * zz + k2 * (sz2 + yz2),
    )
    off = {
        (0, 1): k1 * xy + k2 * (xy * (xx + yy) + xz * yz),
        (0, 2): k1 * xz + k2 * (xz * (xx + zz) + xy * yz),
        (1, 2): k1 * yz + k2 * (yz * (yy + zz) + xyz),
    }
    diag = tuple(v - 1.0 for v in diag)
    out = []
    for c in range(3):
        row = []
        for d in range(3):
            value = f[c][d] * diag[d]
            for j in range(3):
                if j != d:
                    value = value + f[c][j] * off[(min(j, d), max(j, d))]
            row.append(weight * value)
        out.append(row)
    return out


def deform_rows(low, high):
    out = []
    for c in range(3):
        row = [
            add2(low[c][1], high[c][1]),
            sub2(high[c][0], low[c][0]),
            add2(low[c][2], high[c][2]),
        ]
        row[c] = tuple(t + UNIT for t in row[c])
        out.append(row)
    return out


def stress_row(f, weight):
    tiles = [
        polar_stress([[f[c][d][t] for d in range(3)] for c in range(3)], weight[t])
        for t in range(2)
    ]
    return [[(tiles[0][c][d], tiles[1][c][d]) for d in range(3)] for c in range(3)]


def force_parts(now, before):
    out = []
    for c in range(3):
        a = add2(now[c][0], before[c][0])
        b = sub2(now[c][1], before[c][1])
        e = add2(now[c][2], before[c][2])
        left = add2(add2(a, b), prev_x(sub2(b, a)))
        right = add2(e, prev_x(e))
        out.append((add2(left, right), sub2(left, right)))
    return out


def update_row(part, v, vin, prev, g, omega):
    new = []
    for c in range(3):
        row = []
        for t in range(2):
            force = part[c][0][t] + roll_z(part[c][1][t], 1)
            y = v[c][t] - g[t] * ((v[c][t] - vin[c][t]) + force)
            row.append(prev[c][t] + omega * (y - prev[c][t]))
        new.append(tuple(row))
    return new


class Shape:
    def __init__(self, mesh, size):
        self.n = tuple(mesh.shape[a] for a in ("gx", "gy", "gz"))
        self.size = size
        self.mirror = self.n[1] == 2
        self.own = 0 if self.mirror else HALO
        self.rows = size[1] + HALO * (1 if self.mirror else 2)
        self.erows = self.rows // GROUPS


def even(axis):
    return lax.rem(lax.axis_index(axis), 2) == 0


def pack_faces(first, second):
    upper = sub_ids() >= HALO
    low = jnp.where(upper, pltpu.roll(second, HALO, 0), first)
    high = jnp.where(upper, second, pltpu.roll(first, HALO, 0))
    return low, high


def prep_kernel(shape, start, inert, mat, pin, stiff, own, ysend, xsend, xysend):
    sx, sy, sz = shape.size
    gx, gy, gz = (lax.axis_index(a) for a in ("gx", "gy", "gz"))
    flip = (gy == 1) if shape.mirror else False
    sign = jnp.where(flip, -1.0, 1.0).astype(jnp.float32) if shape.mirror else jnp.float32(1.0)
    inside = (sub_ids() + gx * sx < shape.n[0] * sx - 1) & (
        lane_ids() + gz * sz < shape.n[2] * sz - 1
    )
    levels = [stiff[i] * (1.0 / 16.0) for i in range(MATS)]
    own[W_CH, sy] = jnp.zeros((8, 128), jnp.float32)
    for r in range(sy):
        at = pl.ds(r, sx, stride=sy)
        fixed = pin[at, :] > 0
        kind = mat[at, :]
        weight = jnp.zeros((8, 128), jnp.float32)
        for index in range(MATS):
            weight = jnp.where(kind == index, levels[index], weight)
        valid = inside & (r + gy * sy < shape.n[1] * sy - 1)
        weight = jnp.where(valid, weight, 0.0)
        node = jnp.where(flip, sy - 1 - r, r) + 1 if shape.mirror else r + 1
        cell = jnp.where(flip, sy - 2 - r, r) + 1 if shape.mirror else r + 1
        for c in range(3):
            factor = SCALE * sign if c == 1 else SCALE
            goal = inert[c, at, :] * factor
            own[c, node] = jnp.where(fixed, goal, start[c, at, :] * factor)
            own[3 + c, node] = goal
        own[W_CH, cell] = weight
        own[FREE_CH, node] = jnp.where(fixed, 0.0, 1.0)
    ex = even("gx")
    place = lax.rem(sub_ids(), HALO)
    for k in range(sy // 2):
        wlow, whigh = pack_faces(own[W_CH, 2 * k + 1], own[W_CH, 2 * k + 2])
        for index, c in enumerate(CARRY):
            low, high = pack_faces(own[c, 2 * k + 1], own[c, 2 * k + 2])
            if c in SHALLOW:
                q = SHALLOW.index(c)
                low = jnp.where(place == HALO - 1, turn_x(wlow, HALO - 1 - q), low)
                high = jnp.where(place == 0, turn_x(whigh, -q), high)
            xsend[0][index, k] = jnp.where(ex, high, low)
            xsend[1][index, k] = jnp.where(ex, low, high)
    for side in range(len(ysend)):
        rows = []
        for c, d in LAYERS:
            if shape.mirror:
                node = sy - 1 - d
                if c == W_CH:
                    node = node - jnp.where(flip, 1, 0)
            else:
                up = even("gy") if side == 0 else jnp.logical_not(even("gy"))
                node = jnp.where(up, sy - 1 - d, d)
            rows.append(own[c, node + 1])
            ysend[side][len(rows) - 1] = rows[-1]
        for k in range(len(rows) // 2):
            low, high = pack_faces(rows[2 * k], rows[2 * k + 1])
            xysend[2 * side][k] = jnp.where(ex, high, low)
            xysend[2 * side + 1][k] = jnp.where(ex, low, high)


def join_kernel(shape, own, yrecv, xrecv, xyrecv, full, zsend, nat):
    sx, sy, sz = shape.size
    rows = shape.rows
    ex, ez = even("gx"), even("gz")
    flip = (lax.axis_index("gy") == 1) if shape.mirror else False

    gx, gy = lax.axis_index("gx"), lax.axis_index("gy")
    inner = (gx > 0).astype(jnp.float32), (gx < shape.n[0] - 1).astype(jnp.float32)

    def put(c, row, low, mid, high):
        if c == W_CH:
            low, high = low * inner[0], high * inner[1]
        nat[c, row, 0:HALO] = low
        nat[c, row, HALO : HALO + sx] = mid
        nat[c, row, HALO + sx :] = high

    place = lax.rem(sub_ids(), HALO)
    for k in range(sy // 2):
        wlow = whigh = jnp.zeros((8, 128), jnp.float32)
        faces = {}
        for index, c in enumerate(CARRY):
            a, b = xrecv[0][index, k], xrecv[1][index, k]
            low, high = jnp.where(ex, b, a), jnp.where(ex, a, b)
            faces[c] = low, high
            if c in SHALLOW:
                q = SHALLOW.index(c)
                wlow = jnp.where(place == q, turn_x(low, q), wlow)
                whigh = jnp.where(place == q, turn_x(high, q + 1 - HALO), whigh)
        faces[W_CH] = wlow, whigh
        for c, (low, high) in faces.items():
            for h in range(2):
                part = slice(HALO * h, HALO * h + HALO)
                put(c, shape.own + 2 * k + h, low[part], own[c, 2 * k + h + 1], high[part])
    empty = jnp.zeros((sx + 2 * HALO, 128), jnp.float32)
    for c in SHALLOW:
        nat[c, rows - 1] = empty
        if not shape.mirror:
            nat[c, 0] = empty
    for side in range(1 if shape.mirror else 2):
        for k in range(len(LAYERS) // 2):
            near = LAYERS[2 * k : 2 * k + 2]
            if shape.mirror:
                a, b = xyrecv[0][k], xyrecv[1][k]
                mids = [yrecv[0][2 * k + h] for h in range(2)]
            else:
                lower = even("gy") if side else jnp.logical_not(even("gy"))
                a, b = (jnp.where(lower, xyrecv[i][k], xyrecv[2 + i][k]) for i in range(2))
                mids = [
                    jnp.where(lower, yrecv[0][2 * k + h], yrecv[1][2 * k + h]) for h in range(2)
                ]
            low, high = jnp.where(ex, b, a), jnp.where(ex, a, b)
            for h, (c, d) in enumerate(near):
                part = slice(HALO * h, HALO * h + HALO)
                values = [low[part], mids[h], high[part]]
                if shape.mirror:
                    row = sy + d
                    if c == W_CH:
                        row = row - jnp.where(flip, 1, 0)
                    if c in (1, 4):
                        values = [-t for t in values]
                else:
                    row = HALO + sy + d if side else HALO - 1 - d
                    if c == W_CH:
                        there = (gy < shape.n[1] - 1 if side else gy > 0).astype(jnp.float32)
                        values = [t * there for t in values]
                put(c, row, *values)
    nat[W_CH, rows - 1] = empty
    slot = lane_ids() // HALO
    for m in range(shape.erows):
        for t in range(2):
            up = jnp.zeros((8, 128), jnp.float32)
            down = jnp.zeros((8, 128), jnp.float32)
            for g in range(GROUPS):
                for c in range(CH):
                    tile = nat[c, g * shape.erows + m, pl.ds(t, 8, stride=2), :]
                    full[c, g * shape.erows + m, t] = tile
                    place = slot == (SPAN // HALO) * g + c
                    to = SPAN * g + HALO * c
                    up = jnp.where(place, roll_z(tile, to - (sz - HALO)), up)
                    down = jnp.where(place, roll_z(tile, to), down)
            zsend[0][m, t] = jnp.where(ez, up, down)
            zsend[1][m, t] = jnp.where(ez, down, up)


def load_row(ref, row, channels=range(3)):
    return [(ref[c, row, 0], ref[c, row, 1]) for c in channels]


def step_size(now, before, free):
    total = add2(now, before)
    total = add2(total, prev_x(total))
    return tuple(
        RELAX * f / (1.0 + 3.0 * (t + roll_z(t, 1))) for t, f in zip(total, free)
    )


def step_sizes(shape, full, gsize):
    zero = jnp.zeros((8, 128), jnp.float32)
    for row in range(shape.rows):
        now = load_row(full, row, (W_CH,))[0]
        before = load_row(full, row - 1, (W_CH,))[0] if row else (zero, zero)
        g = step_size(now, before, load_row(full, row, (FREE_CH,))[0])
        for t in range(2):
            gsize[row, t] = g[t]


def put9(ref, row, value):
    for c in range(3):
        for k in range(3):
            for t in range(2):
                ref[3 * c + k, row, t] = value[c][k][t]


def get9(ref, row):
    return [[(ref[3 * c + k, row, 0], ref[3 * c + k, row, 1]) for k in range(3)] for c in range(3)]


def packed_stresses(shape, weight, step, rows, flat):
    fflat, wflat, pflat = flat
    width = shape.size[0] + 2 * HALO - 1 - 2 * step
    spans = []
    for t in range(2):
        first = -(-(step - t) // 2)
        spans.append((first, (shape.size[0] + 2 * HALO - 2 - t - step) // 2 - first + 1))
    begin = rows[0]
    state = {"tiles": 0, "rows": 0}

    def at(j, t, first, count):
        return pl.ds(8 + (j - begin) * width + 2 * first + t - step, count, stride=2)

    def run(j, f):
        for t, (first, count) in enumerate(spans):
            here = at(j, t, first, count)
            part = slice(first, first + count)
            for c in range(3):
                for d in range(3):
                    fflat[3 * c + d, here, :] = f[c][d][t][part]
            wflat[here, :] = weight(j)[t][part]
        filled = (j - begin + 1) * width
        upto = filled // 8 if j < rows[-1] else -(-filled // 8)
        for i in range(state["tiles"], upto):
            tile = pl.ds(8 + 8 * i, 8)
            p = polar_stress(
                [[fflat[3 * c + d, tile, :] for d in range(3)] for c in range(3)], wflat[tile, :]
            )
            for c in range(3):
                for d in range(3):
                    pflat[3 * c + d, tile, :] = p[c][d]
        state["tiles"] = upto
        known = []
        while state["rows"] < len(rows) and (state["rows"] + 1) * width <= 8 * upto:
            r = begin + state["rows"]
            known.append(
                (
                    r,
                    [
                        [tuple(pflat[3 * c + d, at(r, t, 0, 8), :] for t in range(2)) for d in range(3)]
                        for c in range(3)
                    ],
                )
            )
            state["rows"] += 1
        return known

    return run


def main_steps(shape, full, gsize, old, oldest, write, grad, stress, part, step, flat=None):
    omega = omegas()[step]
    first = 0 if shape.mirror else step
    last = shape.rows - 1 - step
    zero = jnp.zeros((8, 128), jnp.float32)

    def update(row):
        held = [
            tuple((part[2 * c + i, row, 0], part[2 * c + i, row, 1]) for i in range(2))
            for c in range(3)
        ]
        write(
            row,
            update_row(
                held,
                load_row(old, row),
                load_row(full, row, (3, 4, 5)),
                load_row(oldest, row),
                (gsize[row, 0], gsize[row, 1]),
                omega,
            ),
        )

    def head():
        for row in (first, first + 1):
            put9(grad, row, gradient_row(load_row(old, row)))

    if flat:
        packed = packed_stresses(
            shape,
            lambda j: load_row(full, j, (W_CH,))[0],
            step,
            range(first, last),
            flat,
        )

    def body(j):
        after = gradient_row(load_row(old, j + 2)) if j + 2 <= last else None
        f = deform_rows(get9(grad, j), get9(grad, j + 1))
        if flat:
            known = packed(j, f)
        else:
            known = [(j, stress_row(f, load_row(full, j, (W_CH,))[0]))]
        if after is not None:
            put9(grad, j + 2, after)
        for r, now in known:
            before = get9(stress, r - 1) if r > first else [[(zero, zero)] * 3] * 3
            parts = force_parts(now, before)
            if r > first:
                update(r - 1)
            put9(stress, r, now)
            for c in range(3):
                for t in range(2):
                    for i in range(2):
                        part[2 * c + i, r, t] = parts[c][i][t]
            if r == last - 1:
                update(r)

    return head, [functools.partial(body, j) for j in range(first, last)]


def writer(ref):
    def write(row, new):
        for c in range(3):
            for t in range(2):
                ref[c, row, t] = new[c][t]

    return write


def main_kernel(shape, full, one, two, gsize, grad, stress, part, *flat):
    step_sizes(shape, full, gsize)
    for step, (old, oldest, new) in enumerate(((full, full, one), (one, full, two))):
        head, steps = main_steps(
            shape, full, gsize, old, oldest, writer(new), grad, stress, part, step, flat if step else None
        )
        head()
        for run in steps:
            run()


def edge_parts(shape, full, zrecv, bufs, goal, gsize, stiff, grad, stress, flat):
    sz = shape.size[2]
    erows = shape.erows
    ez = even("gz")
    lane = lane_ids()
    within = lane % SPAN
    half = SPAN // 2
    gz = lax.axis_index("gz")
    inner = (gz > 0).astype(jnp.float32), (gz < shape.n[2] - 1).astype(jnp.float32)

    def window(c, m, t):
        value = jnp.zeros((8, 128), jnp.float32)
        for g in range(GROUPS):
            tile = full[c, g * erows + m, t]
            base = SPAN * g
            value = jnp.where(
                (lane >= base + HALO) & (lane < base + half), roll_z(tile, base + HALO), value
            )
            value = jnp.where(
                (lane >= base + half) & (lane < base + SPAN - HALO),
                roll_z(tile, base + SPAN - HALO - sz),
                value,
            )
        return value

    def setup():
        for m in range(erows):
            for t in range(2):
                a, b = zrecv[0][m, t], zrecv[1][m, t]
                low, high = jnp.where(ez, b, a), jnp.where(ez, a, b)

                def extended(c):
                    below, above = roll_z(low, -HALO * c), roll_z(high, SPAN - HALO - HALO * c)
                    if c == W_CH:
                        below, above = below * inner[0], above * inner[1]
                    value = jnp.where(within < HALO, below, window(c, m, t))
                    return jnp.where(within >= SPAN - HALO, above, value)

                for c in range(3):
                    bufs[0][c, m, t] = extended(c)
                    goal[c, m, t] = extended(3 + c)
                stiff[m, t] = extended(W_CH)
                gsize[m, t] = extended(FREE_CH)
        weights = [(stiff[m, 0], stiff[m, 1]) for m in range(erows)]
        behind = tuple(roll_z(t, SPAN) for t in weights[-1])
        for m in range(erows):
            g = step_size(weights[m], weights[m - 1] if m else behind, (gsize[m, 0], gsize[m, 1]))
            for t in range(2):
                gsize[m, t] = g[t]

    def gradients(step):
        for m in range(erows):
            put9(grad, m, gradient_row(load_row(bufs[step], m)))
        turned = [tuple(roll_z(t, -SPAN) for t in pair) for pair in load_row(bufs[step], 0)]
        put9(grad, erows, gradient_row(turned))

    def keep(m, now):
        put9(stress, m + 1, now)
        if m == erows - 1:
            put9(stress, 0, [[tuple(roll_z(t, SPAN) for t in pair) for pair in row] for row in now])

    def stresses(step):
        def weight(m):
            return (stiff[m, 0], stiff[m, 1])

        rows = range(erows)
        if step:
            packed = packed_stresses(shape, weight, step, rows, flat)
        for m in rows if step else [erows - 1, *rows[:-1]]:
            f = deform_rows(get9(grad, m), get9(grad, m + 1))
            for known in packed(m, f) if step else [(m, stress_row(f, weight(m)))]:
                keep(*known)

    def updates(step, m):
        new = update_row(
            force_parts(get9(stress, m + 1), get9(stress, m)),
            load_row(bufs[step], m),
            load_row(goal, m),
            load_row(bufs[max(step - 1, 0)], m),
            (gsize[m, 0], gsize[m, 1]),
            omegas()[step],
        )
        writer(bufs[step + 1])(m, new)

    return setup, gradients, stresses, updates


def last_kernel(
    shape, full, one, two, gsize, zrecv0, zrecv1, out,
    three, grad, stress, part, bufs, egoal, egsize, estiff, egrad, estress, tiles, *flat,
):
    sx, sy, sz = shape.size
    erows = shape.erows
    lane = lane_ids()
    setup, gradients, stresses, updates = edge_parts(
        shape, full, (zrecv0, zrecv1), bufs, egoal, egsize, estiff, egrad, estress, flat[3:]
    )
    flat = flat[:3]
    flip = (lax.axis_index("gy") == 1) if shape.mirror else False
    turned = jnp.where(flip, -1.0 / SCALE, 1.0 / SCALE).astype(jnp.float32) if shape.mirror else 1.0 / SCALE

    def finish(row, new):
        r = row - shape.own
        if not 0 <= r < sy:
            return
        g, m = divmod(row, erows)
        base = SPAN * g
        place = jnp.where(flip, sy - 1 - r, r) if shape.mirror else r
        for c in range(3):
            for t in range(2):
                edge = bufs[ITERS][c, m, t]
                value = jnp.where(lane < HALO, roll_z(edge, -(base + HALO)), new[c][t])
                value = jnp.where(
                    lane >= sz - HALO, roll_z(edge, sz - HALO - (base + SPAN - 2 * HALO)), value
                )
                tiles[r, c, pl.ds(t, 8, stride=2), :] = value * (turned if c == 1 else 1.0 / SCALE)
            out[c, pl.ds(place, sx, stride=sy), :] = tiles[r, c, HALO : HALO + sx]

    edge = [setup]
    for step in range(ITERS):
        edge.append(functools.partial(gradients, step))
        edge.append(functools.partial(stresses, step))
        edge.append(lambda step=step: [updates(step, m) for m in range(erows)])
    head, steps = main_steps(
        shape, full, gsize, two, one, writer(three), grad, stress, part, 2, flat
    )
    head()
    total = len(steps)
    given = 0
    for index, run in enumerate(steps):
        upto = -(-len(edge) * (index + 1) // total)
        for work in edge[given:upto]:
            work()
        given = max(given, upto)
        run()
    head, steps = main_steps(shape, full, gsize, three, two, finish, grad, stress, part, 3, flat)
    head()
    for run in steps:
        run()


def partner(size, parity, i):
    j = i + 1 if i % 2 == parity else i - 1
    return j if 0 <= j < size else None


def exchange(shape, parities):
    n = shape.n
    pairs = []
    for i in range(n[0]):
        for j in range(n[1]):
            for k in range(n[2]):
                here = (i, j, k)
                there = [
                    at if parity is None else partner(size, parity, at)
                    for at, size, parity in zip(here, n, parities)
                ]
                if None in there:
                    axis = 1 if parities[2] is not None else 2
                    other = partner(n[axis], 0, here[axis])
                    if other is None:
                        continue
                    there = list(here)
                    there[axis] = other
                pairs.append(
                    ((i * n[1] + j) * n[2] + k, (there[0] * n[1] + there[1]) * n[2] + there[2])
                )
    return pairs


def send(shape, value, *parities):
    return lax.ppermute(value, ("gx", "gy", "gz"), exchange(shape, parities))


def f32(*dims):
    return jax.ShapeDtypeStruct(dims, jnp.float32)


def in_hbm(value):
    return pltpu.with_memory_space_constraint(value, pltpu.MemorySpace.HBM)


def scratch(*dims):
    return pltpu.VMEM(dims, jnp.float32)


def call(body, outs, args, scratches=(), specs=None):
    return pl.pallas_call(
        body,
        out_shape=outs,
        in_specs=specs or [VM] * len(args),
        out_specs=jax.tree.map(lambda _: VM, outs),
        scratch_shapes=list(scratches),
        compiler_params=pltpu.CompilerParams(vmem_limit_bytes=40 * 1024 * 1024),
        cost_estimate=pl.CostEstimate(flops=2_000_000, bytes_accessed=100_000, transcendentals=0),
    )(*args)


def per_device(mesh, start_disp, inertial, material, pinned, stiffness):
    shape = Shape(mesh, material.shape)
    sx, sy, sz = shape.size
    sides = 1 if shape.mirror else 2
    rows, erows = shape.rows, shape.erows

    def prep(*refs):
        count = 3 + 3 * sides
        given, (own, *sent), held, sems = refs[:5], refs[5 : 5 + count], refs[5 + count : -1], refs[-1]
        copies = [pltpu.make_async_copy(a, b, sems.at[i]) for i, (a, b) in enumerate(zip(given, held))]
        for copy in copies:
            copy.start()
        for copy in copies:
            copy.wait()
        prep_kernel(shape, *held, own, sent[2 : 2 + sides], sent[:2], sent[2 + sides :])

    outs = [f32(CH, sy + 1, sx, sz)]
    outs += [f32(len(CARRY), sy // 2, 8, sz)] * 2 + [f32(len(LAYERS), sx, sz)] * sides
    outs += [f32(len(LAYERS) // 2, 8, sz)] * (2 * sides)
    own, *sent = call(
        prep,
        outs,
        (
            in_hbm(start_disp.reshape(3, sx * sy, sz)),
            in_hbm(inertial.reshape(3, sx * sy, sz)),
            in_hbm(material.reshape(sx * sy, sz)),
            in_hbm(pinned.reshape(sx * sy, sz)),
            in_hbm(stiffness),
        ),
        [
            scratch(3, sx * sy, sz),
            scratch(3, sx * sy, sz),
            pltpu.VMEM((sx * sy, sz), jnp.int32),
            pltpu.VMEM((sx * sy, sz), jnp.int32),
            pltpu.SMEM((MATS,), jnp.float32),
            pltpu.SemaphoreType.DMA((5,)),
        ],
        [HBM] * 5,
    )
    recv = [send(shape, sent[p], p, None, None) for p in range(2)]
    recv += [send(shape, sent[2 + p], None, p, None) for p in range(sides)]
    recv += [
        send(shape, sent[2 + sides + 2 * q + p], p, q, None) for q in range(sides) for p in range(2)
    ]

    def join(own, *rest):
        x, rest = rest[:2], rest[2:]
        y, rest = rest[:sides], rest[sides:]
        xy, rest = rest[: 2 * sides], rest[2 * sides :]
        full, z0, z1, nat = rest
        join_kernel(shape, own, y, x, xy, full, (z0, z1), nat)

    full, z0, z1 = call(
        join,
        [f32(CH, rows, 2, 8, sz), f32(erows, 2, 8, sz), f32(erows, 2, 8, sz)],
        (own, *recv),
        [scratch(CH, rows, sx + 2 * HALO, sz)],
    )
    z0 = send(shape, z0, None, None, 0)
    z1 = send(shape, z1, None, None, 1)
    def flat(count):
        length = 16 * (count + 2)
        return [scratch(9, length, sz), scratch(length, sz), scratch(9, length, sz)]

    one, two, gsize = call(
        functools.partial(main_kernel, shape),
        [f32(3, rows, 2, 8, sz), f32(3, rows, 2, 8, sz), f32(rows, 2, 8, sz)],
        (full,),
        [scratch(count, rows, 2, 8, sz) for count in (9, 9, 6)] + flat(rows),
    )

    def last(*refs):
        ends = 11 + ITERS + 1
        full, one, two, gsize, z1, z0 = refs[:6]
        last_kernel(shape, full, one, two, gsize, z0, z1, *refs[6:11], refs[11:ends], *refs[ends:])

    (out,) = call(
        last,
        [f32(3, sx * sy, sz)],
        (full, one, two, gsize, z1, z0),
        [scratch(3, rows, 2, 8, sz)]
        + [scratch(count, rows, 2, 8, sz) for count in (9, 9, 6)]
        + [scratch(3, erows, 2, 8, sz) for _ in range(ITERS + 2)]
        + [scratch(erows, 2, 8, sz)] * 2
        + [scratch(9, erows + 1, 2, 8, sz)] * 2
        + [scratch(sy, 3, 2 * 8, sz)]
        + flat(rows)
        + flat(erows),
    )
    return out.reshape(3, sx, sy, sz)


def solution(mesh):
    placed = (
        P(None, "gx", "gy", "gz"),
        P(None, "gx", "gy", "gz"),
        P("gx", "gy", "gz"),
        P("gx", "gy", "gz"),
        P(),
    )
    return jax.shard_map(
        functools.partial(per_device, mesh),
        mesh=mesh,
        in_specs=placed,
        out_specs=P(None, "gx", "gy", "gz"),
        check_vma=False,
    )
```
